32 devices in a mesh: rows: 32 (over z, y, x, core).
Axes of the slice: x: 2, y: 2, z: 4, core: 2. Of those that a mesh axis runs over, the one named last changes fastest.
Arguments:
- elevation_grid: float32 [2048, 640], P('rows'), may hold values from -200 to 200
Outputs:
- slope_field: float32 [2048, 640], P('rows')
- bend_field: float32 [2048, 640], P('rows')
The draws below stay inside these ranges and needn't reach their ends.
All inputs are finite; a program needn't handle non-finite values.
Results may differ from the reference program's by a relative error of at most 0.0003.
Values sent between devices are 32-bit elements; how exact they have to be, the bound alone decides.
No kernel may reach another device: no remote copies, remote signals or barrier semaphores. Data moves between devices by JAX's collectives and lax.ppermute only.
A program may use at most 64 MiB of HBM per device.

```python
import jax
import jax.numpy as jnp
from jax import lax

BAND = 64
COLS = 640
LEVELS = 4
ROWS_ALL = 2048


def draw_elevation_grid(key, part):
    terrain = jnp.zeros((ROWS_ALL, COLS), jnp.float32)
    for octave in range(LEVELS + 1):
        factor = 2 ** octave
        subkey = jax.random.fold_in(key, 101 + octave)
        grid_shape = (ROWS_ALL // factor, COLS // factor)
        noise_grid = jnp.clip(jax.random.normal(subkey, grid_shape, jnp.float32), -4.0, 4.0)
        coarse = jnp.repeat(jnp.repeat(noise_grid, factor, axis=0), factor, axis=1)
        terrain = terrain + 0.5 * factor * coarse
    roughness = 1.0 + 2.0 * jnp.arange(ROWS_ALL, dtype=jnp.float32) / (ROWS_ALL - 1)
    return terrain * roughness[:, None]


def setup_inputs(seed: int = 0) -> dict:
    streams_of = jax.random.split(jax.random.key(seed), 2)
    return {
        "elevation_grid": draw_elevation_grid(jax.random.fold_in(streams_of[1], 71), 0),
    }


TAPS = (0.0625, 0.25, 0.375, 0.25, 0.0625)
epsilon = 1e-06

def coarsen_axis(padded, axis):
    length = padded.shape[axis] - 4
    result = None
    for offset in range(5):
        piece = lax.slice_in_dim(padded, offset, offset + length, 2, axis)
        term = TAPS[offset] * piece
        result = term if result is None else result + term
    return result

def coarsen(padded_rows):
    halfway = coarsen_axis(padded_rows, 0)
    wider = jnp.pad(halfway, ((0, 0), (2, 2)), mode='edge')
    return coarsen_axis(wider, 1)

def derive(extended, spacing):
    padded = jnp.pad(extended, ((0, 0), (1, 1)), mode='edge')
    upper = padded[:-2]
    middle = padded[1:-1]
    lower = padded[2:]
    eastern = upper[:, 2:] + 2.0 * middle[:, 2:] + lower[:, 2:]
    western = upper[:, :-2] + 2.0 * middle[:, :-2] + lower[:, :-2]
    southern = lower[:, :-2] + 2.0 * lower[:, 1:-1] + lower[:, 2:]
    northern = upper[:, :-2] + 2.0 * upper[:, 1:-1] + upper[:, 2:]
    grad_x = (eastern - western) / (8.0 * spacing)
    grad_y = (southern - northern) / (8.0 * spacing)
    centre = middle[:, 1:-1]
    second_xx = (middle[:, 2:] - 2.0 * centre + middle[:, :-2]) / (spacing * spacing)
    second_yy = (lower[:, 1:-1] - 2.0 * centre + upper[:, 1:-1]) / (spacing * spacing)
    second_xy = (lower[:, 2:] - lower[:, :-2] - upper[:, 2:] + upper[:, :-2]) / (4.0 * spacing * spacing)
    steepness = grad_x * grad_x + grad_y * grad_y
    slope_part = jnp.arctan(jnp.sqrt(steepness))
    numerator = grad_x * grad_x * second_xx + 2.0 * grad_x * grad_y * second_xy + grad_y * grad_y * second_yy
    bend_part = -numerator / (1.0 + steepness) ** 1.5
    return (slope_part, bend_part)

def settle(extended, margin, begin_at, limit_rows):
    inside = extended.shape[0] - 2 * margin
    global_row = begin_at - margin + jnp.arange(extended.shape[0], dtype=jnp.int32)
    first_row = extended[margin:margin + 1]
    bottom = extended[margin + inside - 1:margin + inside]
    extended = jnp.where((global_row < 0)[:, None], first_row, extended)
    return jnp.where((global_row >= limit_rows)[:, None], bottom, extended)

def refine_axis(padded, factor, axis):
    length = padded.shape[axis] - 2
    pieces = []
    for sub_row in range(factor):
        position = (sub_row + 0.5) / factor
        if sub_row < factor // 2:
            offset = 0
            fraction = position + 0.5
        else:
            offset = 1
            fraction = position - 0.5
        lower_side = lax.slice_in_dim(padded, offset, offset + length, 1, axis)
        upper_side = lax.slice_in_dim(padded, offset + 1, offset + 1 + length, 1, axis)
        pieces.append((1.0 - fraction) * lower_side + fraction * upper_side)
    stacked = jnp.stack(pieces, axis + 1)
    new_shape = list(padded.shape)
    new_shape[axis] = length * factor
    return stacked.reshape(new_shape)

def spread(part, octave):
    if octave == 0:
        return part[1:-1]
    factor = 2 ** octave
    taller = refine_axis(part, factor, 0)
    return refine_axis(jnp.pad(taller, ((0, 0), (1, 1)), mode='edge'), factor, 1)

def finish(slope_parts, bend_parts, slope_sums, square_sums, cell_counts):
    slope_total = None
    bend_total = None
    for octave in range(len(slope_parts)):
        mean_slope = slope_sums[octave] / cell_counts[octave]
        rms_bend = jnp.sqrt(square_sums[octave] / cell_counts[octave] + epsilon)
        slope_term = spread(slope_parts[octave], octave) / (mean_slope + epsilon)
        bend_term = spread(bend_parts[octave], octave) / rms_bend
        slope_total = slope_term if slope_total is None else slope_total + slope_term
        bend_total = bend_term if bend_total is None else bend_total + bend_term
    return (slope_total, bend_total)

def reference(elevation_grid):
    line_sum, entire_span = elevation_grid.shape
    bands = line_sum // BAND
    surface_levels = [elevation_grid]
    for octave in range(LEVELS):
        surface_levels.append(coarsen(jnp.pad(surface_levels[-1], ((2, 2), (0, 0)), mode='edge')))
    padded_list = [jnp.pad(surface_level, ((2, 2), (0, 0)), mode='edge') for surface_level in surface_levels]
    cell_counts = [line_sum // 2 ** octave * (entire_span // 2 ** octave) for octave in range(LEVELS + 1)]

    def band_parts(band_index):
        slope_parts = []
        bend_parts = []
        for octave in range(LEVELS + 1):
            height_now = BAND // 2 ** octave
            begin_at = band_index * height_now
            window = lax.dynamic_slice_in_dim(padded_list[octave], begin_at, height_now + 4, 0)
            slope_part, bend_part = derive(window, float(2 ** octave))
            limit_rows = line_sum // 2 ** octave
            slope_parts.append(settle(slope_part, 1, begin_at, limit_rows))
            bend_parts.append(settle(bend_part, 1, begin_at, limit_rows))
        return (slope_parts, bend_parts)

    def band_sums(band_index):
        slope_parts, bend_parts = band_parts(band_index)
        first = jnp.stack([jnp.sum(part[1:-1]) for part in slope_parts])
        second = jnp.stack([jnp.sum(part[1:-1] * part[1:-1]) for part in bend_parts])
        return (first, second)
    indices = jnp.arange(bands, dtype=jnp.int32)
    sums_first, sums_second = lax.map(band_sums, indices)
    slope_sums = lax.optimization_barrier(jnp.sum(sums_first, 0))
    square_sums = lax.optimization_barrier(jnp.sum(sums_second, 0))

    def band_out(band_index):
        slope_parts, bend_parts = band_parts(band_index)
        return finish(slope_parts, bend_parts, slope_sums, square_sums, cell_counts)
    slope_bands, bend_bands = lax.map(band_out, indices)
    return (slope_bands.reshape(line_sum, entire_span), bend_bands.reshape(line_sum, entire_span))
```

```python
import functools

import jax
import jax.numpy as jnp
from jax import lax
from jax.experimental import pallas as pl
from jax.experimental.pallas import tpu as pltpu
from jax.sharding import PartitionSpec as P

LEVELS = 4
EPS = 1e-06
OFF = 8
MSG_ROWS = 16
f32 = jnp.float32
bf16 = jnp.bfloat16
ATAN = (
    1.0,
    -0.3333314528,
    0.1999355085,
    -0.1420889944,
    0.1065626393,
    -0.0752896400,
    0.0429096138,
    -0.0161657367,
    0.0028662257,
)


def up128(n):
    return -(-n // 128) * 128


def up16(n):
    return -(-n // 16) * 16


def lane_of(v):
    return lax.broadcasted_iota(jnp.int32, v.shape, 1)


def row_of(v):
    return lax.broadcasted_iota(jnp.int32, v.shape, 0)


def west(v):
    return jnp.where(lane_of(v) == 0, v, pltpu.roll(v, 1, 1))


def east(v, width):
    return jnp.where(lane_of(v) == width - 1, v, pltpu.roll(v, v.shape[1] - 1, 1))


def split3(v):
    hi = v.astype(bf16)
    rest = v - hi.astype(f32)
    mid = rest.astype(bf16)
    low = (rest - mid.astype(f32)).astype(bf16)
    return hi, mid, low


def split2(v):
    hi = v.astype(bf16)
    return hi, (v - hi.astype(f32)).astype(bf16)


def mm(a, b):
    return jnp.dot(a, b, preferred_element_type=f32)


def picker():
    rows = lax.broadcasted_iota(jnp.int32, (256, 128), 0)
    cols = lax.broadcasted_iota(jnp.int32, (256, 128), 1)
    return (rows == 2 * cols).astype(f32).astype(bf16)


def take(ref, at, count):
    return jnp.concatenate([ref[c, at : at + count, :] for c in range(ref.shape[0])], axis=1)


def store(ref, at, v):
    for c in range(ref.shape[0]):
        ref[c, at : at + v.shape[0], :] = v[:, 128 * c : 128 * c + 128]


def rows_sum(ref, start, count):
    out = []
    for c in range(ref.shape[0]):
        part = [ref[c, pl.ds(start + a, count, 2), :] for a in range(5)]
        out.append((part[0] + part[4]) * 0.0625 + (part[1] + part[3]) * 0.25 + part[2] * 0.375)
    return jnp.concatenate(out, axis=1)


def cols_coarsen(v, width, pick):
    w1 = west(v)
    e1 = east(v, width)
    y = (west(w1) + east(e1, width)) * 0.0625 + (w1 + e1) * 0.25 + v * 0.375
    out = []
    for at in range(0, v.shape[1], 256):
        part = y[:, at : at + 256]
        sel = pick[: part.shape[1]]
        hi, mid, low = split3(part)
        out.append(mm(hi, sel) + (mm(mid, sel) + mm(low, sel)))
    return out[0] if len(out) == 1 else jnp.concatenate(out, axis=1)


def pyramid_kernel(sizes, x_ref, m1_ref, m2_ref, z1, z2, z3, z4, z0, tmp):
    pick = picker()
    store(z0, 0, x_ref[...])
    zs = [z0, z1, z2, z3, z4]
    low, high = 0, sizes[0][0] - 1
    spans = []
    for k in range(LEVELS):
        low, high = (low + 3) // 2, (high - 2) // 2
        spans.append((low, high))
        wp = up128(sizes[k][1])
        count = high - low + 1
        rows = -(-(high + 1) // 8) * 8
        tmp[low : high + 1, :wp] = rows_sum(zs[k], 2 * low - 2, count)
        store(zs[k + 1], 0, cols_coarsen(tmp[0:rows, :wp], sizes[k][1], pick))
    odd = lax.rem(lax.axis_index("rows"), 2) == 1
    h = sizes[0][0]

    def put(row, level, top_at, bottom_at, count):
        wp = up128(sizes[level][1])
        top = take(zs[level], top_at, count)
        bottom = take(zs[level], bottom_at, count)
        m1_ref[row : row + count, :wp] = jnp.where(odd, top, bottom)
        m2_ref[row : row + count, :wp] = jnp.where(odd, bottom, top)

    put(0, 0, 0, h - 4, 4)
    row = 4
    for k in range(1, LEVELS):
        low, high = spans[k - 1]
        put(row, k, low, high - 3, 4)
        row += 4
    m = spans[LEVELS - 1][1]
    wp = up128(sizes[LEVELS][1])
    at = m1_ref.shape[1] - wp
    m1_ref[12:13, at:] = take(zs[LEVELS], m, 1)
    m2_ref[12:13, at:] = take(zs[LEVELS], m, 1)


def relief(upper, middle, lower, width, spacing):
    diff = lower - upper
    ends = lower + upper
    tall = ends + 2.0 * middle
    m_e, m_w = east(middle, width), west(middle)
    d_e, d_w = east(diff, width), west(diff)
    p = (east(tall, width) - west(tall)) * (1.0 / (8.0 * spacing))
    q = (d_e + d_w + 2.0 * diff) * (1.0 / (8.0 * spacing))
    inv = 1.0 / (spacing * spacing)
    r = ((m_e - middle) - (middle - m_w)) * inv
    t = ((lower - middle) - (middle - upper)) * inv
    u = (d_e - d_w) * (0.25 * inv)
    pp, qq = p * p, q * q
    steep = pp + qq
    base = 1.0 + steep
    root = jnp.sqrt(base)
    y = jnp.sqrt(steep) / (1.0 + root)
    y2 = y * y
    acc = ATAN[-1]
    for c in ATAN[-2::-1]:
        acc = acc * y2 + c
    slope = 2.0 * y * acc
    bend = -(pp * r + 2.0 * (p * q) * u + qq * t) / (base * root)
    return slope, bend


def relief_kernel(sizes, mid, x_ref, z1, z2, z3, z4, r1_ref, r2_ref, r3_ref, s0_ref, b0_ref, f1, f2, f3, f4, sum_ref,
                  up, lo, ztop, zbot, w1, w2, w3, w4, tmp):
    me = lax.axis_index("rows")
    last_id = lax.axis_size("rows") - 1
    odd = lax.rem(me, 2) == 1
    first, last = me == 0, me == last_id
    r2 = r2_ref[...]
    if mid:
        r2 = jnp.where((me == mid) | (me == mid - 1), r3_ref[...], r2)
    r1 = r1_ref[...]
    up[...] = jnp.where(odd, r1, r2)
    lo[...] = jnp.where(odd, r2, r1)
    pick = picker()
    h0, width0 = sizes[0]

    store(ztop, 8, x_ref[0:8, :])
    store(ztop, 4, jnp.where(first, jnp.broadcast_to(x_ref[0:1, :], (4, width0)), up[0:4, :]))
    store(zbot, 0, x_ref[h0 - 8 : h0, :])
    store(zbot, 8, jnp.where(last, jnp.broadcast_to(x_ref[h0 - 1 : h0, :], (4, width0)), lo[0:4, :]))

    work = [None, w1, w2, w3, w4]
    given = [None, z1, z2, z3, z4]
    last_at = up.shape[1] - up128(sizes[LEVELS][1])
    for k in range(1, LEVELS + 1):
        h, width = sizes[k]
        wp, wq = up128(width), up128(sizes[k - 1][1])
        z = work[k]
        store(z, OFF, take(given[k], 0, given[k].shape[1]))
        if k == 1:
            tmp[0:3, :wq] = rows_sum(ztop, 4, 3)
            tmp[3:5, :wq] = rows_sum(zbot, 4, 2)
        else:
            prev_h = sizes[k - 1][0]
            tmp[0:3, :wq] = rows_sum(work[k - 1], OFF - 4, 3)
            tmp[3:6, :wq] = rows_sum(work[k - 1], OFF + prev_h - 4, 3)
        edge = cols_coarsen(tmp[0:8, :wq], sizes[k - 1][1], pick)
        row0, bottom = edge[1:2], edge[3:4]
        store(z, OFF, edge[1:3])
        store(z, OFF - 1, jnp.where(first, row0, edge[0:1]))
        store(z, OFF + h - 1, bottom)
        store(z, OFF + h, jnp.where(last, bottom, edge[4:5]))
        at = 4 * k
        if k == 1:
            store(z, OFF + h + 1, jnp.where(last, jnp.broadcast_to(bottom, (4, wp)), lo[at : at + 4, :wp]))
        else:
            store(z, OFF + h + 1, jnp.where(last, bottom, edge[5:6]))
            if k < LEVELS:
                store(z, OFF + h + 2, jnp.where(last, jnp.broadcast_to(bottom, (3, wp)), lo[at : at + 3, :wp]))
        if k < LEVELS:
            store(z, OFF - 4, jnp.where(first, jnp.broadcast_to(row0, (3, wp)), up[at + 1 : at + 4, :wp]))
        else:
            store(z, OFF - 2, jnp.where(first, row0, up[12:13, last_at:]))

    slope_sums, bend_sums = [], []

    def fold(v):
        total = v[:, 0:128]
        for at in range(128, v.shape[1], 128):
            total = total + v[:, at : at + 128]
        return total

    s_sum, b_sum = None, None
    for at in range(0, h0, 8):
        top, end = at == 0, at == h0 - 8
        upper = take(ztop, 7, 8) if top else x_ref[at - 1 : at + 7, :]
        middle = x_ref[at : at + 8, :]
        lower = take(zbot, 1, 8) if end else x_ref[at + 1 : at + 9, :]
        slope, bend = relief(upper, middle, lower, width0, 1.0)
        s0_ref[at : at + 8, :] = slope
        b0_ref[at : at + 8, :] = bend
        fs, fb = fold(slope), fold(bend * bend)
        s_sum = fs if top else s_sum + fs
        b_sum = fb if top else b_sum + fb
    slope_sums.append(s_sum)
    bend_sums.append(b_sum)
    for k, out in zip(range(1, LEVELS + 1), (f1, f2, f3, f4)):
        h, width = sizes[k]
        wp = up128(width)
        z = work[k]
        s_sum = b_sum = jnp.zeros((8, 128), f32)
        tiles = -(-(h + 2) // 8)
        for tile in range(tiles):
            at = OFF - 1 + 8 * tile
            slope, bend = relief(take(z, at - 1, 8), take(z, at, 8), take(z, at + 1, 8), width, float(2**k))
            row = row_of(slope) + (8 * tile - 1)
            kept = row <= h
            inner = (row >= 0) & (row < h) & (lane_of(slope) < width)
            s_sum = s_sum + fold(jnp.where(inner, slope, 0.0))
            b_sum = b_sum + fold(jnp.where(inner, bend * bend, 0.0))
            slope, bend = jnp.where(kept, slope, 0.0), jnp.where(kept, bend, 0.0)
            out[0, 8 * tile : 8 * tile + 8, :] = slope
            out[1, 8 * tile : 8 * tile + 8, :] = bend
        for field in range(2):
            if out.shape[1] > 8 * tiles:
                out[field, 8 * tiles :, :] = jnp.zeros((out.shape[1] - 8 * tiles, wp), f32)
            out[field, 0:1, :] = jnp.where(first, out[field, 1:2, :], out[field, 0:1, :])
            out[field, h + 1 : h + 2, :] = jnp.where(last, out[field, h : h + 1, :], out[field, h + 1 : h + 2, :])
        slope_sums.append(s_sum)
        bend_sums.append(b_sum)
    lane = lax.broadcasted_iota(jnp.int32, (1, 128), 1)
    line = jnp.zeros((1, 128), f32)
    for i, v in enumerate(slope_sums + bend_sums):
        total = jnp.sum(jnp.sum(v, axis=0, keepdims=True), axis=1, keepdims=True)
        line = jnp.where(lane == i, total, line)
    sum_ref[...] = jnp.broadcast_to(line.reshape(1, 1, 128), sum_ref.shape)


def hat(shape, factor, count, shift, along):
    fine = lax.broadcasted_iota(jnp.int32, shape, along).astype(f32)
    coarse = lax.broadcasted_iota(jnp.int32, shape, 1 - along).astype(f32)
    y = (fine + 0.5) * (1.0 / factor) - 0.5
    if count is not None:
        y = jnp.clip(y, 0.0, count - 1.0)
    return jnp.maximum(0.0, 1.0 - jnp.abs(y + shift - coarse)).astype(bf16)


def spread_kernel(sizes, f1, f2, f3, f4, u1, u2, u3, u4):
    h0, width0 = sizes[0]
    for k, f, u in zip(range(1, LEVELS + 1), (f1, f2, f3, f4), (u1, u2, u3, u4)):
        rows, wp = f.shape[1], f.shape[2]
        across = hat((wp, width0), 2**k, sizes[k][1], 0.0, 1)
        down = hat((h0, rows), 2**k, None, 1.0, 0)
        for field in range(2):
            hi, low = split2(f[field])
            wide = mm(hi, across) + mm(low, across)
            hi, low = split2(wide)
            u[field] = mm(down, hi) + mm(down, low)


def blend_kernel(cells, v_ref, s0, b0, u1, u2, u3, u4, slope_ref, bend_ref, slope_buf, bend_buf, sems):
    sums = jnp.sum(v_ref[...], axis=0)
    lane = lax.broadcasted_iota(jnp.int32, (1, 128), 1)
    count = jnp.ones((1, 128), f32)
    for k, c in enumerate(cells):
        count = jnp.where((lane == k) | (lane == k + LEVELS + 1), float(c), count)
    mean = sums / count
    scale = jnp.where(lane <= LEVELS, 1.0 / (mean + EPS), 1.0 / jnp.sqrt(mean + EPS))
    rows = slope_buf.shape[0]
    copies = []
    for field, (base, buf, out) in enumerate(((s0, slope_buf, slope_ref), (b0, bend_buf, bend_ref))):
        factors = [jnp.broadcast_to(scale[:, i : i + 1], (8, 128)) for i in range(field * (LEVELS + 1), (field + 1) * (LEVELS + 1))]
        for half in range(2):
            for at in range(half * rows // 2, (half + 1) * rows // 2, 8):
                for c in range(0, buf.shape[1], 128):
                    total = base[at : at + 8, c : c + 128] * factors[0]
                    for factor, u in zip(factors[1:], (u1, u2, u3, u4)):
                        total = total + u[field, at : at + 8, c : c + 128] * factor
                    buf[at : at + 8, c : c + 128] = total
            part = pl.ds(half * rows // 2, rows // 2)
            copy = pltpu.make_async_copy(buf.at[part], out.at[part], sems.at[2 * field + half])
            copy.start()
            copies.append(copy)
    for copy in copies:
        copy.wait()


def halo_pairs(count):
    both = lambda pairs: [(a, b) for a, b in pairs] + [(b, a) for a, b in pairs]
    even = [(i, i + 1) for i in range(0, count - 1, 2)]
    odd = [(i, i + 1) for i in range(1, count - 1, 2)]
    if count % 4 or count < 8:
        return both(even), both(odd), None, 0
    mid = count // 2
    second = [e for e in odd if e[0] != mid - 1] + [(0, mid), (mid - 1, count - 1)]
    third = [e for e in even if e[0] not in (mid - 2, mid)] + [(mid - 1, mid), (mid - 2, mid + 1)]
    return both(even), both(second), both(third), mid


VM = pl.BlockSpec(memory_space=pltpu.VMEM)
HBM = pl.BlockSpec(memory_space=pl.ANY)


def call(kernel, name, outs, scratch, out_specs=None, flops=0, limit=8 << 20):
    return lambda *args: pl.pallas_call(
        kernel,
        name=name,
        out_shape=[jax.ShapeDtypeStruct(s, f32) for s in outs],
        in_specs=[VM] * len(args),
        out_specs=out_specs or [VM] * len(outs),
        scratch_shapes=scratch,
        compiler_params=pltpu.CompilerParams(vmem_limit_bytes=limit),
        cost_estimate=pl.CostEstimate(flops=flops, bytes_accessed=1 << 19, transcendentals=0),
    )(*args)


def local(grid):
    h0, width0 = grid.shape
    count = lax.axis_size("rows")
    sizes = [(h0 >> k, width0 >> k) for k in range(LEVELS + 1)]
    rows8 = lambda n: -(-n // 8) * 8
    blocks = lambda rows, width: (up128(width) // 128, rows8(rows), 128)
    z_shapes = [blocks(h, w) for h, w in sizes[1:]]
    msg = (MSG_ROWS, width0)
    m1, m2, *zs = call(
        functools.partial(pyramid_kernel, sizes),
        "pyramid",
        [msg, msg] + z_shapes,
        [pltpu.VMEM(blocks(h0, width0), f32), pltpu.VMEM((rows8(h0 // 2), width0), f32)],
        flops=10**7,
    )(grid)
    pairs1, pairs2, pairs3, mid = halo_pairs(count)
    r2 = lax.ppermute(m2, "rows", pairs2)
    r3 = lax.ppermute(m2, "rows", pairs3) if mid else m2
    r1 = lax.ppermute(m1, "rows", pairs1)
    f_shapes = [(2, up16(h + 2), up128(w)) for h, w in sizes[1:]]
    s0, b0, f1, f2, f3, f4, sums = call(
        functools.partial(relief_kernel, sizes, mid),
        "relief",
        [grid.shape, grid.shape] + f_shapes + [(count, 1, 128)],
        [pltpu.VMEM(msg, f32)] * 2
        + [pltpu.VMEM(blocks(16, width0), f32)] * 2
        + [pltpu.VMEM(blocks(h + 16, w), f32) for h, w in sizes[1:]]
        + [pltpu.VMEM((8, width0), f32)],
        flops=2 * 10**7,
    )(grid, *zs, r1, r2, r3)
    seen = lax.all_to_all(sums, "rows", 0, 0, tiled=True)
    us = call(
        functools.partial(spread_kernel, sizes),
        "spread",
        [(2, h0, width0)] * LEVELS,
        [],
        flops=10**9,
        limit=16 << 20,
    )(f1, f2, f3, f4)
    cells = [count * h * w for h, w in sizes]
    return tuple(
        call(
            functools.partial(blend_kernel, cells),
            "blend",
            [grid.shape, grid.shape],
            [pltpu.VMEM(grid.shape, f32)] * 2 + [pltpu.SemaphoreType.DMA((4,))],
            out_specs=[HBM, HBM],
            flops=10**6,
        )(seen, s0, b0, *us)
    )


def solution(mesh):
    return jax.shard_map(
        local,
        mesh=mesh,
        in_specs=(P("rows", None),),
        out_specs=(P("rows", None), P("rows", None)),
        check_vma=False,
    )
```

```python
import functools

import jax
import jax.numpy as jnp
from jax import lax
from jax.experimental import pallas as pl
from jax.experimental.pallas import tpu as pltpu
from jax.sharding import PartitionSpec as P

LEVELS = 4
EPS = 1e-06
f32 = jnp.float32
bf16 = jnp.bfloat16
ATAN = (
    1.0,
    -0.3333314528,
    0.1999355085,
    -0.1420889944,
    0.1065626393,
    -0.0752896400,
    0.0429096138,
    -0.0161657367,
    0.0028662257,
)


def up128(n):
    return -(-n // 128) * 128


def up16(n):
    return -(-n // 16) * 16


def lane_of(v):
    return lax.broadcasted_iota(jnp.int32, v.shape, 1)


def row_of(v):
    return lax.broadcasted_iota(jnp.int32, v.shape, 0)


def west(v):
    return jnp.where(lane_of(v) == 0, v, pltpu.roll(v, 1, 1))


def east(v, width):
    return jnp.where(lane_of(v) == width - 1, v, pltpu.roll(v, v.shape[1] - 1, 1))


def split3(v):
    hi = v.astype(bf16)
    rest = v - hi.astype(f32)
    mid = rest.astype(bf16)
    low = (rest - mid.astype(f32)).astype(bf16)
    return hi, mid, low


def split2(v):
    hi = v.astype(bf16)
    return hi, (v - hi.astype(f32)).astype(bf16)


def mm(a, b):
    return jnp.dot(a, b, preferred_element_type=f32)


def picker():
    rows = lax.broadcasted_iota(jnp.int32, (256, 128), 0)
    cols = lax.broadcasted_iota(jnp.int32, (256, 128), 1)
    return (rows == 2 * cols).astype(f32).astype(bf16)


def take(ref, at, count):
    return jnp.concatenate([ref[c, at : at + count, :] for c in range(ref.shape[0])], axis=1)


def store(ref, at, v):
    for c in range(ref.shape[0]):
        ref[c, at : at + v.shape[0], :] = v[:, 128 * c : 128 * c + 128]


def rows_sum(ref, start, count):
    out = []
    for c in range(ref.shape[0]):
        part = [ref[c, pl.ds(start + a, count, 2), :] for a in range(5)]
        out.append((part[0] + part[4]) * 0.0625 + (part[1] + part[3]) * 0.25 + part[2] * 0.375)
    return jnp.concatenate(out, axis=1)


def cols_coarsen(v, width, pick):
    w1 = west(v)
    e1 = east(v, width)
    y = (west(w1) + east(e1, width)) * 0.0625 + (w1 + e1) * 0.25 + v * 0.375
    out = []
    for at in range(0, v.shape[1], 256):
        part = y[:, at : at + 256]
        sel = pick[: part.shape[1]]
        hi, mid, low = split3(part)
        out.append(mm(hi, sel) + (mm(mid, sel) + mm(low, sel)))
    return out[0] if len(out) == 1 else jnp.concatenate(out, axis=1)


def pyramid_kernel(sizes, x_ref, m1_ref, m2_ref, z0, z1, z2, tmp, sems):
    copies = [
        pltpu.make_async_copy(x_ref.at[:, pl.ds(128 * c, 128)], z0.at[c], sems.at[c]) for c in range(z0.shape[0])
    ]
    for copy in copies:
        copy.start()
    pick = picker()
    odd = lax.rem(lax.axis_index("rows"), 2) == 1
    h = sizes[0][0]
    for copy in copies:
        copy.wait()

    def put(row, z, top_at, bottom_at, count):
        for c in range(z.shape[0]):
            top, bottom = z[c, top_at : top_at + count, :], z[c, bottom_at : bottom_at + count, :]
            m1_ref[row : row + count, :] = jnp.where(odd, top, bottom)
            m2_ref[row : row + count, :] = jnp.where(odd, bottom, top)
            row += count
        return row

    row = put(0, z0, 0, h - 4, 4)
    for k, z in ((0, z1), (1, z2)):
        half, wp = sizes[k + 1][0], up128(sizes[k][1])
        low = k + 1
        tmp[low : half - 1, :wp] = rows_sum((z0, z1)[k], 2 * low - 2, half - 1 - low)
        store(z, 0, cols_coarsen(tmp[0:half, :wp], sizes[k][1], pick))
    row = put(row, z1, 1, sizes[1][0] - 5, 4)
    put(row, z2, 0, 0, sizes[2][0])


def relief(upper, middle, lower, width, spacing):
    diff = lower - upper
    ends = lower + upper
    tall = ends + 2.0 * middle
    m_e, m_w = east(middle, width), west(middle)
    d_e, d_w = east(diff, width), west(diff)
    p = (east(tall, width) - west(tall)) * (1.0 / (8.0 * spacing))
    q = (d_e + d_w + 2.0 * diff) * (1.0 / (8.0 * spacing))
    inv = 1.0 / (spacing * spacing)
    r = ((m_e - middle) - (middle - m_w)) * inv
    t = ((lower - middle) - (middle - upper)) * inv
    u = (d_e - d_w) * (0.25 * inv)
    pp, qq = p * p, q * q
    steep = pp + qq
    base = 1.0 + steep
    root = jnp.sqrt(base)
    y = jnp.sqrt(steep) / (1.0 + root)
    y2 = y * y
    acc = ATAN[-1]
    for c in ATAN[-2::-1]:
        acc = acc * y2 + c
    slope = 2.0 * y * acc
    bend = -(pp * r + 2.0 * (p * q) * u + qq * t) / (base * root)
    return slope, bend


def fold(v):
    total = None
    for row in range(0, v.shape[0], 8):
        for at in range(0, v.shape[1], 128):
            part = v[row : row + 8, at : at + 128]
            total = part if total is None else total + part
    return total


def inner_kernel(sizes, z0, z1, z2, s0_ref, b0_ref, f1, f2, acc_ref):
    for k, z in enumerate((z0, z1, z2)):
        h, width = sizes[k]
        s_sum = b_sum = None
        for at in range(0, h, 8):
            middle = take(z, at, 8)
            upper = take(z, at - 1, 8) if at else pltpu.roll(middle, 1, 0)
            lower = take(z, at + 1, 8) if at < h - 8 else pltpu.roll(middle, 7, 0)
            slope, bend = relief(upper, middle, lower, width, float(2**k))
            if k == 0:
                s0_ref[at : at + 8, :] = slope
                b0_ref[at : at + 8, :] = bend
            else:
                f = (f1, f2)[k - 1]
                f[0, at + 1 : at + 9, :] = slope
                f[1, at + 1 : at + 9, :] = bend
            skip = 3 if k else 1
            if at == 0 or at == h - 8 or width % 128:
                row = row_of(slope) + at
                kept = (row >= skip) & (row < h - skip) & (lane_of(slope) < width)
                slope, bend = jnp.where(kept, slope, 0.0), jnp.where(kept, bend, 0.0)
            fs, fb = fold(slope), fold(bend * bend)
            s_sum = fs if at == 0 else s_sum + fs
            b_sum = fb if at == 0 else b_sum + fb
        acc_ref[k] = s_sum
        acc_ref[LEVELS + 1 + k] = b_sum
        if k:
            f = (f1, f2)[k - 1]
            for field in range(2):
                f[field, h + 2 :, :] = jnp.zeros((f.shape[1] - h - 2, f.shape[2]), f32)
    for k in range(3, LEVELS + 1):
        acc_ref[k] = jnp.zeros((8, 128), f32)
        acc_ref[LEVELS + 1 + k] = jnp.zeros((8, 128), f32)


def edge_kernel(sizes, mid, z0, z1, z2, r1_ref, r2_ref, r3_ref, acc_ref, s0_in, b0_in, f1_in, f2_in,
                s0_ref, b0_ref, f1, f2, f3, f4, sum_ref, up, lo, t0, e0, t1, e1, w2, w3, w4, tmp):
    me = lax.axis_index("rows")
    odd = lax.rem(me, 2) == 1
    first, last = me == 0, me == lax.axis_size("rows") - 1
    r1, r2 = r1_ref[...], r2_ref[...]
    if mid:
        r2 = jnp.where((me == mid) | (me == mid - 1), r3_ref[...], r2)
    up[...] = jnp.where(odd, r1, r2)
    lo[...] = jnp.where(odd, r2, r1)
    pick = picker()

    h0, width0 = sizes[0]
    for c in range(z0.shape[0]):
        t0[c, 8:16, :] = z0[c, 0:8, :]
        t0[c, 4:8, :] = jnp.where(first, jnp.broadcast_to(z0[c, 0:1, :], (4, 128)), up[4 * c : 4 * c + 4, :])
        e0[c, 8:16, :] = z0[c, h0 - 8 : h0, :]
        e0[c, 16:20, :] = jnp.where(last, jnp.broadcast_to(z0[c, h0 - 1 : h0, :], (4, 128)), lo[4 * c : 4 * c + 4, :])
    base = 4 * z0.shape[0]
    h1, width1 = sizes[1]
    tmp[0:3, :] = rows_sum(t0, 4, 3)
    tmp[3:5, :] = rows_sum(e0, 12, 2)
    edge = cols_coarsen(tmp[...], width0, pick)
    for c in range(z1.shape[0]):
        part = edge[:, 128 * c : 128 * c + 128]
        row0, end = part[1:2], part[3:4]
        t1[c, 8:16, :] = z1[c, 0:8, :]
        t1[c, 8:9, :] = row0
        t1[c, 7:8, :] = jnp.where(first, row0, part[0:1])
        t1[c, 4:7, :] = jnp.where(first, jnp.broadcast_to(row0, (3, 128)), up[base + 4 * c + 1 : base + 4 * c + 4, :])
        e1[c, 8:16, :] = z1[c, h1 - 8 : h1, :]
        e1[c, 15:16, :] = end
        e1[c, 16:17, :] = jnp.where(last, end, part[4:5])
        e1[c, 17:21, :] = jnp.where(last, jnp.broadcast_to(end, (4, 128)), lo[base + 4 * c : base + 4 * c + 4, :])
    base += 4 * z1.shape[0]
    h2, width2 = sizes[2]
    wq = up128(width1)
    tmp[0:3, :wq] = rows_sum(t1, 4, 3)
    tmp[3:6, :wq] = rows_sum(e1, 12, 3)
    edge = cols_coarsen(tmp[:, :wq], width1, pick)
    for c in range(z2.shape[0]):
        part = edge[:, 128 * c : 128 * c + 128]
        row0, end = part[1:2], part[3:4]
        at = base + h2 * c
        w2[c, 0:h2, :] = jnp.where(first, jnp.broadcast_to(row0, (h2, 128)), up[at : at + h2, :])
        w2[c, h2 : 2 * h2, :] = z2[c]
        w2[c, 2 * h2 : 3 * h2, :] = jnp.where(last, jnp.broadcast_to(end, (h2, 128)), lo[at : at + h2, :])
        w2[c, h2 - 1 : h2, :] = jnp.where(first, row0, part[0:1])
        w2[c, h2 : h2 + 2, :] = part[1:3]
        w2[c, 2 * h2 - 1 : 2 * h2, :] = end
        w2[c, 2 * h2 : 2 * h2 + 1, :] = jnp.where(last, end, part[4:5])
        w2[c, 2 * h2 + 1 : 2 * h2 + 2, :] = jnp.where(last, end, part[5:6])
    h3, width3 = sizes[3]
    wq = up128(width2)
    v = cols_coarsen(pad_rows(rows_sum(w2, h2 - 14, h3 + 11)), width2, pick)
    row = row_of(v) - 6
    v = jnp.where(first & (row < 0), v[6:7], jnp.where(last & (row >= h3), v[h3 + 5 : h3 + 6], v))
    w3[0] = v
    h4, width4 = sizes[4]
    v = cols_coarsen(pad_rows(rows_sum(w3, 0, h4 + 4)), width3, pick)
    row = row_of(v) - 2
    v = jnp.where(first & (row < 0), v[2:3], jnp.where(last & (row >= h4), v[h4 + 1 : h4 + 2], v))
    w4[0, 0:8, :] = v
    w4[0, 8:16, :] = v

    totals = []

    def add(k, slope, bend, kept):
        kept = kept & (lane_of(slope) < sizes[k][1])
        totals.append((acc_ref[k] + fold(jnp.where(kept, slope, 0.0)),
                       acc_ref[LEVELS + 1 + k] + fold(jnp.where(kept, bend * bend, 0.0))))

    def ends(top, top_at, bottom, bottom_at):
        a, b = take(top, top_at, 8), take(bottom, bottom_at - 4, 8)
        return jnp.where(row_of(a) < 4, a, b)

    slope, bend = relief(*(ends(t0, 7 + i, e0, 11 + i) for i in range(3)), width0, 1.0)
    for ref, v in ((s0_ref, slope), (b0_ref, bend)):
        ref[0:4, :] = v[0:4]
        ref[h0 - 4 : h0, :] = v[4:8]
    add(0, slope, bend, (row_of(slope) == 0) | (row_of(slope) == 7))
    for k, top, bottom, top_at, bottom_at, f in ((1, t1, e1, 7, 13, f1), (2, w2, w2, h2 - 1, 2 * h2 - 3, f2)):
        h, width = sizes[k]
        slope, bend = relief(*(ends(top, top_at - 1 + i, bottom, bottom_at - 1 + i) for i in range(3)), width, float(2**k))
        add(k, slope, bend, (row_of(slope) > 0) & (row_of(slope) < 7))
        for field, v in enumerate((slope, bend)):
            row = row_of(v)
            v = jnp.where(first & (row == 0), v[1:2], jnp.where(last & (row == 7), v[6:7], v))
            f[field, 0:4, :] = v[0:4]
            f[field, h - 2 : h + 2, :] = v[4:8]
    for k, z, at, f in ((3, w3, 5, f3), (4, w4, 1, f4)):
        h, width = sizes[k]
        rows = -(-(h + 2) // 8) * 8
        slope, bend = relief(take(z, at - 1, rows), take(z, at, rows), take(z, at + 1, rows), width, float(2**k))
        row = row_of(slope) - 1
        add(k, slope, bend, (row >= 0) & (row < h))
        for field, v in enumerate((slope, bend)):
            v = jnp.where(first & (row < 0), v[1:2], jnp.where(last & (row >= h), v[h : h + 1], v))
            f[field, 0:rows, :] = jnp.where(row <= h, v, 0.0)
            if rows < f.shape[1]:
                f[field, rows:, :] = jnp.zeros((f.shape[1] - rows, f.shape[2]), f32)
    table = jnp.zeros((16, 128), f32)
    table_row = row_of(table)
    for i, v in enumerate([t[0] for t in totals] + [t[1] for t in totals]):
        table = jnp.where(table_row == i, jnp.sum(v, axis=0, keepdims=True), table)
    table = jnp.where(table_row == lane_of(table), jnp.sum(table, axis=1, keepdims=True), 0.0)
    line = jnp.sum(table, axis=0, keepdims=True)
    sum_ref[...] = jnp.broadcast_to(line.reshape(1, 1, 128), sum_ref.shape)


def pad_rows(v):
    short = -v.shape[0] % 8
    return jnp.concatenate([v, jnp.zeros((short, v.shape[1]), f32)], axis=0) if short else v


def hat(shape, factor, count, shift, along):
    fine = lax.broadcasted_iota(jnp.int32, shape, along).astype(f32)
    coarse = lax.broadcasted_iota(jnp.int32, shape, 1 - along).astype(f32)
    y = (fine + 0.5) * (1.0 / factor) - 0.5
    if count is not None:
        y = jnp.clip(y, 0.0, count - 1.0)
    return jnp.maximum(0.0, 1.0 - jnp.abs(y + shift - coarse)).astype(bf16)


def spread_kernel(sizes, f1, f2, f3, f4, u1, u2, u3, u4):
    h0, width0 = sizes[0]
    for k, f, u in zip(range(1, LEVELS + 1), (f1, f2, f3, f4), (u1, u2, u3, u4)):
        rows, wp = f.shape[1], f.shape[2]
        across = hat((wp, width0), 2**k, sizes[k][1], 0.0, 1)
        down = hat((h0, rows), 2**k, None, 1.0, 0)
        for field in range(2):
            hi, low = split2(f[field])
            wide = mm(hi, across) + mm(low, across)
            hi, low = split2(wide)
            u[field] = mm(down, hi) + mm(down, low)


def blend_kernel(cells, v_ref, s0, b0, u1, u2, u3, u4, slope_ref, bend_ref, slope_buf, bend_buf, sems):
    sums = jnp.sum(v_ref[...], axis=0)
    lane = lax.broadcasted_iota(jnp.int32, (1, 128), 1)
    count = jnp.ones((1, 128), f32)
    for k, c in enumerate(cells):
        count = jnp.where((lane == k) | (lane == k + LEVELS + 1), float(c), count)
    mean = sums / count
    scale = jnp.where(lane <= LEVELS, 1.0 / (mean + EPS), 1.0 / jnp.sqrt(mean + EPS))
    rows = slope_buf.shape[0]
    copies = []
    for field, (base, buf, out) in enumerate(((s0, slope_buf, slope_ref), (b0, bend_buf, bend_ref))):
        factors = [jnp.broadcast_to(scale[:, i : i + 1], (8, 128)) for i in range(field * (LEVELS + 1), (field + 1) * (LEVELS + 1))]
        for half in range(2):
            for at in range(half * rows // 2, (half + 1) * rows // 2, 8):
                for c in range(0, buf.shape[1], 128):
                    total = base[at : at + 8, c : c + 128] * factors[0]
                    for factor, u in zip(factors[1:], (u1, u2, u3, u4)):
                        total = total + u[field, at : at + 8, c : c + 128] * factor
                    buf[at : at + 8, c : c + 128] = total
            part = pl.ds(half * rows // 2, rows // 2)
            copy = pltpu.make_async_copy(buf.at[part], out.at[part], sems.at[2 * field + half])
            copy.start()
            copies.append(copy)
    for copy in copies:
        copy.wait()


def halo_pairs(count):
    both = lambda pairs: [(a, b) for a, b in pairs] + [(b, a) for a, b in pairs]
    even = [(i, i + 1) for i in range(0, count - 1, 2)]
    odd = [(i, i + 1) for i in range(1, count - 1, 2)]
    if count % 4 or count < 8:
        return both(even), both(odd), None, 0
    mid = count // 2
    second = [e for e in odd if e[0] != mid - 1] + [(0, mid), (mid - 1, count - 1)]
    third = [e for e in even if e[0] not in (mid - 2, mid)] + [(mid - 1, mid), (mid - 2, mid + 1)]
    return both(even), both(second), both(third), mid


VM = pl.BlockSpec(memory_space=pltpu.VMEM)
ANY = pl.BlockSpec(memory_space=pl.ANY)


def call(kernel, name, outs, scratch=(), in_specs=None, out_specs=None, flops=10**6, limit=8 << 20, aliases=None):
    return lambda *args: pl.pallas_call(
        kernel,
        name=name,
        out_shape=[jax.ShapeDtypeStruct(s, f32) for s in outs],
        in_specs=in_specs or [VM] * len(args),
        out_specs=out_specs or [VM] * len(outs),
        scratch_shapes=list(scratch),
        input_output_aliases=aliases or {},
        compiler_params=pltpu.CompilerParams(vmem_limit_bytes=limit),
        cost_estimate=pl.CostEstimate(flops=flops, bytes_accessed=1 << 19, transcendentals=0),
    )(*args)


def local(grid):
    h0, width0 = grid.shape
    count = lax.axis_size("rows")
    sizes = [(h0 >> k, width0 >> k) for k in range(LEVELS + 1)]

    def blocks(rows, width):
        return (up128(width) // 128, -(-rows // 8) * 8, 128)

    z_shapes = [blocks(*size) for size in sizes]
    msg = (4 * z_shapes[0][0] + 4 * z_shapes[1][0] + sizes[2][0] * z_shapes[2][0], 128)
    m1, m2, z0, z1, z2 = call(
        functools.partial(pyramid_kernel, sizes),
        "pyramid",
        [msg, msg] + z_shapes[:3],
        [pltpu.VMEM((h0 // 2, width0), f32), pltpu.SemaphoreType.DMA((z_shapes[0][0],))],
        in_specs=[pl.BlockSpec(memory_space=pltpu.HBM)],
    )(pltpu.with_memory_space_constraint(grid, pltpu.HBM))
    pairs1, pairs2, pairs3, mid = halo_pairs(count)
    r2 = lax.ppermute(m2, "rows", pairs2)
    r3 = lax.ppermute(m2, "rows", pairs3) if mid else m2
    r1 = lax.ppermute(m1, "rows", pairs1)
    f_shapes = [(2, up16(h + 2), up128(w)) for h, w in sizes[1:]]
    acc = (2 * LEVELS + 2, 8, 128)
    s0, b0, f1, f2, sums = call(
        functools.partial(inner_kernel, sizes),
        "inner",
        [grid.shape, grid.shape] + f_shapes[:2] + [acc],
        flops=10**8,
    )(z0, z1, z2)
    s0, b0, f1, f2, f3, f4, sums = call(
        functools.partial(edge_kernel, sizes, mid),
        "edge",
        [grid.shape, grid.shape] + f_shapes + [(count, 1, 128)],
        [pltpu.VMEM(msg, f32)] * 2
        + [pltpu.VMEM(blocks(rows, sizes[k][1]), f32) for k in range(2) for rows in (24, 24)]
        + [pltpu.VMEM(blocks(3 * sizes[2][0], sizes[2][1]), f32)]
        + [pltpu.VMEM(blocks(sizes[3][0] + 16, sizes[3][1]), f32)]
        + [pltpu.VMEM(blocks(16, sizes[4][1]), f32), pltpu.VMEM((8, width0), f32)],
        aliases={7: 0, 8: 1, 9: 2, 10: 3},
    )(z0, z1, z2, r1, r2, r3, sums, s0, b0, f1, f2)
    sums = pltpu.with_memory_space_constraint(sums, pltpu.VMEM)
    seen = lax.all_to_all(sums, "rows", 0, 0, tiled=True)
    us = call(
        functools.partial(spread_kernel, sizes),
        "spread",
        [(2, h0, width0)] * LEVELS,
        flops=10**9,
        limit=16 << 20,
    )(f1, f2, f3, f4)
    cells = [count * h * w for h, w in sizes]
    return tuple(
        call(
            functools.partial(blend_kernel, cells),
            "blend",
            [grid.shape, grid.shape],
            [pltpu.VMEM(grid.shape, f32)] * 2 + [pltpu.SemaphoreType.DMA((4,))],
            out_specs=[ANY, ANY],
        )(seen, s0, b0, *us)
    )


def solution(mesh):
    return jax.shard_map(
        local,
        mesh=mesh,
        in_specs=(P("rows", None),),
        out_specs=(P("rows", None), P("rows", None)),
        check_vma=False,
    )
```

```python
import functools

import jax
import jax.numpy as jnp
from jax import lax
from jax.experimental import pallas as pl
from jax.experimental.pallas import tpu as pltpu
from jax.sharding import PartitionSpec as P

LEVELS = 4
EPS = 1e-06
f32 = jnp.float32
bf16 = jnp.bfloat16
ATAN = (
    1.0,
    -0.3333314528,
    0.1999355085,
    -0.1420889944,
    0.1065626393,
    -0.0752896400,
    0.0429096138,
    -0.0161657367,
    0.0028662257,
)


def up128(n):
    return -(-n // 128) * 128


def up16(n):
    return -(-n // 16) * 16


def lane_of(v):
    return lax.broadcasted_iota(jnp.int32, v.shape, 1)


def row_of(v):
    return lax.broadcasted_iota(jnp.int32, v.shape, 0)


def west(v):
    return jnp.where(lane_of(v) == 0, v, pltpu.roll(v, 1, 1))


def east(v, width):
    return jnp.where(lane_of(v) == width - 1, v, pltpu.roll(v, v.shape[1] - 1, 1))


def split2(v):
    hi = v.astype(bf16)
    return hi, (v - hi.astype(f32)).astype(bf16)


def mm(a, b):
    return jnp.dot(a, b, preferred_element_type=f32)


def take(ref, at, count):
    return jnp.concatenate([ref[c, at : at + count, :] for c in range(ref.shape[0])], axis=1)


def store(ref, at, v):
    for c in range(ref.shape[0]):
        ref[c, at : at + v.shape[0], :] = v[:, 128 * c : 128 * c + 128]


def rows_sum(ref, start, count):
    out = []
    for c in range(ref.shape[0]):
        part = [ref[c, pl.ds(start + a, count, 2), :] for a in range(5)]
        out.append((part[0] + part[4]) * 0.0625 + (part[1] + part[3]) * 0.25 + part[2] * 0.375)
    return jnp.concatenate(out, axis=1)


def every_second(blocks):
    shape = blocks[0].shape
    lane = lax.broadcasted_iota(jnp.int32, shape, 1)
    at = lax.rem(2 * lane, 128)
    out = ([], [])
    for i in range(0, len(blocks), 2):
        for side in range(2):
            part = jnp.take_along_axis(blocks[i], at + side, axis=1, mode="promise_in_bounds")
            if i + 1 < len(blocks):
                other = jnp.take_along_axis(blocks[i + 1], at + side, axis=1, mode="promise_in_bounds")
                part = jnp.where(lane < 64, part, other)
            out[side].append(part)
    return [jnp.concatenate(v, axis=1) for v in out]


def cols_coarsen(v, width):
    even, odd = every_second([v[:, at : at + 128] for at in range(0, v.shape[1], 128)])
    lane = lane_of(even)
    even_w = jnp.where(lane == 0, even, pltpu.roll(even, 1, 1))
    odd_w = jnp.where(lane == 0, even, pltpu.roll(odd, 1, 1))
    even_e = jnp.where(lane == width // 2 - 1, odd, pltpu.roll(even, even.shape[1] - 1, 1))
    return (even_w + even_e) * 0.0625 + (odd_w + odd) * 0.25 + even * 0.375


def pyramid_kernel(sizes, x_ref, m1_ref, m2_ref, z0, z1, z2, tmp, sems):
    copies = [
        pltpu.make_async_copy(x_ref.at[:, pl.ds(128 * c, 128)], z0.at[c], sems.at[c]) for c in range(z0.shape[0])
    ]
    for copy in copies:
        copy.start()
    odd = lax.rem(lax.axis_index("rows"), 2) == 1
    h = sizes[0][0]
    for copy in copies:
        copy.wait()

    def put(row, z, top_at, bottom_at, count):
        for c in range(z.shape[0]):
            top, bottom = z[c, top_at : top_at + count, :], z[c, bottom_at : bottom_at + count, :]
            m1_ref[row : row + count, :] = jnp.where(odd, top, bottom)
            m2_ref[row : row + count, :] = jnp.where(odd, bottom, top)
            row += count
        return row

    row = put(0, z0, 0, h - 4, 4)
    for k, z in ((0, z1), (1, z2)):
        half, wp = sizes[k + 1][0], up128(sizes[k][1])
        low = k + 1
        tmp[low : half - 1, :wp] = rows_sum((z0, z1)[k], 2 * low - 2, half - 1 - low)
        store(z, 0, cols_coarsen(tmp[0:half, :wp], sizes[k][1]))
    row = put(row, z1, 1, sizes[1][0] - 5, 4)
    put(row, z2, 0, 0, sizes[2][0])


def relief(upper, middle, lower, width, spacing):
    diff = lower - upper
    ends = lower + upper
    tall = ends + 2.0 * middle
    m_e, m_w = east(middle, width), west(middle)
    d_e, d_w = east(diff, width), west(diff)
    p = (east(tall, width) - west(tall)) * (1.0 / (8.0 * spacing))
    q = (d_e + d_w + 2.0 * diff) * (1.0 / (8.0 * spacing))
    inv = 1.0 / (spacing * spacing)
    r = ((m_e - middle) - (middle - m_w)) * inv
    t = ((lower - middle) - (middle - upper)) * inv
    u = (d_e - d_w) * (0.25 * inv)
    pp, qq = p * p, q * q
    steep = pp + qq
    base = 1.0 + steep
    root = jnp.sqrt(base)
    y = jnp.sqrt(steep) / (1.0 + root)
    y2 = y * y
    acc = ATAN[-1]
    for c in ATAN[-2::-1]:
        acc = acc * y2 + c
    slope = 2.0 * y * acc
    bend = -(pp * r + 2.0 * (p * q) * u + qq * t) / (base * root)
    return slope, bend


def fold(v):
    total = None
    for row in range(0, v.shape[0], 8):
        for at in range(0, v.shape[1], 128):
            part = v[row : row + 8, at : at + 128]
            total = part if total is None else total + part
    return total


def inner_kernel(sizes, z0, z1, z2, s0_ref, b0_ref, f1, f2, acc_ref):
    for k, z in enumerate((z0, z1, z2)):
        h, width = sizes[k]
        s_sum = b_sum = None
        for at in range(0, h, 8):
            middle = take(z, at, 8)
            upper = take(z, at - 1, 8) if at else pltpu.roll(middle, 1, 0)
            lower = take(z, at + 1, 8) if at < h - 8 else pltpu.roll(middle, 7, 0)
            slope, bend = relief(upper, middle, lower, width, float(2**k))
            if k == 0:
                s0_ref[at : at + 8, :] = slope
                b0_ref[at : at + 8, :] = bend
            else:
                f = (f1, f2)[k - 1]
                f[0, at + 1 : at + 9, :] = slope
                f[1, at + 1 : at + 9, :] = bend
            skip = 3 if k else 1
            if at == 0 or at == h - 8 or width % 128:
                row = row_of(slope) + at
                kept = (row >= skip) & (row < h - skip) & (lane_of(slope) < width)
                slope, bend = jnp.where(kept, slope, 0.0), jnp.where(kept, bend, 0.0)
            fs, fb = fold(slope), fold(bend * bend)
            s_sum = fs if at == 0 else s_sum + fs
            b_sum = fb if at == 0 else b_sum + fb
        acc_ref[k] = s_sum
        acc_ref[LEVELS + 1 + k] = b_sum
        if k:
            f = (f1, f2)[k - 1]
            for field in range(2):
                f[field, h + 2 :, :] = jnp.zeros((f.shape[1] - h - 2, f.shape[2]), f32)
    for k in range(3, LEVELS + 1):
        acc_ref[k] = jnp.zeros((8, 128), f32)
        acc_ref[LEVELS + 1 + k] = jnp.zeros((8, 128), f32)


def edge_kernel(sizes, mid, z0, z1, z2, r1_ref, r2_ref, r3_ref, acc_ref, s0_in, b0_in, f1_in, f2_in,
                s0_ref, b0_ref, f1, f2, f3, f4, sum_ref, up, lo, t0, e0, t1, e1, w2, w3, w4, tmp):
    me = lax.axis_index("rows")
    odd = lax.rem(me, 2) == 1
    first, last = me == 0, me == lax.axis_size("rows") - 1
    r1, r2 = r1_ref[...], r2_ref[...]
    if mid:
        r2 = jnp.where((me == mid) | (me == mid - 1), r3_ref[...], r2)
    up[...] = jnp.where(odd, r1, r2)
    lo[...] = jnp.where(odd, r2, r1)

    h0, width0 = sizes[0]
    for c in range(z0.shape[0]):
        t0[c, 8:16, :] = z0[c, 0:8, :]
        t0[c, 4:8, :] = jnp.where(first, jnp.broadcast_to(z0[c, 0:1, :], (4, 128)), up[4 * c : 4 * c + 4, :])
        e0[c, 8:16, :] = z0[c, h0 - 8 : h0, :]
        e0[c, 16:20, :] = jnp.where(last, jnp.broadcast_to(z0[c, h0 - 1 : h0, :], (4, 128)), lo[4 * c : 4 * c + 4, :])
    base = 4 * z0.shape[0]
    h1, width1 = sizes[1]
    tmp[0:3, :] = rows_sum(t0, 4, 3)
    tmp[3:5, :] = rows_sum(e0, 12, 2)
    edge = cols_coarsen(tmp[...], width0)
    for c in range(z1.shape[0]):
        part = edge[:, 128 * c : 128 * c + 128]
        row0, end = part[1:2], part[3:4]
        t1[c, 8:16, :] = z1[c, 0:8, :]
        t1[c, 8:9, :] = row0
        t1[c, 7:8, :] = jnp.where(first, row0, part[0:1])
        t1[c, 4:7, :] = jnp.where(first, jnp.broadcast_to(row0, (3, 128)), up[base + 4 * c + 1 : base + 4 * c + 4, :])
        e1[c, 8:16, :] = z1[c, h1 - 8 : h1, :]
        e1[c, 15:16, :] = end
        e1[c, 16:17, :] = jnp.where(last, end, part[4:5])
        e1[c, 17:21, :] = jnp.where(last, jnp.broadcast_to(end, (4, 128)), lo[base + 4 * c : base + 4 * c + 4, :])
    base += 4 * z1.shape[0]
    h2, width2 = sizes[2]
    wq = up128(width1)
    tmp[0:3, :wq] = rows_sum(t1, 4, 3)
    tmp[3:6, :wq] = rows_sum(e1, 12, 3)
    edge = cols_coarsen(tmp[:, :wq], width1)
    for c in range(z2.shape[0]):
        part = edge[:, 128 * c : 128 * c + 128]
        row0, end = part[1:2], part[3:4]
        at = base + h2 * c
        w2[c, 0:h2, :] = jnp.where(first, jnp.broadcast_to(row0, (h2, 128)), up[at : at + h2, :])
        w2[c, h2 : 2 * h2, :] = z2[c]
        w2[c, 2 * h2 : 3 * h2, :] = jnp.where(last, jnp.broadcast_to(end, (h2, 128)), lo[at : at + h2, :])
        w2[c, h2 - 1 : h2, :] = jnp.where(first, row0, part[0:1])
        w2[c, h2 : h2 + 2, :] = part[1:3]
        w2[c, 2 * h2 - 1 : 2 * h2, :] = end
        w2[c, 2 * h2 : 2 * h2 + 1, :] = jnp.where(last, end, part[4:5])
        w2[c, 2 * h2 + 1 : 2 * h2 + 2, :] = jnp.where(last, end, part[5:6])
    h3, width3 = sizes[3]
    wq = up128(width2)
    v = cols_coarsen(pad_rows(rows_sum(w2, h2 - 14, h3 + 11)), width2)
    row = row_of(v) - 6
    v = jnp.where(first & (row < 0), v[6:7], jnp.where(last & (row >= h3), v[h3 + 5 : h3 + 6], v))
    w3[0] = v
    h4, _ = sizes[4]
    v = cols_coarsen(pad_rows(rows_sum(w3, 0, h4 + 4)), width3)
    row = row_of(v) - 2
    v = jnp.where(first & (row < 0), v[2:3], jnp.where(last & (row >= h4), v[h4 + 1 : h4 + 2], v))
    w4[0, 0:8, :] = v
    w4[0, 8:16, :] = v

    totals = []

    def add(k, slope, bend, kept):
        kept = kept & (lane_of(slope) < sizes[k][1])
        totals.append((acc_ref[k] + fold(jnp.where(kept, slope, 0.0)),
                       acc_ref[LEVELS + 1 + k] + fold(jnp.where(kept, bend * bend, 0.0))))

    def ends(top, top_at, bottom, bottom_at):
        a, b = take(top, top_at, 8), take(bottom, bottom_at - 4, 8)
        return jnp.where(row_of(a) < 4, a, b)

    slope, bend = relief(*(ends(t0, 7 + i, e0, 11 + i) for i in range(3)), width0, 1.0)
    for ref, v in ((s0_ref, slope), (b0_ref, bend)):
        ref[0:4, :] = v[0:4]
        ref[h0 - 4 : h0, :] = v[4:8]
    add(0, slope, bend, (row_of(slope) == 0) | (row_of(slope) == 7))
    for k, top, bottom, top_at, bottom_at, f in ((1, t1, e1, 7, 13, f1), (2, w2, w2, h2 - 1, 2 * h2 - 3, f2)):
        h, width = sizes[k]
        slope, bend = relief(*(ends(top, top_at - 1 + i, bottom, bottom_at - 1 + i) for i in range(3)), width, float(2**k))
        add(k, slope, bend, (row_of(slope) > 0) & (row_of(slope) < 7))
        for field, v in enumerate((slope, bend)):
            row = row_of(v)
            v = jnp.where(first & (row == 0), v[1:2], jnp.where(last & (row == 7), v[6:7], v))
            f[field, 0:4, :] = v[0:4]
            f[field, h - 2 : h + 2, :] = v[4:8]
    for k, z, at, f in ((3, w3, 5, f3), (4, w4, 1, f4)):
        h, width = sizes[k]
        rows = -(-(h + 2) // 8) * 8
        slope, bend = relief(take(z, at - 1, rows), take(z, at, rows), take(z, at + 1, rows), width, float(2**k))
        row = row_of(slope) - 1
        add(k, slope, bend, (row >= 0) & (row < h))
        for field, v in enumerate((slope, bend)):
            v = jnp.where(first & (row < 0), v[1:2], jnp.where(last & (row >= h), v[h : h + 1], v))
            f[field, 0:rows, :] = jnp.where(row <= h, v, 0.0)
            if rows < f.shape[1]:
                f[field, rows:, :] = jnp.zeros((f.shape[1] - rows, f.shape[2]), f32)
    table = jnp.zeros((16, 128), f32)
    table_row = row_of(table)
    for i, v in enumerate([t[0] for t in totals] + [t[1] for t in totals]):
        table = jnp.where(table_row == i, jnp.sum(v, axis=0, keepdims=True), table)
    table = jnp.where(table_row == lane_of(table), jnp.sum(table, axis=1, keepdims=True), 0.0)
    line = jnp.sum(table, axis=0, keepdims=True)
    sum_ref[...] = jnp.broadcast_to(line.reshape(1, 1, 128), sum_ref.shape)


def pad_rows(v):
    short = -v.shape[0] % 8
    return jnp.concatenate([v, jnp.zeros((short, v.shape[1]), f32)], axis=0) if short else v


def hat(shape, factor, count, shift, along):
    fine = lax.broadcasted_iota(jnp.int32, shape, along).astype(f32)
    coarse = lax.broadcasted_iota(jnp.int32, shape, 1 - along).astype(f32)
    y = (fine + 0.5) * (1.0 / factor) - 0.5
    if count is not None:
        y = jnp.clip(y, 0.0, count - 1.0)
    return jnp.maximum(0.0, 1.0 - jnp.abs(y + shift - coarse)).astype(bf16)


def spread_kernel(sizes, f1, f2, f3, f4, u1, u2, u3, u4):
    h0, width0 = sizes[0]
    for k, f, u in zip(range(1, LEVELS + 1), (f1, f2, f3, f4), (u1, u2, u3, u4)):
        rows, wp = f.shape[1], f.shape[2]
        across = hat((wp, width0), 2**k, sizes[k][1], 0.0, 1)
        down = hat((h0, rows), 2**k, None, 1.0, 0)
        for field in range(2):
            hi, low = split2(f[field])
            wide = mm(hi, across) + mm(low, across)
            hi, low = split2(wide)
            u[field] = mm(down, hi) + mm(down, low)


def blend_kernel(cells, v_ref, s0, b0, u1, u2, u3, u4, slope_ref, bend_ref, slope_buf, bend_buf, sems):
    sums = jnp.sum(v_ref[...], axis=0)
    lane = lax.broadcasted_iota(jnp.int32, (1, 128), 1)
    count = jnp.ones((1, 128), f32)
    for k, c in enumerate(cells):
        count = jnp.where((lane == k) | (lane == k + LEVELS + 1), float(c), count)
    mean = sums / count
    scale = jnp.where(lane <= LEVELS, 1.0 / (mean + EPS), 1.0 / jnp.sqrt(mean + EPS))
    rows = slope_buf.shape[0]
    copies = []
    for field, (base, buf, out) in enumerate(((s0, slope_buf, slope_ref), (b0, bend_buf, bend_ref))):
        factors = [jnp.broadcast_to(scale[:, i : i + 1], (8, 128)) for i in range(field * (LEVELS + 1), (field + 1) * (LEVELS + 1))]
        for half in range(2):
            for at in range(half * rows // 2, (half + 1) * rows // 2, 8):
                for c in range(0, buf.shape[1], 128):
                    total = base[at : at + 8, c : c + 128] * factors[0]
                    for factor, u in zip(factors[1:], (u1, u2, u3, u4)):
                        total = total + u[field, at : at + 8, c : c + 128] * factor
                    buf[at : at + 8, c : c + 128] = total
            part = pl.ds(half * rows // 2, rows // 2)
            copy = pltpu.make_async_copy(buf.at[part], out.at[part], sems.at[2 * field + half])
            copy.start()
            copies.append(copy)
    for copy in copies:
        copy.wait()


def halo_pairs(count):
    both = lambda pairs: [(a, b) for a, b in pairs] + [(b, a) for a, b in pairs]
    even = [(i, i + 1) for i in range(0, count - 1, 2)]
    odd = [(i, i + 1) for i in range(1, count - 1, 2)]
    if count % 2 or count < 8:
        return both(even), both(odd), None, 0
    mid = (2 * count // 3 | 1) + 1
    second = [e for e in odd if e[1] != mid] + [(0, mid - 1), (mid, count - 1)]
    third = [e for e in even if e[0] not in (mid - 2, mid)] + [(mid - 1, mid), (mid - 2, mid + 1)]
    return both(even), both(second), both(third), mid


VM = pl.BlockSpec(memory_space=pltpu.VMEM)
ANY = pl.BlockSpec(memory_space=pl.ANY)


def call(kernel, outs, scratch=(), in_specs=None, out_specs=None, flops=10**6, limit=8 << 20, aliases=None):
    return lambda *args: pl.pallas_call(
        kernel,
        out_shape=[jax.ShapeDtypeStruct(s, f32) for s in outs],
        in_specs=in_specs or [VM] * len(args),
        out_specs=out_specs or [VM] * len(outs),
        scratch_shapes=list(scratch),
        input_output_aliases=aliases or {},
        compiler_params=pltpu.CompilerParams(vmem_limit_bytes=limit),
        cost_estimate=pl.CostEstimate(flops=flops, bytes_accessed=1 << 19, transcendentals=0),
    )(*args)


def local(grid):
    h0, width0 = grid.shape
    count = lax.axis_size("rows")
    sizes = [(h0 >> k, width0 >> k) for k in range(LEVELS + 1)]

    def blocks(rows, width):
        return (up128(width) // 128, -(-rows // 8) * 8, 128)

    z_shapes = [blocks(*size) for size in sizes]
    msg = (4 * z_shapes[0][0] + 4 * z_shapes[1][0] + sizes[2][0] * z_shapes[2][0], 128)
    m1, m2, z0, z1, z2 = call(
        functools.partial(pyramid_kernel, sizes),
        [msg, msg] + z_shapes[:3],
        [pltpu.VMEM((h0 // 2, width0), f32), pltpu.SemaphoreType.DMA((z_shapes[0][0],))],
        in_specs=[pl.BlockSpec(memory_space=pltpu.HBM)],
    )(pltpu.with_memory_space_constraint(grid, pltpu.HBM))
    pairs1, pairs2, pairs3, mid = halo_pairs(count)
    r2 = lax.ppermute(m2, "rows", pairs2)
    r1 = lax.ppermute(m1, "rows", pairs1)
    r3 = lax.ppermute(m2, "rows", pairs3) if mid else m2
    f_shapes = [(2, up16(h + 2), up128(w)) for h, w in sizes[1:]]
    acc = (2 * LEVELS + 2, 8, 128)
    s0, b0, f1, f2, sums = call(
        functools.partial(inner_kernel, sizes), [grid.shape, grid.shape] + f_shapes[:2] + [acc], flops=10**8
    )(z0, z1, z2)
    s0, b0, f1, f2, f3, f4, sums = call(
        functools.partial(edge_kernel, sizes, mid),
        [grid.shape, grid.shape] + f_shapes + [(count, 1, 128)],
        [pltpu.VMEM(msg, f32)] * 2
        + [pltpu.VMEM(blocks(rows, sizes[k][1]), f32) for k in range(2) for rows in (24, 24)]
        + [pltpu.VMEM(blocks(3 * sizes[2][0], sizes[2][1]), f32)]
        + [pltpu.VMEM(blocks(sizes[3][0] + 16, sizes[3][1]), f32)]
        + [pltpu.VMEM(blocks(16, sizes[4][1]), f32), pltpu.VMEM((8, width0), f32)],
        aliases={7: 0, 8: 1, 9: 2, 10: 3},
    )(z0, z1, z2, r1, r2, r3, sums, s0, b0, f1, f2)
    sums = pltpu.with_memory_space_constraint(sums, pltpu.VMEM)
    seen = lax.all_to_all(sums, "rows", 0, 0, tiled=True)
    us = call(
        functools.partial(spread_kernel, sizes), [(2, h0, width0)] * LEVELS, flops=10**9, limit=16 << 20
    )(f1, f2, f3, f4)
    cells = [count * h * w for h, w in sizes]
    return tuple(
        call(
            functools.partial(blend_kernel, cells),
            [grid.shape, grid.shape],
            [pltpu.VMEM(grid.shape, f32)] * 2 + [pltpu.SemaphoreType.DMA((4,))],
            out_specs=[ANY, ANY],
        )(seen, s0, b0, *us)
    )


def solution(mesh):
    return jax.shard_map(
        local,
        mesh=mesh,
        in_specs=(P("rows", None),),
        out_specs=(P("rows", None), P("rows", None)),
        check_vma=False,
    )
```

```python
import functools

import jax
import jax.numpy as jnp
from jax import lax
from jax.experimental import pallas as pl
from jax.experimental.pallas import tpu as pltpu
from jax.sharding import PartitionSpec as P

LEVELS = 4
EPS = 1e-06
f32 = jnp.float32
bf16 = jnp.bfloat16
ATAN = (
    1.0,
    -0.3333314528,
    0.1999355085,
    -0.1420889944,
    0.1065626393,
    -0.0752896400,
    0.0429096138,
    -0.0161657367,
    0.0028662257,
)


def up128(n):
    return -(-n // 128) * 128


def up16(n):
    return -(-n // 16) * 16


def lane_of(v):
    return lax.broadcasted_iota(jnp.int32, v.shape, 1)


def row_of(v):
    return lax.broadcasted_iota(jnp.int32, v.shape, 0)


def west(v):
    return jnp.where(lane_of(v) == 0, v, pltpu.roll(v, 1, 1))


def east(v, width):
    return jnp.where(lane_of(v) == width - 1, v, pltpu.roll(v, v.shape[1] - 1, 1))


def split2(v):
    hi = v.astype(bf16)
    return hi, (v - hi.astype(f32)).astype(bf16)


def mm(a, b):
    return jnp.dot(a, b, preferred_element_type=f32)


def take(ref, at, count):
    return jnp.concatenate([ref[c, at : at + count, :] for c in range(ref.shape[0])], axis=1)


def store(ref, at, v):
    for c in range(ref.shape[0]):
        ref[c, at : at + v.shape[0], :] = v[:, 128 * c : 128 * c + 128]


def rows_sum(ref, start, count):
    out = []
    for c in range(ref.shape[0]):
        part = [ref[c, pl.ds(start + a, count, 2), :] for a in range(5)]
        out.append((part[0] + part[4]) * 0.0625 + (part[1] + part[3]) * 0.25 + part[2] * 0.375)
    return jnp.concatenate(out, axis=1)


def lanes(v, at):
    return jnp.take_along_axis(v, at, axis=1, mode="promise_in_bounds")


def cols_coarsen(v, width):
    blocks = [v[:, at : at + 128] for at in range(0, v.shape[1], 128)]
    lane = lax.broadcasted_iota(jnp.int32, blocks[0].shape, 1)
    patterns = [(2 * lane + tap + 128) & 127 for tap in (-2, -1, 0, 1, 2)]
    out = []
    for c in range(0, len(blocks), 2):
        taps = []
        for tap, at in zip((-2, -1, 0, 1, 2), patterns):
            part = lanes(blocks[c], at)
            if c + 1 < len(blocks):
                part = jnp.where(2 * lane + tap < 128, part, lanes(blocks[c + 1], at))
            if tap < 0 and c:
                part = jnp.where(lane == 0, lanes(blocks[c - 1], at), part)
            if tap > 1 and c + 2 < len(blocks):
                part = jnp.where(lane == 127, lanes(blocks[c + 2], at), part)
            taps.append(part)
        if c == 0:
            taps[0] = jnp.where(lane == 0, taps[2], taps[0])
            taps[1] = jnp.where(lane == 0, taps[2], taps[1])
        taps[4] = jnp.where(lane == width // 2 - 1 - 64 * c, taps[3], taps[4])
        out.append((taps[0] + taps[4]) * 0.0625 + (taps[1] + taps[3]) * 0.25 + taps[2] * 0.375)
    return out[0] if len(out) == 1 else jnp.concatenate(out, axis=1)


def pyramid_kernel(sizes, x_ref, m1_ref, m2_ref, z0, z1, z2, tmp, sems):
    copies = [
        pltpu.make_async_copy(x_ref.at[:, pl.ds(128 * c, 128)], z0.at[c], sems.at[c]) for c in range(z0.shape[0])
    ]
    for copy in copies:
        copy.start()
    odd = lax.rem(lax.axis_index("rows"), 2) == 1
    h = sizes[0][0]
    for copy in copies:
        copy.wait()

    def put(row, z, top_at, bottom_at, count):
        for c in range(z.shape[0]):
            top, bottom = z[c, top_at : top_at + count, :], z[c, bottom_at : bottom_at + count, :]
            m1_ref[row : row + count, :] = jnp.where(odd, top, bottom)
            m2_ref[row : row + count, :] = jnp.where(odd, bottom, top)
            row += count
        return row

    row = put(0, z0, 0, h - 4, 4)
    for k, z in ((0, z1), (1, z2)):
        half, wp = sizes[k + 1][0], up128(sizes[k][1])
        low = k + 1
        tmp[low : half - 1, :wp] = rows_sum((z0, z1)[k], 2 * low - 2, half - 1 - low)
        store(z, 0, cols_coarsen(tmp[0:half, :wp], sizes[k][1]))
    row = put(row, z1, 1, sizes[1][0] - 5, 4)
    put(row, z2, 0, 0, sizes[2][0])


def relief(upper, middle, lower, width, spacing):
    diff = lower - upper
    ends = lower + upper
    tall = ends + 2.0 * middle
    m_e, m_w = east(middle, width), west(middle)
    d_e, d_w = east(diff, width), west(diff)
    p = (east(tall, width) - west(tall)) * (1.0 / (8.0 * spacing))
    q = (d_e + d_w + 2.0 * diff) * (1.0 / (8.0 * spacing))
    inv = 1.0 / (spacing * spacing)
    r = ((m_e - middle) - (middle - m_w)) * inv
    t = ((lower - middle) - (middle - upper)) * inv
    u = (d_e - d_w) * (0.25 * inv)
    pp, qq = p * p, q * q
    steep = pp + qq
    base = 1.0 + steep
    root = jnp.sqrt(base)
    y = jnp.sqrt(steep) / (1.0 + root)
    y2 = y * y
    acc = ATAN[-1]
    for c in ATAN[-2::-1]:
        acc = acc * y2 + c
    slope = 2.0 * y * acc
    bend = -(pp * r + 2.0 * (p * q) * u + qq * t) / (base * root)
    return slope, bend


def fold(v):
    total = None
    for row in range(0, v.shape[0], 8):
        for at in range(0, v.shape[1], 128):
            part = v[row : row + 8, at : at + 128]
            total = part if total is None else total + part
    return total


def inner_kernel(sizes, z0, z1, z2, s0_ref, b0_ref, f1, f2, acc_ref):
    for k, z in enumerate((z0, z1, z2)):
        h, width = sizes[k]
        s_sum = b_sum = None
        for at in range(0, h, 8):
            middle = take(z, at, 8)
            upper = take(z, at - 1, 8) if at else pltpu.roll(middle, 1, 0)
            lower = take(z, at + 1, 8) if at < h - 8 else pltpu.roll(middle, 7, 0)
            slope, bend = relief(upper, middle, lower, width, float(2**k))
            if k == 0:
                s0_ref[at : at + 8, :] = slope
                b0_ref[at : at + 8, :] = bend
            else:
                f = (f1, f2)[k - 1]
                f[0, at + 1 : at + 9, :] = slope
                f[1, at + 1 : at + 9, :] = bend
            skip = 3 if k else 1
            if at == 0 or at == h - 8 or width % 128:
                row = row_of(slope) + at
                kept = (row >= skip) & (row < h - skip) & (lane_of(slope) < width)
                slope, bend = jnp.where(kept, slope, 0.0), jnp.where(kept, bend, 0.0)
            fs, fb = fold(slope), fold(bend * bend)
            s_sum = fs if at == 0 else s_sum + fs
            b_sum = fb if at == 0 else b_sum + fb
        acc_ref[k] = s_sum
        acc_ref[LEVELS + 1 + k] = b_sum
        if k:
            f = (f1, f2)[k - 1]
            for field in range(2):
                f[field, h + 2 :, :] = jnp.zeros((f.shape[1] - h - 2, f.shape[2]), f32)
    for k in range(3, LEVELS + 1):
        acc_ref[k] = jnp.zeros((8, 128), f32)
        acc_ref[LEVELS + 1 + k] = jnp.zeros((8, 128), f32)


def edge_kernel(sizes, mid, z0, z1, z2, r1_ref, r2_ref, r3_ref, acc_ref, s0_in, b0_in, f1_in, f2_in,
                s0_ref, b0_ref, f1, f2, f3, f4, sum_ref, up, lo, t0, e0, t1, e1, w2, w3, w4, tmp):
    me = lax.axis_index("rows")
    odd = lax.rem(me, 2) == 1
    first, last = me == 0, me == lax.axis_size("rows") - 1
    r1, r2 = r1_ref[...], r2_ref[...]
    if mid:
        r2 = jnp.where((me == mid) | (me == mid - 1), r3_ref[...], r2)
    up[...] = jnp.where(odd, r1, r2)
    lo[...] = jnp.where(odd, r2, r1)

    h0, width0 = sizes[0]
    for c in range(z0.shape[0]):
        t0[c, 8:16, :] = z0[c, 0:8, :]
        t0[c, 4:8, :] = jnp.where(first, jnp.broadcast_to(z0[c, 0:1, :], (4, 128)), up[4 * c : 4 * c + 4, :])
        e0[c, 8:16, :] = z0[c, h0 - 8 : h0, :]
        e0[c, 16:20, :] = jnp.where(last, jnp.broadcast_to(z0[c, h0 - 1 : h0, :], (4, 128)), lo[4 * c : 4 * c + 4, :])
    base = 4 * z0.shape[0]
    h1, width1 = sizes[1]
    tmp[0:3, :] = rows_sum(t0, 4, 3)
    tmp[3:5, :] = rows_sum(e0, 12, 2)
    edge = cols_coarsen(tmp[...], width0)
    for c in range(z1.shape[0]):
        part = edge[:, 128 * c : 128 * c + 128]
        row0, end = part[1:2], part[3:4]
        t1[c, 8:16, :] = z1[c, 0:8, :]
        t1[c, 8:9, :] = row0
        t1[c, 7:8, :] = jnp.where(first, row0, part[0:1])
        t1[c, 4:7, :] = jnp.where(first, jnp.broadcast_to(row0, (3, 128)), up[base + 4 * c + 1 : base + 4 * c + 4, :])
        e1[c, 8:16, :] = z1[c, h1 - 8 : h1, :]
        e1[c, 15:16, :] = end
        e1[c, 16:17, :] = jnp.where(last, end, part[4:5])
        e1[c, 17:21, :] = jnp.where(last, jnp.broadcast_to(end, (4, 128)), lo[base + 4 * c : base + 4 * c + 4, :])
    base += 4 * z1.shape[0]
    h2, width2 = sizes[2]
    wq = up128(width1)
    tmp[0:3, :wq] = rows_sum(t1, 4, 3)
    tmp[3:6, :wq] = rows_sum(e1, 12, 3)
    edge = cols_coarsen(tmp[:, :wq], width1)
    for c in range(z2.shape[0]):
        part = edge[:, 128 * c : 128 * c + 128]
        row0, end = part[1:2], part[3:4]
        at = base + h2 * c
        w2[c, 0:h2, :] = jnp.where(first, jnp.broadcast_to(row0, (h2, 128)), up[at : at + h2, :])
        w2[c, h2 : 2 * h2, :] = z2[c]
        w2[c, 2 * h2 : 3 * h2, :] = jnp.where(last, jnp.broadcast_to(end, (h2, 128)), lo[at : at + h2, :])
        w2[c, h2 - 1 : h2, :] = jnp.where(first, row0, part[0:1])
        w2[c, h2 : h2 + 2, :] = part[1:3]
        w2[c, 2 * h2 - 1 : 2 * h2, :] = end
        w2[c, 2 * h2 : 2 * h2 + 1, :] = jnp.where(last, end, part[4:5])
        w2[c, 2 * h2 + 1 : 2 * h2 + 2, :] = jnp.where(last, end, part[5:6])
    h3, width3 = sizes[3]
    wq = up128(width2)
    v = cols_coarsen(pad_rows(rows_sum(w2, h2 - 14, h3 + 11)), width2)
    row = row_of(v) - 6
    v = jnp.where(first & (row < 0), v[6:7], jnp.where(last & (row >= h3), v[h3 + 5 : h3 + 6], v))
    w3[0] = v
    h4, _ = sizes[4]
    v = cols_coarsen(pad_rows(rows_sum(w3, 0, h4 + 4)), width3)
    row = row_of(v) - 2
    v = jnp.where(first & (row < 0), v[2:3], jnp.where(last & (row >= h4), v[h4 + 1 : h4 + 2], v))
    w4[0, 0:8, :] = v
    w4[0, 8:16, :] = v

    totals = []

    def add(k, slope, bend, kept):
        kept = kept & (lane_of(slope) < sizes[k][1])
        totals.append((acc_ref[k] + fold(jnp.where(kept, slope, 0.0)),
                       acc_ref[LEVELS + 1 + k] + fold(jnp.where(kept, bend * bend, 0.0))))

    def ends(top, top_at, bottom, bottom_at):
        a, b = take(top, top_at, 8), take(bottom, bottom_at - 4, 8)
        return jnp.where(row_of(a) < 4, a, b)

    slope, bend = relief(*(ends(t0, 7 + i, e0, 11 + i) for i in range(3)), width0, 1.0)
    for ref, v in ((s0_ref, slope), (b0_ref, bend)):
        ref[0:4, :] = v[0:4]
        ref[h0 - 4 : h0, :] = v[4:8]
    add(0, slope, bend, (row_of(slope) == 0) | (row_of(slope) == 7))
    for k, top, bottom, top_at, bottom_at, f in ((1, t1, e1, 7, 13, f1), (2, w2, w2, h2 - 1, 2 * h2 - 3, f2)):
        h, width = sizes[k]
        slope, bend = relief(*(ends(top, top_at - 1 + i, bottom, bottom_at - 1 + i) for i in range(3)), width, float(2**k))
        add(k, slope, bend, (row_of(slope) > 0) & (row_of(slope) < 7))
        for field, v in enumerate((slope, bend)):
            row = row_of(v)
            v = jnp.where(first & (row == 0), v[1:2], jnp.where(last & (row == 7), v[6:7], v))
            f[field, 0:4, :] = v[0:4]
            f[field, h - 2 : h + 2, :] = v[4:8]
    for k, z, at, f in ((3, w3, 5, f3), (4, w4, 1, f4)):
        h, width = sizes[k]
        rows = -(-(h + 2) // 8) * 8
        slope, bend = relief(take(z, at - 1, rows), take(z, at, rows), take(z, at + 1, rows), width, float(2**k))
        row = row_of(slope) - 1
        add(k, slope, bend, (row >= 0) & (row < h))
        for field, v in enumerate((slope, bend)):
            v = jnp.where(first & (row < 0), v[1:2], jnp.where(last & (row >= h), v[h : h + 1], v))
            f[field, 0:rows, :] = jnp.where(row <= h, v, 0.0)
            if rows < f.shape[1]:
                f[field, rows:, :] = jnp.zeros((f.shape[1] - rows, f.shape[2]), f32)
    table = jnp.zeros((8, 128), f32)
    for i, v in enumerate([t[0] for t in totals] + [t[1] for t in totals]):
        table = jnp.where(lane_of(table) == i, jnp.sum(v, axis=1, keepdims=True), table)
    line = jnp.sum(table, axis=0, keepdims=True)
    sum_ref[...] = jnp.broadcast_to(line.reshape(1, 1, 128), sum_ref.shape)


def pad_rows(v):
    short = -v.shape[0] % 8
    return jnp.concatenate([v, jnp.zeros((short, v.shape[1]), f32)], axis=0) if short else v


def hat(shape, factor, count, shift, along):
    fine = lax.broadcasted_iota(jnp.int32, shape, along).astype(f32)
    coarse = lax.broadcasted_iota(jnp.int32, shape, 1 - along).astype(f32)
    y = (fine + 0.5) * (1.0 / factor) - 0.5
    if count is not None:
        y = jnp.clip(y, 0.0, count - 1.0)
    return jnp.maximum(0.0, 1.0 - jnp.abs(y + shift - coarse)).astype(bf16)


def spread_kernel(sizes, f1, f2, f3, f4, u1, u2, u3, u4):
    h0, width0 = sizes[0]
    for k, f, u in zip(range(1, LEVELS + 1), (f1, f2, f3, f4), (u1, u2, u3, u4)):
        rows, wp = f.shape[1], f.shape[2]
        across = hat((wp, width0), 2**k, sizes[k][1], 0.0, 1)
        down = hat((h0, rows), 2**k, None, 1.0, 0)
        for field in range(2):
            hi, low = split2(f[field])
            wide = mm(hi, across) + mm(low, across)
            hi, low = split2(wide)
            u[field] = mm(down, hi) + mm(down, low)


def blend_kernel(cells, v_ref, s0, b0, u1, u2, u3, u4, slope_ref, bend_ref, slope_buf, bend_buf, sems):
    sums = jnp.sum(v_ref[...], axis=0)
    lane = lax.broadcasted_iota(jnp.int32, (1, 128), 1)
    count = jnp.ones((1, 128), f32)
    for k, c in enumerate(cells):
        count = jnp.where((lane == k) | (lane == k + LEVELS + 1), float(c), count)
    mean = sums / count
    scale = jnp.where(lane <= LEVELS, 1.0 / (mean + EPS), 1.0 / jnp.sqrt(mean + EPS))
    rows = slope_buf.shape[0]
    copies = []
    for field, (base, buf, out) in enumerate(((s0, slope_buf, slope_ref), (b0, bend_buf, bend_ref))):
        factors = [jnp.broadcast_to(scale[:, i : i + 1], (8, 128)) for i in range(field * (LEVELS + 1), (field + 1) * (LEVELS + 1))]
        for half in range(2):
            for at in range(half * rows // 2, (half + 1) * rows // 2, 8):
                for c in range(0, buf.shape[1], 128):
                    total = base[at : at + 8, c : c + 128] * factors[0]
                    for factor, u in zip(factors[1:], (u1, u2, u3, u4)):
                        total = total + u[field, at : at + 8, c : c + 128] * factor
                    buf[at : at + 8, c : c + 128] = total
            part = pl.ds(half * rows // 2, rows // 2)
            copy = pltpu.make_async_copy(buf.at[part], out.at[part], sems.at[2 * field + half])
            copy.start()
            copies.append(copy)
    for copy in copies:
        copy.wait()


def halo_pairs(count):
    both = lambda pairs: [(a, b) for a, b in pairs] + [(b, a) for a, b in pairs]
    even = [(i, i + 1) for i in range(0, count - 1, 2)]
    odd = [(i, i + 1) for i in range(1, count - 1, 2)]
    if count % 2 or count < 8:
        return both(even), both(odd), None, 0
    mid = count * 13 // 16 & ~1
    second = [e for e in odd if e[1] != mid] + [(0, mid - 1), (mid, count - 1)]
    third = [e for e in even if e[0] not in (mid - 2, mid)] + [(mid - 1, mid), (mid - 2, mid + 1)]
    return both(even), both(second), both(third), mid


VM = pl.BlockSpec(memory_space=pltpu.VMEM)
ANY = pl.BlockSpec(memory_space=pl.ANY)


def call(kernel, outs, scratch=(), in_specs=None, out_specs=None, flops=10**6, limit=8 << 20, aliases=None):
    return lambda *args: pl.pallas_call(
        kernel,
        out_shape=[jax.ShapeDtypeStruct(s, f32) for s in outs],
        in_specs=in_specs or [VM] * len(args),
        out_specs=out_specs or [VM] * len(outs),
        scratch_shapes=list(scratch),
        input_output_aliases=aliases or {},
        compiler_params=pltpu.CompilerParams(vmem_limit_bytes=limit),
        cost_estimate=pl.CostEstimate(flops=flops, bytes_accessed=1 << 19, transcendentals=0),
    )(*args)


def local(grid):
    h0, width0 = grid.shape
    count = lax.axis_size("rows")
    sizes = [(h0 >> k, width0 >> k) for k in range(LEVELS + 1)]

    def blocks(rows, width):
        return (up128(width) // 128, -(-rows // 8) * 8, 128)

    z_shapes = [blocks(*size) for size in sizes]
    msg = (4 * z_shapes[0][0] + 4 * z_shapes[1][0] + sizes[2][0] * z_shapes[2][0], 128)
    m1, m2, z0, z1, z2 = call(
        functools.partial(pyramid_kernel, sizes),
        [msg, msg] + z_shapes[:3],
        [pltpu.VMEM((h0 // 2, width0), f32), pltpu.SemaphoreType.DMA((z_shapes[0][0],))],
        in_specs=[pl.BlockSpec(memory_space=pltpu.HBM)],
    )(pltpu.with_memory_space_constraint(grid, pltpu.HBM))
    pairs1, pairs2, pairs3, mid = halo_pairs(count)
    r2 = lax.ppermute(m2, "rows", pairs2)
    r1 = lax.ppermute(m1, "rows", pairs1)
    r3 = lax.ppermute(m2, "rows", pairs3) if mid else m2
    f_shapes = [(2, up16(h + 2), up128(w)) for h, w in sizes[1:]]
    acc = (2 * LEVELS + 2, 8, 128)
    s0, b0, f1, f2, sums = call(
        functools.partial(inner_kernel, sizes), [grid.shape, grid.shape] + f_shapes[:2] + [acc], flops=10**8
    )(z0, z1, z2)
    s0, b0, f1, f2, f3, f4, sums = call(
        functools.partial(edge_kernel, sizes, mid),
        [grid.shape, grid.shape] + f_shapes + [(count, 1, 128)],
        [pltpu.VMEM(msg, f32)] * 2
        + [pltpu.VMEM(blocks(rows, sizes[k][1]), f32) for k in range(2) for rows in (24, 24)]
        + [pltpu.VMEM(blocks(3 * sizes[2][0], sizes[2][1]), f32)]
        + [pltpu.VMEM(blocks(sizes[3][0] + 16, sizes[3][1]), f32)]
        + [pltpu.VMEM(blocks(16, sizes[4][1]), f32), pltpu.VMEM((8, width0), f32)],
        aliases={7: 0, 8: 1, 9: 2, 10: 3},
    )(z0, z1, z2, r1, r2, r3, sums, s0, b0, f1, f2)
    sums = pltpu.with_memory_space_constraint(sums, pltpu.VMEM)
    seen = lax.all_to_all(sums, "rows", 0, 0, tiled=True)
    us = call(
        functools.partial(spread_kernel, sizes), [(2, h0, width0)] * LEVELS, flops=10**9, limit=16 << 20
    )(f1, f2, f3, f4)
    cells = [count * h * w for h, w in sizes]
    return tuple(
        call(
            functools.partial(blend_kernel, cells),
            [grid.shape, grid.shape],
            [pltpu.VMEM(grid.shape, f32)] * 2 + [pltpu.SemaphoreType.DMA((4,))],
            out_specs=[ANY, ANY],
        )(seen, s0, b0, *us)
    )


def solution(mesh):
    return jax.shard_map(
        local,
        mesh=mesh,
        in_specs=(P("rows", None),),
        out_specs=(P("rows", None), P("rows", None)),
        check_vma=False,
    )
```

```python
import functools

import jax
import jax.numpy as jnp
from jax import lax
from jax.experimental import pallas as pl
from jax.experimental.pallas import tpu as pltpu
from jax.sharding import PartitionSpec as P

LEVELS = 4
EPS = 1e-06
f32 = jnp.float32
ATAN = (
    1.0,
    -0.3333314528,
    0.1999355085,
    -0.1420889944,
    0.1065626393,
    -0.0752896400,
    0.0429096138,
    -0.0161657367,
    0.0028662257,
)


def up128(n):
    return -(-n // 128) * 128


def lane_of(v):
    return lax.broadcasted_iota(jnp.int32, v.shape, 1)


def row_of(v):
    return lax.broadcasted_iota(jnp.int32, v.shape, 0)


def west(v):
    return jnp.where(lane_of(v) == 0, v, pltpu.roll(v, 1, 1))


def east(v, width):
    return jnp.where(lane_of(v) == width - 1, v, pltpu.roll(v, v.shape[1] - 1, 1))


def take(ref, at, count):
    return jnp.concatenate([ref[c, at : at + count, :] for c in range(ref.shape[0])], axis=1)


def store(ref, at, v):
    for c in range(ref.shape[0]):
        ref[c, at : at + v.shape[0], :] = v[:, 128 * c : 128 * c + 128]


def rows_sum(ref, start, count):
    out = []
    for c in range(ref.shape[0]):
        part = [ref[c, pl.ds(start + a, count, 2), :] for a in range(5)]
        out.append((part[0] + part[4]) * 0.0625 + (part[1] + part[3]) * 0.25 + part[2] * 0.375)
    return jnp.concatenate(out, axis=1)


def lanes(v, at):
    return jnp.take_along_axis(v, at, axis=1, mode="promise_in_bounds")


def split(v):
    return [v[:, at : at + 128] for at in range(0, v.shape[1], 128)]


def cols_coarsen(v, width):
    blocks = split(v)
    lane = lax.broadcasted_iota(jnp.int32, blocks[0].shape, 1)
    patterns = [(2 * lane + tap + 128) & 127 for tap in (-2, -1, 0, 1, 2)]
    found = [[lanes(v, at) for v in blocks] for at in patterns]
    out = []
    for c in range(0, len(blocks), 2):
        taps = []
        for tap, got in zip((-2, -1, 0, 1, 2), found):
            part = got[c]
            if c + 1 < len(blocks):
                part = jnp.where(2 * lane + tap < 128, part, got[c + 1])
            if tap < 0 and c:
                part = jnp.where(lane == 0, got[c - 1], part)
            if tap > 1 and c + 2 < len(blocks):
                part = jnp.where(lane == 127, got[c + 2], part)
            taps.append(part)
        if c == 0:
            taps[0] = jnp.where(lane == 0, taps[2], taps[0])
            taps[1] = jnp.where(lane == 0, taps[2], taps[1])
        taps[4] = jnp.where(lane == width // 2 - 1 - 64 * c, taps[3], taps[4])
        out.append((taps[0] + taps[4]) * 0.0625 + (taps[1] + taps[3]) * 0.25 + taps[2] * 0.375)
    return out[0] if len(out) == 1 else jnp.concatenate(out, axis=1)


def pyramid_kernel(sizes, x_ref, m1_ref, m2_ref, z0, z1, z2, tmp, sems):
    copies = [
        pltpu.make_async_copy(x_ref.at[:, pl.ds(128 * c, 128)], z0.at[c], sems.at[c]) for c in range(z0.shape[0])
    ]
    for copy in copies:
        copy.start()
    odd = lax.rem(lax.axis_index("rows"), 2) == 1
    h = sizes[0][0]
    for copy in copies:
        copy.wait()

    def put(row, z, top_at, bottom_at, count):
        for c in range(z.shape[0]):
            top, bottom = z[c, top_at : top_at + count, :], z[c, bottom_at : bottom_at + count, :]
            m1_ref[row : row + count, :] = jnp.where(odd, top, bottom)
            m2_ref[row : row + count, :] = jnp.where(odd, bottom, top)
            row += count
        return row

    row = put(0, z0, 0, h - 4, 4)
    for k, z in ((0, z1), (1, z2)):
        half, wp = sizes[k + 1][0], up128(sizes[k][1])
        low = k + 1
        tmp[low : half - 1, :wp] = rows_sum((z0, z1)[k], 2 * low - 2, half - 1 - low)
        store(z, 0, cols_coarsen(tmp[0:half, :wp], sizes[k][1]))
    row = put(row, z1, 1, sizes[1][0] - 5, 4)
    put(row, z2, 0, 0, sizes[2][0])


def relief(upper, middle, lower, width, spacing):
    diff = lower - upper
    ends = lower + upper
    tall = ends + 2.0 * middle
    m_e, m_w = east(middle, width), west(middle)
    d_e, d_w = east(diff, width), west(diff)
    p = (east(tall, width) - west(tall)) * (1.0 / (8.0 * spacing))
    q = (d_e + d_w + 2.0 * diff) * (1.0 / (8.0 * spacing))
    inv = 1.0 / (spacing * spacing)
    r = ((m_e - middle) - (middle - m_w)) * inv
    t = ((lower - middle) - (middle - upper)) * inv
    u = (d_e - d_w) * (0.25 * inv)
    pp, qq = p * p, q * q
    steep = pp + qq
    base = 1.0 + steep
    root = jnp.sqrt(base)
    y = jnp.sqrt(steep) / (1.0 + root)
    y2 = y * y
    acc = ATAN[-1]
    for c in ATAN[-2::-1]:
        acc = acc * y2 + c
    slope = 2.0 * y * acc
    bend = -(pp * r + 2.0 * (p * q) * u + qq * t) / (base * root)
    return slope, bend


def fold(v):
    total = None
    for row in range(0, v.shape[0], 8):
        for at in range(0, v.shape[1], 128):
            part = v[row : row + 8, at : at + 128]
            total = part if total is None else total + part
    return total


def inner_kernel(sizes, z0, z1, z2, s0_ref, b0_ref, t1, t2, acc_ref):
    for k, z in enumerate((z0, z1, z2)):
        h, width = sizes[k]
        s_sum = b_sum = None
        for at in range(0, h, 8):
            middle = take(z, at, 8)
            upper = take(z, at - 1, 8) if at else pltpu.roll(middle, 1, 0)
            lower = take(z, at + 1, 8) if at < h - 8 else pltpu.roll(middle, 7, 0)
            slope, bend = relief(upper, middle, lower, width, float(2**k))
            if k == 0:
                s0_ref[at : at + 8, :] = slope
                b0_ref[at : at + 8, :] = bend
            else:
                t = (t1, t2)[k - 1]
                for field, v in enumerate((slope, bend)):
                    for c, part in enumerate(cols_refine(split(v), k, width, t.shape[1])):
                        t[field, c, at + 1 : at + 9, :] = part
            skip = 3 if k else 1
            if at == 0 or at == h - 8 or width % 128:
                row = row_of(slope) + at
                kept = (row >= skip) & (row < h - skip) & (lane_of(slope) < width)
                slope, bend = jnp.where(kept, slope, 0.0), jnp.where(kept, bend, 0.0)
            fs, fb = fold(slope), fold(bend * bend)
            s_sum = fs if at == 0 else s_sum + fs
            b_sum = fb if at == 0 else b_sum + fb
        acc_ref[k] = s_sum
        acc_ref[LEVELS + 1 + k] = b_sum
    for k in range(3, LEVELS + 1):
        acc_ref[k] = jnp.zeros((8, 128), f32)
        acc_ref[LEVELS + 1 + k] = jnp.zeros((8, 128), f32)


def edge_kernel(sizes, mid, z0, z1, z2, r1_ref, r2_ref, r3_ref, acc_ref, s0_in, b0_in,
                s0_ref, b0_ref, f1, f2, f3, f4, sum_ref, up, lo, t0, e0, t1, e1, w2, w3, w4, tmp):
    me = lax.axis_index("rows")
    odd = lax.rem(me, 2) == 1
    first, last = me == 0, me == lax.axis_size("rows") - 1
    r1, r2 = r1_ref[...], r2_ref[...]
    if mid:
        r2 = jnp.where((me == mid) | (me == mid - 1), r3_ref[...], r2)
    up[...] = jnp.where(odd, r1, r2)
    lo[...] = jnp.where(odd, r2, r1)

    h0, width0 = sizes[0]
    for c in range(z0.shape[0]):
        t0[c, 8:16, :] = z0[c, 0:8, :]
        t0[c, 4:8, :] = jnp.where(first, jnp.broadcast_to(z0[c, 0:1, :], (4, 128)), up[4 * c : 4 * c + 4, :])
        e0[c, 8:16, :] = z0[c, h0 - 8 : h0, :]
        e0[c, 16:20, :] = jnp.where(last, jnp.broadcast_to(z0[c, h0 - 1 : h0, :], (4, 128)), lo[4 * c : 4 * c + 4, :])
    base = 4 * z0.shape[0]
    h1, width1 = sizes[1]
    tmp[0:3, :] = rows_sum(t0, 4, 3)
    tmp[3:5, :] = rows_sum(e0, 12, 2)
    edge = cols_coarsen(tmp[...], width0)
    for c in range(z1.shape[0]):
        part = edge[:, 128 * c : 128 * c + 128]
        row0, end = part[1:2], part[3:4]
        t1[c, 8:16, :] = z1[c, 0:8, :]
        t1[c, 8:9, :] = row0
        t1[c, 7:8, :] = jnp.where(first, row0, part[0:1])
        t1[c, 4:7, :] = jnp.where(first, jnp.broadcast_to(row0, (3, 128)), up[base + 4 * c + 1 : base + 4 * c + 4, :])
        e1[c, 8:16, :] = z1[c, h1 - 8 : h1, :]
        e1[c, 15:16, :] = end
        e1[c, 16:17, :] = jnp.where(last, end, part[4:5])
        e1[c, 17:21, :] = jnp.where(last, jnp.broadcast_to(end, (4, 128)), lo[base + 4 * c : base + 4 * c + 4, :])
    base += 4 * z1.shape[0]
    h2, width2 = sizes[2]
    wq = up128(width1)
    tmp[0:3, :wq] = rows_sum(t1, 4, 3)
    tmp[3:6, :wq] = rows_sum(e1, 12, 3)
    edge = cols_coarsen(tmp[:, :wq], width1)
    for c in range(z2.shape[0]):
        part = edge[:, 128 * c : 128 * c + 128]
        row0, end = part[1:2], part[3:4]
        at = base + h2 * c
        w2[c, 0:h2, :] = jnp.where(first, jnp.broadcast_to(row0, (h2, 128)), up[at : at + h2, :])
        w2[c, h2 : 2 * h2, :] = z2[c]
        w2[c, 2 * h2 : 3 * h2, :] = jnp.where(last, jnp.broadcast_to(end, (h2, 128)), lo[at : at + h2, :])
        w2[c, h2 - 1 : h2, :] = jnp.where(first, row0, part[0:1])
        w2[c, h2 : h2 + 2, :] = part[1:3]
        w2[c, 2 * h2 - 1 : 2 * h2, :] = end
        w2[c, 2 * h2 : 2 * h2 + 1, :] = jnp.where(last, end, part[4:5])
        w2[c, 2 * h2 + 1 : 2 * h2 + 2, :] = jnp.where(last, end, part[5:6])
    h3, width3 = sizes[3]
    wq = up128(width2)
    v = cols_coarsen(pad_rows(rows_sum(w2, h2 - 14, h3 + 11)), width2)
    row = row_of(v) - 6
    v = jnp.where(first & (row < 0), v[6:7], jnp.where(last & (row >= h3), v[h3 + 5 : h3 + 6], v))
    w3[0] = v
    h4, _ = sizes[4]
    v = cols_coarsen(pad_rows(rows_sum(w3, 0, h4 + 4)), width3)
    row = row_of(v) - 2
    v = jnp.where(first & (row < 0), v[2:3], jnp.where(last & (row >= h4), v[h4 + 1 : h4 + 2], v))
    w4[0, 0:8, :] = v
    w4[0, 8:16, :] = v

    totals = []

    def add(k, slope, bend, kept):
        kept = kept & (lane_of(slope) < sizes[k][1])
        totals.append((acc_ref[k] + fold(jnp.where(kept, slope, 0.0)),
                       acc_ref[LEVELS + 1 + k] + fold(jnp.where(kept, bend * bend, 0.0))))

    def ends(top, top_at, bottom, bottom_at):
        a, b = take(top, top_at, 8), take(bottom, bottom_at - 4, 8)
        return jnp.where(row_of(a) < 4, a, b)

    slope, bend = relief(*(ends(t0, 7 + i, e0, 11 + i) for i in range(3)), width0, 1.0)
    for ref, v in ((s0_ref, slope), (b0_ref, bend)):
        ref[0:4, :] = v[0:4]
        ref[h0 - 4 : h0, :] = v[4:8]
    add(0, slope, bend, (row_of(slope) == 0) | (row_of(slope) == 7))
    for k, top, bottom, top_at, bottom_at, f in ((1, t1, e1, 7, 13, f1), (2, w2, w2, h2 - 1, 2 * h2 - 3, f2)):
        h, width = sizes[k]
        slope, bend = relief(*(ends(top, top_at - 1 + i, bottom, bottom_at - 1 + i) for i in range(3)), width, float(2**k))
        add(k, slope, bend, (row_of(slope) > 0) & (row_of(slope) < 7))
        for field, v in enumerate((slope, bend)):
            row = row_of(v)
            v = jnp.where(first & (row == 0), v[1:2], jnp.where(last & (row == 7), v[6:7], v))
            f[field] = v
    for k, z, at, f in ((3, w3, 5, f3), (4, w4, 1, f4)):
        h, width = sizes[k]
        rows = -(-(h + 2) // 8) * 8
        slope, bend = relief(take(z, at - 1, rows), take(z, at, rows), take(z, at + 1, rows), width, float(2**k))
        row = row_of(slope) - 1
        add(k, slope, bend, (row >= 0) & (row < h))
        for field, v in enumerate((slope, bend)):
            v = jnp.where(first & (row < 0), v[1:2], jnp.where(last & (row >= h), v[h : h + 1], v))
            f[field, 0:rows, :] = jnp.where(row <= h, v, 0.0)
    table = jnp.zeros((8, 128), f32)
    for i, v in enumerate([t[0] for t in totals] + [t[1] for t in totals]):
        table = jnp.where(lane_of(table) == i, jnp.sum(v, axis=1, keepdims=True), table)
    line = jnp.sum(table, axis=0, keepdims=True)
    sum_ref[...] = jnp.broadcast_to(line.reshape(1, 1, 128), sum_ref.shape)


def pad_rows(v):
    short = -v.shape[0] % 8
    return jnp.concatenate([v, jnp.zeros((short, v.shape[1]), f32)], axis=0) if short else v


def cols_refine(blocks, k, width, count):
    f = 1 << k
    lane = lax.broadcasted_iota(jnp.int32, blocks[0].shape, 1)
    west_side = (lane & (f - 1)) < f // 2
    pos = ((lane & (f - 1)).astype(f32) + 0.5) * (1.0 / f)
    other = jnp.abs(pos - 0.5)
    out = []
    for c in range(count):
        at, first = divmod((128 * c) >> k, 128)
        centre = first + (lane >> k)
        near = jnp.where(west_side, centre - 1, centre + 1)
        if c == 0:
            near = jnp.maximum(near, 0)
        if c == count - 1:
            near = jnp.minimum(near, width - 1 - 128 * at)
        near = near & 127
        side = lanes(blocks[at], near)
        if c and first == 0:
            side = jnp.where(lane < f // 2, lanes(blocks[at - 1], near), side)
        if c < count - 1 and first + (128 >> k) == 128:
            side = jnp.where(lane >= 128 - f // 2, lanes(blocks[at + 1], near), side)
        out.append((1.0 - other) * lanes(blocks[at], centre) + other * side)
    return out


def finish_kernel(sizes, cells, v_ref, s0, b0, f1, f2, f3, f4, t1_in, t2_in, slope_ref, bend_ref, t1, t2, t3, t4, u1, u2, slope_buf, bend_buf, sems):
    h0, width0 = sizes[0]
    count = width0 // 128
    sums = jnp.sum(v_ref[...], axis=0)
    lane = lax.broadcasted_iota(jnp.int32, (1, 128), 1)
    number = jnp.ones((1, 128), f32)
    for k, c in enumerate(cells):
        number = jnp.where((lane == k) | (lane == k + LEVELS + 1), float(c), number)
    mean = sums / number
    scale = jnp.where(lane <= LEVELS, 1.0 / (mean + EPS), 1.0 / jnp.sqrt(mean + EPS))
    sub = lax.broadcasted_iota(jnp.int32, (8, 128), 0)
    copies = []
    for field, (base, buf, out) in enumerate(((s0, slope_buf, slope_ref), (b0, bend_buf, bend_ref))):
        for k, f, t in ((4, f4, t4), (3, f3, t3), (2, f2, t2), (1, f1, t1)):
            for at in range(0, f.shape[1], 8):
                for c, v in enumerate(cols_refine(split(f[field, at : at + 8, :]), k, sizes[k][1], count)):
                    if k > 2:
                        t[field, c, at : at + 8, :] = v
                    else:
                        t[field, c, 0:4, :] = v[0:4]
                        t[field, c, sizes[k][0] - 2 : sizes[k][0] + 2, :] = v[4:8]
        c0, c1, c2, c3, c4 = (
            jnp.broadcast_to(scale[:, i : i + 1], (8, 128)) for i in range(field * (LEVELS + 1), (field + 1) * (LEVELS + 1))
        )
        pos = (sub.astype(f32) + 0.5) * 0.125
        high = sub < 4
        w3 = (jnp.where(high, 0.5 - pos, 0.0) * c3, jnp.where(high, 0.5 + pos, 1.5 - pos) * c3, jnp.where(high, 0.0, pos - 0.5) * c3)
        half = pos * 0.5
        w4 = (((0.5 - half) * c4, (0.5 + half) * c4), ((1.0 - half) * c4, half * c4))
        for part in range(2):
            begin, end = part * h0 // 2, (part + 1) * h0 // 2
            for c in range(count):
                for k, t, u, scaled in ((1, t1, u1, c1), (2, t2, u2, c2)):
                    f = 1 << k
                    near = [abs((s + 0.5) / f - 0.5) * scaled for s in range(f)]
                    own = [(1.0 - abs((s + 0.5) / f - 0.5)) * scaled for s in range(f)]
                    for at in range(begin >> k, end >> k, 8):
                        before, centre, after = (t[field, c, at + i : at + i + 8, :] for i in range(3))
                        for s in range(f):
                            u[c, pl.ds(f * at + s, 8, f), :] = own[s] * centre + near[s] * (before if s < f // 2 else after)
                for at in range(begin, end, 8):
                    tile = at // 8
                    total = base[at : at + 8, 128 * c : 128 * c + 128] * c0 + u1[c, at : at + 8, :] + u2[c, at : at + 8, :]
                    for i in range(3):
                        total = total + w3[i] * jnp.broadcast_to(t3[field, c, tile + i : tile + i + 1, :], (8, 128))
                    for i in range(2):
                        row = (tile + 1) // 2 + i
                        total = total + w4[tile % 2][i] * jnp.broadcast_to(t4[field, c, row : row + 1, :], (8, 128))
                    buf[at : at + 8, 128 * c : 128 * c + 128] = total
            rows = pl.ds(begin, end - begin)
            copy = pltpu.make_async_copy(buf.at[rows], out.at[rows], sems.at[2 * field + part])
            copy.start()
            copies.append(copy)
    for copy in copies:
        copy.wait()


def halo_pairs(count):
    both = lambda pairs: [(a, b) for a, b in pairs] + [(b, a) for a, b in pairs]
    even = [(i, i + 1) for i in range(0, count - 1, 2)]
    odd = [(i, i + 1) for i in range(1, count - 1, 2)]
    if count % 2 or count < 8:
        return both(even), both(odd), None, 0
    mid = count * 13 // 16 & ~1
    second = [e for e in odd if e[1] != mid] + [(0, mid - 1), (mid, count - 1)]
    third = [e for e in even if e[0] not in (mid - 2, mid)] + [(mid - 1, mid), (mid - 2, mid + 1)]
    return both(even), both(second), both(third), mid


VM = pl.BlockSpec(memory_space=pltpu.VMEM)
ANY = pl.BlockSpec(memory_space=pl.ANY)


def call(kernel, outs, scratch=(), in_specs=None, out_specs=None, flops=10**6, limit=8 << 20, aliases=None):
    return lambda *args: pl.pallas_call(
        kernel,
        out_shape=[jax.ShapeDtypeStruct(s, f32) for s in outs],
        in_specs=in_specs or [VM] * len(args),
        out_specs=out_specs or [VM] * len(outs),
        scratch_shapes=list(scratch),
        input_output_aliases=aliases or {},
        compiler_params=pltpu.CompilerParams(vmem_limit_bytes=limit),
        cost_estimate=pl.CostEstimate(flops=flops, bytes_accessed=1 << 19, transcendentals=0),
    )(*args)


def local(grid):
    h0, width0 = grid.shape
    count = lax.axis_size("rows")
    sizes = [(h0 >> k, width0 >> k) for k in range(LEVELS + 1)]

    def blocks(rows, width):
        return (up128(width) // 128, -(-rows // 8) * 8, 128)

    z_shapes = [blocks(*size) for size in sizes]
    msg = (4 * z_shapes[0][0] + 4 * z_shapes[1][0] + sizes[2][0] * z_shapes[2][0], 128)
    m1, m2, z0, z1, z2 = call(
        functools.partial(pyramid_kernel, sizes),
        [msg, msg] + z_shapes[:3],
        [pltpu.VMEM((h0 // 2, width0), f32), pltpu.SemaphoreType.DMA((z_shapes[0][0],))],
        in_specs=[pl.BlockSpec(memory_space=pltpu.HBM)],
    )(pltpu.with_memory_space_constraint(grid, pltpu.HBM))
    pairs1, pairs2, pairs3, mid = halo_pairs(count)
    r2 = lax.ppermute(m2, "rows", pairs2)
    r1 = lax.ppermute(m1, "rows", pairs1)
    r3 = lax.ppermute(m2, "rows", pairs3) if mid else m2
    acc = (2 * LEVELS + 2, 8, 128)
    fine = [(2, z_shapes[0][0], -(-(h + 2) // 8) * 8, 128) for h, _ in sizes[1:]]
    f_shapes = [(2, 8, up128(w)) for _, w in sizes[1:3]] + [(2, -(-(h + 2) // 8) * 8, up128(w)) for h, w in sizes[3:]]
    s0, b0, t1, t2, sums = call(
        functools.partial(inner_kernel, sizes), [grid.shape, grid.shape] + fine[:2] + [acc], flops=10**8
    )(z0, z1, z2)
    s0, b0, f1, f2, f3, f4, sums = call(
        functools.partial(edge_kernel, sizes, mid),
        [grid.shape, grid.shape] + f_shapes + [(count, 1, 128)],
        [pltpu.VMEM(msg, f32)] * 2
        + [pltpu.VMEM(blocks(rows, sizes[k][1]), f32) for k in range(2) for rows in (24, 24)]
        + [pltpu.VMEM(blocks(3 * sizes[2][0], sizes[2][1]), f32)]
        + [pltpu.VMEM(blocks(sizes[3][0] + 16, sizes[3][1]), f32)]
        + [pltpu.VMEM(blocks(16, sizes[4][1]), f32), pltpu.VMEM((8, width0), f32)],
        aliases={7: 0, 8: 1},
    )(z0, z1, z2, r1, r2, r3, sums, s0, b0)
    seen = lax.all_to_all(sums, "rows", 0, 0, tiled=True)
    cells = [count * h * w for h, w in sizes]
    return tuple(
        call(
            functools.partial(finish_kernel, sizes, cells),
            [grid.shape, grid.shape] + fine[:2],
            [pltpu.VMEM(v, f32) for v in fine[2:] + z_shapes[:1] * 2 + [grid.shape] * 2] + [pltpu.SemaphoreType.DMA((4,))],
            out_specs=[ANY, ANY, VM, VM],
            aliases={7: 2, 8: 3},
        )(seen, s0, b0, f1, f2, f3, f4, t1, t2)[:2]
    )


def solution(mesh):
    return jax.shard_map(
        local,
        mesh=mesh,
        in_specs=(P("rows", None),),
        out_specs=(P("rows", None), P("rows", None)),
        check_vma=False,
    )
```

```python
import functools

import jax
import jax.numpy as jnp
from jax import lax
from jax.experimental import pallas as pl
from jax.experimental.pallas import tpu as pltpu
from jax.sharding import PartitionSpec as P

LEVELS = 4
EPS = 1e-06
f32 = jnp.float32
ATAN = (
    1.0,
    -0.3333314528,
    0.1999355085,
    -0.1420889944,
    0.1065626393,
    -0.0752896400,
    0.0429096138,
    -0.0161657367,
    0.0028662257,
)


def up128(n):
    return -(-n // 128) * 128


def lane_of(v):
    return lax.broadcasted_iota(jnp.int32, v.shape, 1)


def row_of(v):
    return lax.broadcasted_iota(jnp.int32, v.shape, 0)


def west(v):
    return jnp.where(lane_of(v) == 0, v, pltpu.roll(v, 1, 1))


def east(v, width):
    return jnp.where(lane_of(v) == width - 1, v, pltpu.roll(v, v.shape[1] - 1, 1))


def take(ref, at, count):
    return jnp.concatenate([ref[c, at : at + count, :] for c in range(ref.shape[0])], axis=1)


def store(ref, at, v):
    for c in range(ref.shape[0]):
        ref[c, at : at + v.shape[0], :] = v[:, 128 * c : 128 * c + 128]


def rows_sum(ref, start, count):
    out = []
    for c in range(ref.shape[0]):
        part = [ref[c, pl.ds(start + a, count, 2), :] for a in range(5)]
        out.append((part[0] + part[4]) * 0.0625 + (part[1] + part[3]) * 0.25 + part[2] * 0.375)
    return jnp.concatenate(out, axis=1)


def lanes(v, at):
    return jnp.take_along_axis(v, at, axis=1, mode="promise_in_bounds")


def split(v):
    return [v[:, at : at + 128] for at in range(0, v.shape[1], 128)]


def cols_coarsen(v, width):
    blocks = split(v)
    lane = lax.broadcasted_iota(jnp.int32, blocks[0].shape, 1)
    patterns = [(2 * lane + tap + 128) & 127 for tap in (-2, -1, 0, 1, 2)]
    found = [[lanes(v, at) for v in blocks] for at in patterns]
    out = []
    for c in range(0, len(blocks), 2):
        taps = []
        for tap, got in zip((-2, -1, 0, 1, 2), found):
            part = got[c]
            if c + 1 < len(blocks):
                part = jnp.where(2 * lane + tap < 128, part, got[c + 1])
            if tap < 0 and c:
                part = jnp.where(lane == 0, got[c - 1], part)
            if tap > 1 and c + 2 < len(blocks):
                part = jnp.where(lane == 127, got[c + 2], part)
            taps.append(part)
        if c == 0:
            taps[0] = jnp.where(lane == 0, taps[2], taps[0])
            taps[1] = jnp.where(lane == 0, taps[2], taps[1])
        taps[4] = jnp.where(lane == width // 2 - 1 - 64 * c, taps[3], taps[4])
        out.append((taps[0] + taps[4]) * 0.0625 + (taps[1] + taps[3]) * 0.25 + taps[2] * 0.375)
    return out[0] if len(out) == 1 else jnp.concatenate(out, axis=1)


def pyramid_kernel(sizes, x_ref, m1_ref, m2_ref, z0, z1, z2, tmp, sems):
    copies = [
        pltpu.make_async_copy(x_ref.at[:, pl.ds(128 * c, 128)], z0.at[c], sems.at[c]) for c in range(z0.shape[0])
    ]
    for copy in copies:
        copy.start()
    odd = lax.rem(lax.axis_index("rows"), 2) == 1
    h = sizes[0][0]
    for copy in copies:
        copy.wait()

    def put(row, z, top_at, bottom_at, count):
        for c in range(z.shape[0]):
            top, bottom = z[c, top_at : top_at + count, :], z[c, bottom_at : bottom_at + count, :]
            m1_ref[row : row + count, :] = jnp.where(odd, top, bottom)
            m2_ref[row : row + count, :] = jnp.where(odd, bottom, top)
            row += count
        return row

    row = put(0, z0, 0, h - 4, 4)
    for k, z in ((0, z1), (1, z2)):
        half, wp = sizes[k + 1][0], up128(sizes[k][1])
        low = k + 1
        tmp[low : half - 1, :wp] = rows_sum((z0, z1)[k], 2 * low - 2, half - 1 - low)
        store(z, 0, cols_coarsen(tmp[0:half, :wp], sizes[k][1]))
    row = put(row, z1, 1, sizes[1][0] - 5, 4)
    put(row, z2, 0, 0, sizes[2][0])


def relief(upper, middle, lower, width, spacing, sides=None):
    diff = lower - upper
    if sides is None:
        tall = lower + upper + 2.0 * middle
        (d_w, m_w, t_w), (d_e, m_e, t_e) = ([west(v) for v in (diff, middle, tall)], [east(v, width) for v in (diff, middle, tall)])
    else:
        (d_w, m_w, t_w), (d_e, m_e, t_e) = ((c - a, b, c + a + 2.0 * b) for a, b, c in sides)
    p = (t_e - t_w) * (1.0 / (8.0 * spacing))
    q = (d_e + d_w + 2.0 * diff) * (1.0 / (8.0 * spacing))
    inv = 1.0 / (spacing * spacing)
    r = ((m_e - middle) - (middle - m_w)) * inv
    t = ((lower - middle) - (middle - upper)) * inv
    u = (d_e - d_w) * (0.25 * inv)
    pp, qq = p * p, q * q
    steep = pp + qq
    base = 1.0 + steep
    root = jnp.sqrt(base)
    y = jnp.sqrt(steep) / (1.0 + root)
    y2 = y * y
    acc = ATAN[-1]
    for c in ATAN[-2::-1]:
        acc = acc * y2 + c
    slope = 2.0 * y * acc
    bend = -(pp * r + 2.0 * (p * q) * u + qq * t) / (base * root)
    return slope, bend


def fold(v):
    total = None
    for row in range(0, v.shape[0], 8):
        for at in range(0, v.shape[1], 128):
            part = v[row : row + 8, at : at + 128]
            total = part if total is None else total + part
    return total


def inner_kernel(sizes, z0, z1, z2, s0_ref, b0_ref, t1, t2, acc_ref):
    for k, z in enumerate((z0, z1, z2)):
        h, width = sizes[k]
        s_sum = b_sum = None
        for at in range(0, h, 8):
            middle = take(z, at, 8)
            upper = take(z, at - 1, 8) if at else pltpu.roll(middle, 1, 0)
            lower = take(z, at + 1, 8) if at < h - 8 else pltpu.roll(middle, 7, 0)
            slope, bend = relief(upper, middle, lower, width, float(2**k))
            if k == 0:
                s0_ref[at : at + 8, :] = slope
                b0_ref[at : at + 8, :] = bend
            else:
                t = (t1, t2)[k - 1]
                for field, v in enumerate((slope, bend)):
                    for c, part in enumerate(cols_refine(split(v), k, width, t.shape[1])):
                        t[field, c, at + 1 : at + 9, :] = part
            skip = 3 if k else 1
            if at == 0 or at == h - 8 or width % 128:
                row = row_of(slope) + at
                kept = (row >= skip) & (row < h - skip) & (lane_of(slope) < width)
                slope, bend = jnp.where(kept, slope, 0.0), jnp.where(kept, bend, 0.0)
            fs, fb = fold(slope), fold(bend * bend)
            s_sum = fs if at == 0 else s_sum + fs
            b_sum = fb if at == 0 else b_sum + fb
        acc_ref[k] = s_sum
        acc_ref[LEVELS + k] = b_sum
    for k in range(3, LEVELS):
        acc_ref[k] = jnp.zeros((8, 128), f32)
        acc_ref[LEVELS + k] = jnp.zeros((8, 128), f32)


def edge_kernel(sizes, mid, z0, z1, z2, r1_ref, r2_ref, r3_ref, acc_ref, s0_in, b0_in,
                s0_ref, b0_ref, f1, f2, f3, f4, sum_ref, up, lo, t0, e0, t1, e1, w2, w3, w4, tmp):
    me = lax.axis_index("rows")
    odd = lax.rem(me, 2) == 1
    first, last = me == 0, me == lax.axis_size("rows") - 1
    r1, r2 = r1_ref[...], r2_ref[...]
    if mid:
        r2 = jnp.where((me == mid) | (me == mid - 1), r3_ref[...], r2)
    up[...] = jnp.where(odd, r1, r2)
    lo[...] = jnp.where(odd, r2, r1)

    h0, width0 = sizes[0]
    for c in range(z0.shape[0]):
        t0[c, 8:16, :] = z0[c, 0:8, :]
        t0[c, 4:8, :] = jnp.where(first, jnp.broadcast_to(z0[c, 0:1, :], (4, 128)), up[4 * c : 4 * c + 4, :])
        e0[c, 8:16, :] = z0[c, h0 - 8 : h0, :]
        e0[c, 16:20, :] = jnp.where(last, jnp.broadcast_to(z0[c, h0 - 1 : h0, :], (4, 128)), lo[4 * c : 4 * c + 4, :])
    base = 4 * z0.shape[0]
    h1, width1 = sizes[1]
    tmp[0:3, :] = rows_sum(t0, 4, 3)
    tmp[3:5, :] = rows_sum(e0, 12, 2)
    edge = cols_coarsen(tmp[...], width0)
    for c in range(z1.shape[0]):
        part = edge[:, 128 * c : 128 * c + 128]
        row0, end = part[1:2], part[3:4]
        t1[c, 8:16, :] = z1[c, 0:8, :]
        t1[c, 8:9, :] = row0
        t1[c, 7:8, :] = jnp.where(first, row0, part[0:1])
        t1[c, 4:7, :] = jnp.where(first, jnp.broadcast_to(row0, (3, 128)), up[base + 4 * c + 1 : base + 4 * c + 4, :])
        e1[c, 8:16, :] = z1[c, h1 - 8 : h1, :]
        e1[c, 15:16, :] = end
        e1[c, 16:17, :] = jnp.where(last, end, part[4:5])
        e1[c, 17:21, :] = jnp.where(last, jnp.broadcast_to(end, (4, 128)), lo[base + 4 * c : base + 4 * c + 4, :])
    base += 4 * z1.shape[0]
    h2, width2 = sizes[2]
    wq = up128(width1)
    tmp[0:3, :wq] = rows_sum(t1, 4, 3)
    tmp[3:6, :wq] = rows_sum(e1, 12, 3)
    edge = cols_coarsen(tmp[:, :wq], width1)
    for c in range(z2.shape[0]):
        part = edge[:, 128 * c : 128 * c + 128]
        row0, end = part[1:2], part[3:4]
        at = base + h2 * c
        w2[c, 0:h2, :] = jnp.where(first, jnp.broadcast_to(row0, (h2, 128)), up[at : at + h2, :])
        w2[c, h2 : 2 * h2, :] = z2[c]
        w2[c, 2 * h2 : 3 * h2, :] = jnp.where(last, jnp.broadcast_to(end, (h2, 128)), lo[at : at + h2, :])
        w2[c, h2 - 1 : h2, :] = jnp.where(first, row0, part[0:1])
        w2[c, h2 : h2 + 2, :] = part[1:3]
        w2[c, 2 * h2 - 1 : 2 * h2, :] = end
        w2[c, 2 * h2 : 2 * h2 + 1, :] = jnp.where(last, end, part[4:5])
        w2[c, 2 * h2 + 1 : 2 * h2 + 2, :] = jnp.where(last, end, part[5:6])
    h3, width3 = sizes[3]
    wq = up128(width2)
    v = cols_coarsen(pad_rows(rows_sum(w2, h2 - 14, h3 + 11)), width2)
    row = row_of(v) - 6
    v = jnp.where(first & (row < 0), v[6:7], jnp.where(last & (row >= h3), v[h3 + 5 : h3 + 6], v))
    w3[0] = v
    h4, width4 = sizes[4]
    v = pad_rows(rows_sum(w3, 0, h4 + 4))
    row = row_of(v) - 2
    column = lane_of(v) & 63
    for i, step in enumerate((0, -1, 1)):
        at = 2 * jnp.clip(column + step, 0, width4 - 1)
        taps = [lanes(v, jnp.clip(at + tap, 0, width3 - 1)) for tap in (-2, -1, 0, 1, 2)]
        level = (taps[0] + taps[4]) * 0.0625 + (taps[1] + taps[3]) * 0.25 + taps[2] * 0.375
        level = jnp.where(first & (row < 0), level[2:3], jnp.where(last & (row >= h4), level[h4 + 1 : h4 + 2], level))
        w4[i, 0:8, :] = level
        w4[i, 8:16, :] = level

    totals = []

    def add(k, slope, bend, kept):
        kept = kept & (lane_of(slope) < sizes[k][1])
        totals.append((acc_ref[k] + fold(jnp.where(kept, slope, 0.0)),
                       acc_ref[LEVELS + k] + fold(jnp.where(kept, bend * bend, 0.0))))

    def ends(top, top_at, bottom, bottom_at):
        a, b = take(top, top_at, 8), take(bottom, bottom_at - 4, 8)
        return jnp.where(row_of(a) < 4, a, b)

    slope, bend = relief(*(ends(t0, 7 + i, e0, 11 + i) for i in range(3)), width0, 1.0)
    for ref, v in ((s0_ref, slope), (b0_ref, bend)):
        ref[0:4, :] = v[0:4]
        ref[h0 - 4 : h0, :] = v[4:8]
    add(0, slope, bend, (row_of(slope) == 0) | (row_of(slope) == 7))
    for k, top, bottom, top_at, bottom_at, f in ((1, t1, e1, 7, 13, f1), (2, w2, w2, h2 - 1, 2 * h2 - 3, f2)):
        h, width = sizes[k]
        slope, bend = relief(*(ends(top, top_at - 1 + i, bottom, bottom_at - 1 + i) for i in range(3)), width, float(2**k))
        add(k, slope, bend, (row_of(slope) > 0) & (row_of(slope) < 7))
        for field, v in enumerate((slope, bend)):
            row = row_of(v)
            v = jnp.where(first & (row == 0), v[1:2], jnp.where(last & (row == 7), v[6:7], v))
            for c, part in enumerate(cols_refine(split(v), k, width, f.shape[1])):
                f[field, c] = part
    for k, z, at, f in ((3, w3, 5, f3), (4, w4, 1, f4)):
        h, width = sizes[k]
        rows = -(-(h + 2) // 8) * 8
        if k == 3:
            slope, bend = relief(take(z, at - 1, rows), take(z, at, rows), take(z, at + 1, rows), width, float(2**k))
        else:
            around = [[z[i, at + j : at + j + rows, :] for j in (-1, 0, 1)] for i in range(3)]
            slope, bend = relief(*around[0], width, float(2**k), around[1:])
        row = row_of(slope) - 1
        if k == 3:
            add(k, slope, bend, (row >= 0) & (row < h))
        else:
            kept = (row >= 0) & (row < h)
            slope4, bend4 = jnp.where(kept, slope, 0.0), jnp.where(kept, bend * bend, 0.0)
        for field, v in enumerate((slope, bend)):
            v = jnp.where(first & (row < 0), v[1:2], jnp.where(last & (row >= h), v[h : h + 1], v))
            f[field, 0:rows, :] = jnp.where(row <= h, v, 0.0)
    table = jnp.zeros((8, 128), f32)
    lane = lane_of(table)
    for k, pair in enumerate(totals):
        for field, v in enumerate(pair):
            table = jnp.where(lane == 64 * field + width4 + k, jnp.sum(v, axis=1, keepdims=True), table)
    table = jnp.where((lane & 63) < width4, jnp.where(lane < 64, slope4, bend4), table)
    line = jnp.sum(table, axis=0, keepdims=True)
    sum_ref[...] = jnp.broadcast_to(line.reshape(1, 1, 128), sum_ref.shape)


def pad_rows(v):
    short = -v.shape[0] % 8
    return jnp.concatenate([v, jnp.zeros((short, v.shape[1]), f32)], axis=0) if short else v


def cols_refine(blocks, k, width, count):
    f = 1 << k
    lane = lax.broadcasted_iota(jnp.int32, blocks[0].shape, 1)
    west_side = (lane & (f - 1)) < f // 2
    pos = ((lane & (f - 1)).astype(f32) + 0.5) * (1.0 / f)
    other = jnp.abs(pos - 0.5)
    out = []
    for c in range(count):
        at, first = divmod((128 * c) >> k, 128)
        centre = first + (lane >> k)
        near = jnp.where(west_side, centre - 1, centre + 1)
        if c == 0:
            near = jnp.maximum(near, 0)
        if c == count - 1:
            near = jnp.minimum(near, width - 1 - 128 * at)
        near = near & 127
        side = lanes(blocks[at], near)
        if c and first == 0:
            side = jnp.where(lane < f // 2, lanes(blocks[at - 1], near), side)
        if c < count - 1 and first + (128 >> k) == 128:
            side = jnp.where(lane >= 128 - f // 2, lanes(blocks[at + 1], near), side)
        out.append((1.0 - other) * lanes(blocks[at], centre) + other * side)
    return out


def finish_kernel(sizes, cells, v_ref, s0, b0, f1, f2, f3, f4, t1_in, t2_in, slope_ref, bend_ref, t1, t2, t3, t4, u1, u2, u3, u4, slope_buf, bend_buf, sems):
    h0, width0 = sizes[0]
    count = width0 // 128
    sums = jnp.sum(v_ref[...], axis=0, keepdims=True)
    lane = lax.broadcasted_iota(jnp.int32, (1, 128), 1)
    slot = sizes[LEVELS][1]
    number = jnp.ones((1, 128), f32)
    for k, c in enumerate(cells):
        number = jnp.where((lane & 63) == slot + k, float(c), number)
    last = [
        jnp.sum(jnp.where((lane >= at) & (lane < at + slot), sums, 0.0), axis=1, keepdims=True) for at in (0, 64)
    ]
    sums = jnp.where(lane == slot + LEVELS, last[0], jnp.where(lane == 64 + slot + LEVELS, last[1], sums))
    mean = sums / number
    scale = jnp.where(lane < 64, 1.0 / (mean + EPS), 1.0 / jnp.sqrt(mean + EPS))
    for field in range(2):
        for k, f, t in ((1, f1, t1), (2, f2, t2)):
            for c in range(count):
                t[field, c, 0:4, :] = f[field, c, 0:4, :]
                t[field, c, sizes[k][0] - 2 : sizes[k][0] + 2, :] = f[field, c, 4:8, :]
        for k, f, t in ((4, f4, t4), (3, f3, t3)):
            for at in range(0, f.shape[1], 8):
                for c, v in enumerate(cols_refine(split(f[field, at : at + 8, :]), k, sizes[k][1], count)):
                    t[field, c, at : at + 8, :] = v
        for k, t, u in ((1, t1, u1), (2, t2, u2), (3, t3, u3)):
            f = 1 << k
            for c in range(count):
                for at in range(0, sizes[k][0], 8):
                    before, centre, after = (t[field, c, at + i : at + i + 8, :] for i in range(3))
                    for s in range(f):
                        near = abs((s + 0.5) / f - 0.5)
                        u[field, c, pl.ds(f * at + s, 8, f), :] = (1.0 - near) * centre + near * (before if s < f // 2 else after)
        pos = (lax.broadcasted_iota(jnp.int32, (8, 128), 0).astype(f32) + 0.5) * 0.0625
        for c in range(count):
            for at in range(0, h0, 16):
                a, b, d = (jnp.broadcast_to(t4[field, c, at // 16 + i : at // 16 + i + 1, :], (8, 128)) for i in range(3))
                u4[field, c, at : at + 8, :] = (0.5 - pos) * a + (0.5 + pos) * b
                u4[field, c, at + 8 : at + 16, :] = (1.0 - pos) * b + pos * d
    copies = []
    for field, (base, buf, out) in enumerate(((s0, slope_buf, slope_ref), (b0, bend_buf, bend_ref))):
        weights = [jnp.broadcast_to(scale[:, i : i + 1], (8, 128)) for i in range(64 * field + slot, 64 * field + slot + LEVELS + 1)]
        for part in range(2):
            begin, end = part * h0 // 2, (part + 1) * h0 // 2
            for c in range(count):
                for at in range(begin, end, 8):
                    total = base[at : at + 8, 128 * c : 128 * c + 128] * weights[0]
                    for weight, u in zip(weights[1:], (u1, u2, u3, u4)):
                        total = total + u[field, c, at : at + 8, :] * weight
                    buf[at : at + 8, 128 * c : 128 * c + 128] = total
            rows = pl.ds(begin, end - begin)
            copy = pltpu.make_async_copy(buf.at[rows], out.at[rows], sems.at[2 * field + part])
            copy.start()
            copies.append(copy)
    for copy in copies:
        copy.wait()


def halo_pairs(count):
    both = lambda pairs: [(a, b) for a, b in pairs] + [(b, a) for a, b in pairs]
    even = [(i, i + 1) for i in range(0, count - 1, 2)]
    odd = [(i, i + 1) for i in range(1, count - 1, 2)]
    if count % 2 or count < 8:
        return both(even), both(odd), None, 0
    mid = count * 13 // 16 & ~1
    second = [e for e in odd if e[1] != mid] + [(0, mid - 1), (mid, count - 1)]
    third = [e for e in even if e[0] not in (mid - 2, mid)] + [(mid - 1, mid), (mid - 2, mid + 1)]
    return both(even), both(second), both(third), mid


VM = pl.BlockSpec(memory_space=pltpu.VMEM)
ANY = pl.BlockSpec(memory_space=pl.ANY)


def call(kernel, outs, scratch=(), in_specs=None, out_specs=None, flops=10**6, limit=8 << 20, aliases=None):
    return lambda *args: pl.pallas_call(
        kernel,
        out_shape=[jax.ShapeDtypeStruct(s, f32) for s in outs],
        in_specs=in_specs or [VM] * len(args),
        out_specs=out_specs or [VM] * len(outs),
        scratch_shapes=list(scratch),
        input_output_aliases=aliases or {},
        compiler_params=pltpu.CompilerParams(vmem_limit_bytes=limit),
        cost_estimate=pl.CostEstimate(flops=flops, bytes_accessed=1 << 19, transcendentals=0),
    )(*args)


def local(grid):
    h0, width0 = grid.shape
    count = lax.axis_size("rows")
    sizes = [(h0 >> k, width0 >> k) for k in range(LEVELS + 1)]

    def blocks(rows, width):
        return (up128(width) // 128, -(-rows // 8) * 8, 128)

    z_shapes = [blocks(*size) for size in sizes]
    msg = (4 * z_shapes[0][0] + 4 * z_shapes[1][0] + sizes[2][0] * z_shapes[2][0], 128)
    m1, m2, z0, z1, z2 = call(
        functools.partial(pyramid_kernel, sizes),
        [msg, msg] + z_shapes[:3],
        [pltpu.VMEM((h0 // 2, width0), f32), pltpu.SemaphoreType.DMA((z_shapes[0][0],))],
        in_specs=[pl.BlockSpec(memory_space=pltpu.HBM)],
    )(pltpu.with_memory_space_constraint(grid, pltpu.HBM))
    pairs1, pairs2, pairs3, mid = halo_pairs(count)
    r2 = lax.ppermute(m2, "rows", pairs2)
    r1 = lax.ppermute(m1, "rows", pairs1)
    r3 = lax.ppermute(m2, "rows", pairs3) if mid else m2
    acc = (2 * LEVELS, 8, 128)
    fine = [(2, z_shapes[0][0], -(-(h + 2) // 8) * 8, 128) for h, _ in sizes[1:]]
    f_shapes = [(2, z_shapes[0][0], 8, 128)] * 2 + [(2, -(-(h + 2) // 8) * 8, up128(w)) for h, w in sizes[3:]]
    s0, b0, t1, t2, sums = call(
        functools.partial(inner_kernel, sizes), [grid.shape, grid.shape] + fine[:2] + [acc], flops=10**8
    )(z0, z1, z2)
    s0, b0, f1, f2, f3, f4, sums = call(
        functools.partial(edge_kernel, sizes, mid),
        [grid.shape, grid.shape] + f_shapes + [(count, 1, 128)],
        [pltpu.VMEM(msg, f32)] * 2
        + [pltpu.VMEM(blocks(rows, sizes[k][1]), f32) for k in range(2) for rows in (24, 24)]
        + [pltpu.VMEM(blocks(3 * sizes[2][0], sizes[2][1]), f32)]
        + [pltpu.VMEM(blocks(sizes[3][0] + 16, sizes[3][1]), f32)]
        + [pltpu.VMEM((3, 16, 128), f32), pltpu.VMEM((8, width0), f32)],
        aliases={7: 0, 8: 1},
    )(z0, z1, z2, r1, r2, r3, sums, s0, b0)
    seen = lax.all_to_all(sums, "rows", 0, 0, tiled=True).reshape(count, 128)
    cells = [count * h * w for h, w in sizes]
    return tuple(
        call(
            functools.partial(finish_kernel, sizes, cells),
            [grid.shape, grid.shape] + fine[:2],
            [pltpu.VMEM(v, f32) for v in fine[2:] + [(2, *z_shapes[0])] * 4 + [grid.shape] * 2] + [pltpu.SemaphoreType.DMA((4,))],
            out_specs=[ANY, ANY, VM, VM],
            aliases={7: 2, 8: 3},
        )(seen, s0, b0, f1, f2, f3, f4, t1, t2)[:2]
    )


def solution(mesh):
    return jax.shard_map(
        local,
        mesh=mesh,
        in_specs=(P("rows", None),),
        out_specs=(P("rows", None), P("rows", None)),
        check_vma=False,
    )
```

```python
import functools

import jax
import jax.numpy as jnp
from jax import lax
from jax.experimental import pallas as pl
from jax.experimental.pallas import tpu as pltpu
from jax.sharding import PartitionSpec as P

LEVELS = 4
EPS = 1e-06
f32 = jnp.float32
ATAN = (
    1.0,
    -0.3333314528,
    0.1999355085,
    -0.1420889944,
    0.1065626393,
    -0.0752896400,
    0.0429096138,
    -0.0161657367,
    0.0028662257,
)


def up128(n):
    return -(-n // 128) * 128


def lane_of(v):
    return lax.broadcasted_iota(jnp.int32, v.shape, 1)


def row_of(v):
    return lax.broadcasted_iota(jnp.int32, v.shape, 0)


def west(v):
    return jnp.where(lane_of(v) == 0, v, pltpu.roll(v, 1, 1))


def east(v, width):
    return jnp.where(lane_of(v) == width - 1, v, pltpu.roll(v, v.shape[1] - 1, 1))


def take(ref, at, count):
    return jnp.concatenate([ref[c, at : at + count, :] for c in range(ref.shape[0])], axis=1)


def store(ref, at, v):
    for c in range(ref.shape[0]):
        ref[c, at : at + v.shape[0], :] = v[:, 128 * c : 128 * c + 128]


def rows_sum(ref, start, count):
    out = []
    for c in range(ref.shape[0]):
        part = [ref[c, pl.ds(start + a, count, 2), :] for a in range(5)]
        out.append((part[0] + part[4]) * 0.0625 + (part[1] + part[3]) * 0.25 + part[2] * 0.375)
    return jnp.concatenate(out, axis=1)


def lanes(v, at):
    return jnp.take_along_axis(v, at, axis=1, mode="promise_in_bounds")


def split(v):
    return [v[:, at : at + 128] for at in range(0, v.shape[1], 128)]


def cols_coarsen(v, width):
    blocks = split(v)
    lane = lax.broadcasted_iota(jnp.int32, blocks[0].shape, 1)
    patterns = [(2 * lane + tap + 128) & 127 for tap in (-2, -1, 0, 1, 2)]
    found = [[lanes(v, at) for v in blocks] for at in patterns]
    out = []
    for c in range(0, len(blocks), 2):
        taps = []
        for tap, got in zip((-2, -1, 0, 1, 2), found):
            part = got[c]
            if c + 1 < len(blocks):
                part = jnp.where(2 * lane + tap < 128, part, got[c + 1])
            if tap < 0 and c:
                part = jnp.where(lane == 0, got[c - 1], part)
            if tap > 1 and c + 2 < len(blocks):
                part = jnp.where(lane == 127, got[c + 2], part)
            taps.append(part)
        if c == 0:
            taps[0] = jnp.where(lane == 0, taps[2], taps[0])
            taps[1] = jnp.where(lane == 0, taps[2], taps[1])
        taps[4] = jnp.where(lane == width // 2 - 1 - 64 * c, taps[3], taps[4])
        out.append((taps[0] + taps[4]) * 0.0625 + (taps[1] + taps[3]) * 0.25 + taps[2] * 0.375)
    return out[0] if len(out) == 1 else jnp.concatenate(out, axis=1)


def pyramid_kernel(sizes, x_ref, m1_ref, m2_ref, z0, z1, z2, tmp, sems):
    copies = [
        pltpu.make_async_copy(x_ref.at[:, pl.ds(128 * c, 128)], z0.at[c], sems.at[c]) for c in range(z0.shape[0])
    ]
    for copy in copies:
        copy.start()
    odd = lax.rem(lax.axis_index("rows"), 2) == 1
    h = sizes[0][0]
    for copy in copies:
        copy.wait()

    def put(row, z, top_at, bottom_at, count):
        for c in range(z.shape[0]):
            top, bottom = z[c, top_at : top_at + count, :], z[c, bottom_at : bottom_at + count, :]
            m1_ref[row : row + count, :] = jnp.where(odd, top, bottom)
            m2_ref[row : row + count, :] = jnp.where(odd, bottom, top)
            row += count
        return row

    row = put(0, z0, 0, h - 4, 4)
    for k, z in ((0, z1), (1, z2)):
        half, wp = sizes[k + 1][0], up128(sizes[k][1])
        low = k + 1
        tmp[low : half - 1, :wp] = rows_sum((z0, z1)[k], 2 * low - 2, half - 1 - low)
        store(z, 0, cols_coarsen(tmp[0:half, :wp], sizes[k][1]))
    row = put(row, z1, 1, sizes[1][0] - 5, 4)
    put(row, z2, 0, 0, sizes[2][0])


def relief(upper, middle, lower, width, spacing, sides=None):
    diff = lower - upper
    if sides is None:
        tall = lower + upper + 2.0 * middle
        (d_w, m_w, t_w), (d_e, m_e, t_e) = ([west(v) for v in (diff, middle, tall)], [east(v, width) for v in (diff, middle, tall)])
    else:
        (d_w, m_w, t_w), (d_e, m_e, t_e) = ((c - a, b, c + a + 2.0 * b) for a, b, c in sides)
    p = (t_e - t_w) * (1.0 / (8.0 * spacing))
    q = (d_e + d_w + 2.0 * diff) * (1.0 / (8.0 * spacing))
    inv = 1.0 / (spacing * spacing)
    r = ((m_e - middle) - (middle - m_w)) * inv
    t = ((lower - middle) - (middle - upper)) * inv
    u = (d_e - d_w) * (0.25 * inv)
    pp, qq = p * p, q * q
    steep = pp + qq
    base = 1.0 + steep
    root = jnp.sqrt(base)
    y = jnp.sqrt(steep) / (1.0 + root)
    y2 = y * y
    acc = ATAN[-1]
    for c in ATAN[-2::-1]:
        acc = acc * y2 + c
    slope = 2.0 * y * acc
    bend = -(pp * r + 2.0 * (p * q) * u + qq * t) / (base * root)
    return slope, bend


def fold(v):
    total = None
    for row in range(0, v.shape[0], 8):
        for at in range(0, v.shape[1], 128):
            part = v[row : row + 8, at : at + 128]
            total = part if total is None else total + part
    return total


def inner_kernel(sizes, z0, z1, z2, s0_ref, b0_ref, t1, t2, acc_ref):
    for k, z in enumerate((z0, z1, z2)):
        h, width = sizes[k]
        s_sum = b_sum = None
        for at in range(0, h, 8):
            middle = take(z, at, 8)
            upper = take(z, at - 1, 8) if at else pltpu.roll(middle, 1, 0)
            lower = take(z, at + 1, 8) if at < h - 8 else pltpu.roll(middle, 7, 0)
            slope, bend = relief(upper, middle, lower, width, float(2**k))
            if k == 0:
                s0_ref[at : at + 8, :] = slope
                b0_ref[at : at + 8, :] = bend
            else:
                t = (t1, t2)[k - 1]
                for field, v in enumerate((slope, bend)):
                    for c, part in enumerate(cols_refine(split(v), k, width, t.shape[1])):
                        t[field, c, at + 1 : at + 9, :] = part
            skip = 3 if k else 1
            if at == 0 or at == h - 8 or width % 128:
                row = row_of(slope) + at
                kept = (row >= skip) & (row < h - skip) & (lane_of(slope) < width)
                slope, bend = jnp.where(kept, slope, 0.0), jnp.where(kept, bend, 0.0)
            fs, fb = fold(slope), fold(bend * bend)
            s_sum = fs if at == 0 else s_sum + fs
            b_sum = fb if at == 0 else b_sum + fb
        acc_ref[k] = s_sum
        acc_ref[LEVELS + k] = b_sum
    for k in range(3, LEVELS):
        acc_ref[k] = jnp.zeros((8, 128), f32)
        acc_ref[LEVELS + k] = jnp.zeros((8, 128), f32)


def rows_refine(t, u, field, k, height):
    f = 1 << k
    for c in range(t.shape[1]):
        for at in range(0, height, 8):
            before, centre, after = (t[field, c, at + i : at + i + 8, :] for i in range(3))
            for s in range(f):
                near = abs((s + 0.5) / f - 0.5)
                u[field, c, pl.ds(f * at + s, 8, f), :] = (1.0 - near) * centre + near * (before if s < f // 2 else after)


def edge_kernel(sizes, mid, z0, z1, z2, r1_ref, r2_ref, r3_ref, acc_ref, s0_in, b0_in, t1_in, t2_in,
                s0_ref, b0_ref, t1, t2, u1, u2, f3, f4, sum_ref, up, lo, top0, end0, top1, end1, w2, w3, w4, tmp):
    me = lax.axis_index("rows")
    odd = lax.rem(me, 2) == 1
    first, last = me == 0, me == lax.axis_size("rows") - 1
    r1, r2 = r1_ref[...], r2_ref[...]
    if mid:
        r2 = jnp.where((me == mid) | (me == mid - 1), r3_ref[...], r2)
    up[...] = jnp.where(odd, r1, r2)
    lo[...] = jnp.where(odd, r2, r1)

    h0, width0 = sizes[0]
    for c in range(z0.shape[0]):
        top0[c, 8:16, :] = z0[c, 0:8, :]
        top0[c, 4:8, :] = jnp.where(first, jnp.broadcast_to(z0[c, 0:1, :], (4, 128)), up[4 * c : 4 * c + 4, :])
        end0[c, 8:16, :] = z0[c, h0 - 8 : h0, :]
        end0[c, 16:20, :] = jnp.where(last, jnp.broadcast_to(z0[c, h0 - 1 : h0, :], (4, 128)), lo[4 * c : 4 * c + 4, :])
    base = 4 * z0.shape[0]
    h1, width1 = sizes[1]
    tmp[0:3, :] = rows_sum(top0, 4, 3)
    tmp[3:5, :] = rows_sum(end0, 12, 2)
    edge = cols_coarsen(tmp[...], width0)
    for c in range(z1.shape[0]):
        part = edge[:, 128 * c : 128 * c + 128]
        row0, end = part[1:2], part[3:4]
        top1[c, 8:16, :] = z1[c, 0:8, :]
        top1[c, 8:9, :] = row0
        top1[c, 7:8, :] = jnp.where(first, row0, part[0:1])
        top1[c, 4:7, :] = jnp.where(first, jnp.broadcast_to(row0, (3, 128)), up[base + 4 * c + 1 : base + 4 * c + 4, :])
        end1[c, 8:16, :] = z1[c, h1 - 8 : h1, :]
        end1[c, 15:16, :] = end
        end1[c, 16:17, :] = jnp.where(last, end, part[4:5])
        end1[c, 17:21, :] = jnp.where(last, jnp.broadcast_to(end, (4, 128)), lo[base + 4 * c : base + 4 * c + 4, :])
    base += 4 * z1.shape[0]
    h2, width2 = sizes[2]
    wq = up128(width1)
    tmp[0:3, :wq] = rows_sum(top1, 4, 3)
    tmp[3:6, :wq] = rows_sum(end1, 12, 3)
    edge = cols_coarsen(tmp[:, :wq], width1)
    for c in range(z2.shape[0]):
        part = edge[:, 128 * c : 128 * c + 128]
        row0, end = part[1:2], part[3:4]
        at = base + h2 * c
        w2[c, 0:h2, :] = jnp.where(first, jnp.broadcast_to(row0, (h2, 128)), up[at : at + h2, :])
        w2[c, h2 : 2 * h2, :] = z2[c]
        w2[c, 2 * h2 : 3 * h2, :] = jnp.where(last, jnp.broadcast_to(end, (h2, 128)), lo[at : at + h2, :])
        w2[c, h2 - 1 : h2, :] = jnp.where(first, row0, part[0:1])
        w2[c, h2 : h2 + 2, :] = part[1:3]
        w2[c, 2 * h2 - 1 : 2 * h2, :] = end
        w2[c, 2 * h2 : 2 * h2 + 1, :] = jnp.where(last, end, part[4:5])
        w2[c, 2 * h2 + 1 : 2 * h2 + 2, :] = jnp.where(last, end, part[5:6])
    h3, width3 = sizes[3]
    wq = up128(width2)
    v = cols_coarsen(pad_rows(rows_sum(w2, h2 - 14, h3 + 11)), width2)
    row = row_of(v) - 6
    v = jnp.where(first & (row < 0), v[6:7], jnp.where(last & (row >= h3), v[h3 + 5 : h3 + 6], v))
    w3[0] = v
    h4, width4 = sizes[4]
    v = pad_rows(rows_sum(w3, 0, h4 + 4))
    row = row_of(v) - 2
    column = lane_of(v) & 63
    for i, step in enumerate((0, -1, 1)):
        at = 2 * jnp.clip(column + step, 0, width4 - 1)
        taps = [lanes(v, jnp.clip(at + tap, 0, width3 - 1)) for tap in (-2, -1, 0, 1, 2)]
        level = (taps[0] + taps[4]) * 0.0625 + (taps[1] + taps[3]) * 0.25 + taps[2] * 0.375
        level = jnp.where(first & (row < 0), level[2:3], jnp.where(last & (row >= h4), level[h4 + 1 : h4 + 2], level))
        w4[i, 0:8, :] = level
        w4[i, 8:16, :] = level

    totals = []

    def add(k, slope, bend, kept):
        kept = kept & (lane_of(slope) < sizes[k][1])
        totals.append((acc_ref[k] + fold(jnp.where(kept, slope, 0.0)),
                       acc_ref[LEVELS + k] + fold(jnp.where(kept, bend * bend, 0.0))))

    def ends(top, top_at, bottom, bottom_at):
        a, b = take(top, top_at, 8), take(bottom, bottom_at - 4, 8)
        return jnp.where(row_of(a) < 4, a, b)

    slope, bend = relief(*(ends(top0, 7 + i, end0, 11 + i) for i in range(3)), width0, 1.0)
    for ref, v in ((s0_ref, slope), (b0_ref, bend)):
        ref[0:4, :] = v[0:4]
        ref[h0 - 4 : h0, :] = v[4:8]
    add(0, slope, bend, (row_of(slope) == 0) | (row_of(slope) == 7))
    for k, top, bottom, top_at, bottom_at, t, u in ((1, top1, end1, 7, 13, t1, u1), (2, w2, w2, h2 - 1, 2 * h2 - 3, t2, u2)):
        h, width = sizes[k]
        slope, bend = relief(*(ends(top, top_at - 1 + i, bottom, bottom_at - 1 + i) for i in range(3)), width, float(2**k))
        add(k, slope, bend, (row_of(slope) > 0) & (row_of(slope) < 7))
        for field, v in enumerate((slope, bend)):
            row = row_of(v)
            v = jnp.where(first & (row == 0), v[1:2], jnp.where(last & (row == 7), v[6:7], v))
            for c, part in enumerate(cols_refine(split(v), k, width, t.shape[1])):
                t[field, c, 0:4, :] = part[0:4]
                t[field, c, h - 2 : h + 2, :] = part[4:8]
            rows_refine(t, u, field, k, h)
    for k, z, at, f in ((3, w3, 5, f3), (4, w4, 1, f4)):
        h, width = sizes[k]
        rows = -(-(h + 2) // 8) * 8
        if k == 3:
            slope, bend = relief(take(z, at - 1, rows), take(z, at, rows), take(z, at + 1, rows), width, float(2**k))
        else:
            around = [[z[i, at + j : at + j + rows, :] for j in (-1, 0, 1)] for i in range(3)]
            slope, bend = relief(*around[0], width, float(2**k), around[1:])
        row = row_of(slope) - 1
        if k == 3:
            add(k, slope, bend, (row >= 0) & (row < h))
        else:
            kept = (row >= 0) & (row < h)
            slope4, bend4 = jnp.where(kept, slope, 0.0), jnp.where(kept, bend * bend, 0.0)
        for field, v in enumerate((slope, bend)):
            v = jnp.where(first & (row < 0), v[1:2], jnp.where(last & (row >= h), v[h : h + 1], v))
            f[field, 0:rows, :] = jnp.where(row <= h, v, 0.0)
    table = jnp.zeros((8, 128), f32)
    lane = lane_of(table)
    for k, pair in enumerate(totals):
        for field, v in enumerate(pair):
            table = jnp.where(lane == 64 * field + width4 + k, jnp.sum(v, axis=1, keepdims=True), table)
    table = jnp.where((lane & 63) < width4, jnp.where(lane < 64, slope4, bend4), table)
    line = jnp.sum(table, axis=0, keepdims=True)
    sum_ref[...] = jnp.broadcast_to(line.reshape(1, 1, 128), sum_ref.shape)


def pad_rows(v):
    short = -v.shape[0] % 8
    return jnp.concatenate([v, jnp.zeros((short, v.shape[1]), f32)], axis=0) if short else v


def cols_refine(blocks, k, width, count):
    f = 1 << k
    lane = lax.broadcasted_iota(jnp.int32, blocks[0].shape, 1)
    west_side = (lane & (f - 1)) < f // 2
    pos = ((lane & (f - 1)).astype(f32) + 0.5) * (1.0 / f)
    other = jnp.abs(pos - 0.5)
    out = []
    for c in range(count):
        at, first = divmod((128 * c) >> k, 128)
        centre = first + (lane >> k)
        near = jnp.where(west_side, centre - 1, centre + 1)
        if c == 0:
            near = jnp.maximum(near, 0)
        if c == count - 1:
            near = jnp.minimum(near, width - 1 - 128 * at)
        near = near & 127
        side = lanes(blocks[at], near)
        if c and first == 0:
            side = jnp.where(lane < f // 2, lanes(blocks[at - 1], near), side)
        if c < count - 1 and first + (128 >> k) == 128:
            side = jnp.where(lane >= 128 - f // 2, lanes(blocks[at + 1], near), side)
        out.append((1.0 - other) * lanes(blocks[at], centre) + other * side)
    return out


def finish_kernel(sizes, cells, v_ref, s0, b0, u1, u2, f3, f4, slope_ref, bend_ref, t3, t4, u3, u4, slope_buf, bend_buf, sems):
    h0, width0 = sizes[0]
    count = width0 // 128
    sums = jnp.sum(v_ref[...], axis=0, keepdims=True)
    lane = lax.broadcasted_iota(jnp.int32, (1, 128), 1)
    slot = sizes[LEVELS][1]
    number = jnp.ones((1, 128), f32)
    for k, c in enumerate(cells):
        number = jnp.where((lane & 63) == slot + k, float(c), number)
    last = [
        jnp.sum(jnp.where((lane >= at) & (lane < at + slot), sums, 0.0), axis=1, keepdims=True) for at in (0, 64)
    ]
    sums = jnp.where(lane == slot + LEVELS, last[0], jnp.where(lane == 64 + slot + LEVELS, last[1], sums))
    mean = sums / number
    scale = jnp.where(lane < 64, 1.0 / (mean + EPS), 1.0 / jnp.sqrt(mean + EPS))
    for field in range(2):
        for k, f, t in ((4, f4, t4), (3, f3, t3)):
            for at in range(0, f.shape[1], 8):
                for c, v in enumerate(cols_refine(split(f[field, at : at + 8, :]), k, sizes[k][1], count)):
                    t[field, c, at : at + 8, :] = v
        rows_refine(t3, u3, field, 3, sizes[3][0])
        pos = (lax.broadcasted_iota(jnp.int32, (8, 128), 0).astype(f32) + 0.5) * 0.0625
        for c in range(count):
            for at in range(0, h0, 16):
                a, b, d = (jnp.broadcast_to(t4[field, c, at // 16 + i : at // 16 + i + 1, :], (8, 128)) for i in range(3))
                u4[field, c, at : at + 8, :] = (0.5 - pos) * a + (0.5 + pos) * b
                u4[field, c, at + 8 : at + 16, :] = (1.0 - pos) * b + pos * d
    copies = []
    for field, (base, buf, out) in enumerate(((s0, slope_buf, slope_ref), (b0, bend_buf, bend_ref))):
        weights = [jnp.broadcast_to(scale[:, i : i + 1], (8, 128)) for i in range(64 * field + slot, 64 * field + slot + LEVELS + 1)]
        for part in range(2):
            begin, end = part * h0 // 2, (part + 1) * h0 // 2
            for c in range(count):
                for at in range(begin, end, 8):
                    total = base[at : at + 8, 128 * c : 128 * c + 128] * weights[0]
                    for weight, u in zip(weights[1:], (u1, u2, u3, u4)):
                        total = total + u[field, c, at : at + 8, :] * weight
                    buf[at : at + 8, 128 * c : 128 * c + 128] = total
            rows = pl.ds(begin, end - begin)
            copy = pltpu.make_async_copy(buf.at[rows], out.at[rows], sems.at[2 * field + part])
            copy.start()
            copies.append(copy)
    for copy in copies:
        copy.wait()


def halo_pairs(count):
    both = lambda pairs: [(a, b) for a, b in pairs] + [(b, a) for a, b in pairs]
    even = [(i, i + 1) for i in range(0, count - 1, 2)]
    odd = [(i, i + 1) for i in range(1, count - 1, 2)]
    if count % 2 or count < 8:
        return both(even), both(odd), None, 0
    mid = count * 13 // 16 & ~1
    second = [e for e in odd if e[1] != mid] + [(0, mid - 1), (mid, count - 1)]
    third = [e for e in even if e[0] not in (mid - 2, mid)] + [(mid - 1, mid), (mid - 2, mid + 1)]
    return both(even), both(second), both(third), mid


VM = pl.BlockSpec(memory_space=pltpu.VMEM)
ANY = pl.BlockSpec(memory_space=pl.ANY)


def call(kernel, outs, scratch=(), in_specs=None, out_specs=None, flops=10**6, limit=8 << 20, aliases=None):
    return lambda *args: pl.pallas_call(
        kernel,
        out_shape=[jax.ShapeDtypeStruct(s, f32) for s in outs],
        in_specs=in_specs or [VM] * len(args),
        out_specs=out_specs or [VM] * len(outs),
        scratch_shapes=list(scratch),
        input_output_aliases=aliases or {},
        compiler_params=pltpu.CompilerParams(vmem_limit_bytes=limit),
        cost_estimate=pl.CostEstimate(flops=flops, bytes_accessed=1 << 19, transcendentals=0),
    )(*args)


def local(grid):
    h0, width0 = grid.shape
    count = lax.axis_size("rows")
    sizes = [(h0 >> k, width0 >> k) for k in range(LEVELS + 1)]

    def blocks(rows, width):
        return (up128(width) // 128, -(-rows // 8) * 8, 128)

    z_shapes = [blocks(*size) for size in sizes]
    msg = (4 * z_shapes[0][0] + 4 * z_shapes[1][0] + sizes[2][0] * z_shapes[2][0], 128)
    m1, m2, z0, z1, z2 = call(
        functools.partial(pyramid_kernel, sizes),
        [msg, msg] + z_shapes[:3],
        [pltpu.VMEM((h0 // 2, width0), f32), pltpu.SemaphoreType.DMA((z_shapes[0][0],))],
        in_specs=[pl.BlockSpec(memory_space=pltpu.HBM)],
    )(pltpu.with_memory_space_constraint(grid, pltpu.HBM))
    pairs1, pairs2, pairs3, mid = halo_pairs(count)
    r2 = lax.ppermute(m2, "rows", pairs2)
    r1 = lax.ppermute(m1, "rows", pairs1)
    r3 = lax.ppermute(m2, "rows", pairs3) if mid else m2
    acc = (2 * LEVELS, 8, 128)
    fine = [(2, z_shapes[0][0], -(-(h + 2) // 8) * 8, 128) for h, _ in sizes[1:]]
    whole = (2, *z_shapes[0])
    f_shapes = fine[:2] + [whole] * 2 + [(2, -(-(h + 2) // 8) * 8, up128(w)) for h, w in sizes[3:]]
    s0, b0, t1, t2, sums = call(
        functools.partial(inner_kernel, sizes), [grid.shape, grid.shape] + fine[:2] + [acc], flops=10**8
    )(z0, z1, z2)
    s0, b0, _, _, u1, u2, f3, f4, sums = call(
        functools.partial(edge_kernel, sizes, mid),
        [grid.shape, grid.shape] + f_shapes + [(count, 1, 128)],
        [pltpu.VMEM(msg, f32)] * 2
        + [pltpu.VMEM(blocks(rows, sizes[k][1]), f32) for k in range(2) for rows in (24, 24)]
        + [pltpu.VMEM(blocks(3 * sizes[2][0], sizes[2][1]), f32)]
        + [pltpu.VMEM(blocks(sizes[3][0] + 16, sizes[3][1]), f32)]
        + [pltpu.VMEM((3, 16, 128), f32), pltpu.VMEM((8, width0), f32)],
        aliases={7: 0, 8: 1, 9: 2, 10: 3},
    )(z0, z1, z2, r1, r2, r3, sums, s0, b0, t1, t2)
    seen = lax.all_to_all(sums, "rows", 0, 0, tiled=True).reshape(count, 128)
    cells = [count * h * w for h, w in sizes]
    return tuple(
        call(
            functools.partial(finish_kernel, sizes, cells),
            [grid.shape, grid.shape],
            [pltpu.VMEM(v, f32) for v in fine[2:] + [whole] * 2 + [grid.shape] * 2] + [pltpu.SemaphoreType.DMA((4,))],
            out_specs=[ANY, ANY],
        )(seen, s0, b0, u1, u2, f3, f4)
    )


def solution(mesh):
    return jax.shard_map(
        local,
        mesh=mesh,
        in_specs=(P("rows", None),),
        out_specs=(P("rows", None), P("rows", None)),
        check_vma=False,
    )
```

```python
import functools

import jax
import jax.numpy as jnp
from jax import lax
from jax.experimental import pallas as pl
from jax.experimental.pallas import tpu as pltpu
from jax.sharding import PartitionSpec as P

LEVELS = 4
EPS = 1e-06
f32 = jnp.float32
ATAN = (
    1.0,
    -0.3333314528,
    0.1999355085,
    -0.1420889944,
    0.1065626393,
    -0.0752896400,
    0.0429096138,
    -0.0161657367,
    0.0028662257,
)


def up128(n):
    return -(-n // 128) * 128


def lane_of(v):
    return lax.broadcasted_iota(jnp.int32, v.shape, 1)


def row_of(v):
    return lax.broadcasted_iota(jnp.int32, v.shape, 0)


def west(v):
    return jnp.where(lane_of(v) == 0, v, pltpu.roll(v, 1, 1))


def east(v, width):
    return jnp.where(lane_of(v) == width - 1, v, pltpu.roll(v, v.shape[1] - 1, 1))


def take(ref, at, count):
    return jnp.concatenate([ref[c, at : at + count, :] for c in range(ref.shape[0])], axis=1)


def store(ref, at, v):
    for c in range(ref.shape[0]):
        ref[c, at : at + v.shape[0], :] = v[:, 128 * c : 128 * c + 128]


def head(a, b, c):
    return (a * 0.0625 + b * 0.25) + c * 0.375


def tail(d, e):
    return d * 0.25 + e * 0.0625


def rows_sum(ref, start, count):
    out = []
    for c in range(ref.shape[0]):
        part = [ref[c, pl.ds(start + a, count, 2), :] for a in range(5)]
        out.append(head(*part[:3]) + tail(*part[3:]))
    return jnp.concatenate(out, axis=1)


def lanes(v, at):
    return jnp.take_along_axis(v, at, axis=1, mode="promise_in_bounds")


def split(v):
    return [v[:, at : at + 128] for at in range(0, v.shape[1], 128)]


def cols_coarsen(v, width):
    blocks = split(v)
    lane = lax.broadcasted_iota(jnp.int32, blocks[0].shape, 1)
    patterns = [(2 * lane + tap + 128) & 127 for tap in (-2, -1, 0, 1, 2)]
    found = [[lanes(v, at) for v in blocks] for at in patterns]
    out = []
    for c in range(0, len(blocks), 2):
        taps = []
        for tap, got in zip((-2, -1, 0, 1, 2), found):
            part = got[c]
            if c + 1 < len(blocks):
                part = jnp.where(2 * lane + tap < 128, part, got[c + 1])
            if tap < 0 and c:
                part = jnp.where(lane == 0, got[c - 1], part)
            if tap > 1 and c + 2 < len(blocks):
                part = jnp.where(lane == 127, got[c + 2], part)
            taps.append(part)
        if c == 0:
            taps[0] = jnp.where(lane == 0, taps[2], taps[0])
            taps[1] = jnp.where(lane == 0, taps[2], taps[1])
        taps[4] = jnp.where(lane == width // 2 - 1 - 64 * c, taps[3], taps[4])
        out.append((taps[0] + taps[4]) * 0.0625 + (taps[1] + taps[3]) * 0.25 + taps[2] * 0.375)
    return out[0] if len(out) == 1 else jnp.concatenate(out, axis=1)


def pyramid_kernel(sizes, x_ref, m1_ref, m2_ref, z0, z1, z2, tmp, below, above, sems):
    copies = [
        pltpu.make_async_copy(x_ref.at[:, pl.ds(128 * c, 128)], z0.at[c], sems.at[c]) for c in range(z0.shape[0])
    ]
    for copy in copies:
        copy.start()
    odd = lax.rem(lax.axis_index("rows"), 2) == 1
    h = sizes[0][0]
    for copy in copies:
        copy.wait()

    for c in range(z0.shape[0]):
        above[3 * c : 3 * c + 3, :] = z0[c, 0:3, :]
        w = [z0[c, h - 4 + i : h - 3 + i, :] for i in range(4)]
        below[3 * c : 3 * c + 1, :] = head(*w[:3])
        below[3 * c + 1 : 3 * c + 2, :] = w[2] * 0.0625 + w[3] * 0.25
        below[3 * c + 2 : 3 * c + 3, :] = w[3]
    row = 3 * z0.shape[0]
    for k, z in ((0, z1), (1, z2)):
        half, wp = sizes[k + 1][0], up128(sizes[k][1])
        low = k + 1
        tmp[low : half - 1, :wp] = rows_sum((z0, z1)[k], 2 * low - 2, half - 1 - low)
        store(z, 0, cols_coarsen(tmp[0:half, :wp], sizes[k][1]))
    h1, h2 = sizes[1][0], sizes[2][0]
    at = row
    for c in range(z1.shape[0]):
        above[row + 4 * c : row + 4 * c + 4, :] = z1[c, 1:5, :]
        w = [z1[c, h1 - 4 + i : h1 - 3 + i, :] for i in range(3)]
        below[at : at + 1, :] = head(*w)
        below[at + 1 : at + 2, :] = w[2]
        at += 2
    row += 4 * z1.shape[0]
    for c in range(z2.shape[0]):
        above[row + 9 * c : row + 9 * c + 9, :] = z2[c, 2:11, :]
        below[at + 13 * c : at + 13 * c + 13, :] = z2[c, h2 - 14 : h2 - 1, :]
    m1_ref[...] = jnp.where(odd, above[...], below[...])
    m2_ref[...] = jnp.where(odd, below[...], above[...])


def relief(upper, middle, lower, width, spacing, sides=None):
    diff = lower - upper
    if sides is None:
        tall = lower + upper + 2.0 * middle
        (d_w, m_w, t_w), (d_e, m_e, t_e) = ([west(v) for v in (diff, middle, tall)], [east(v, width) for v in (diff, middle, tall)])
    else:
        (d_w, m_w, t_w), (d_e, m_e, t_e) = ((c - a, b, c + a + 2.0 * b) for a, b, c in sides)
    p = (t_e - t_w) * (1.0 / (8.0 * spacing))
    q = (d_e + d_w + 2.0 * diff) * (1.0 / (8.0 * spacing))
    inv = 1.0 / (spacing * spacing)
    r = ((m_e - middle) - (middle - m_w)) * inv
    t = ((lower - middle) - (middle - upper)) * inv
    u = (d_e - d_w) * (0.25 * inv)
    pp, qq = p * p, q * q
    steep = pp + qq
    base = 1.0 + steep
    root = jnp.sqrt(base)
    y = jnp.sqrt(steep) / (1.0 + root)
    y2 = y * y
    acc = ATAN[-1]
    for c in ATAN[-2::-1]:
        acc = acc * y2 + c
    slope = 2.0 * y * acc
    bend = -(pp * r + 2.0 * (p * q) * u + qq * t) / (base * root)
    return slope, bend


def fold(v):
    total = None
    for row in range(0, v.shape[0], 8):
        for at in range(0, v.shape[1], 128):
            part = v[row : row + 8, at : at + 128]
            total = part if total is None else total + part
    return total


def inner_kernel(sizes, z0, z1, z2, s0_ref, b0_ref, t1, t2, acc_ref):
    for k, z in enumerate((z0, z1, z2)):
        h, width = sizes[k]
        s_sum = b_sum = None
        for at in range(0, h, 8):
            middle = take(z, at, 8)
            upper = take(z, at - 1, 8) if at else pltpu.roll(middle, 1, 0)
            lower = take(z, at + 1, 8) if at < h - 8 else pltpu.roll(middle, 7, 0)
            slope, bend = relief(upper, middle, lower, width, float(2**k))
            if k == 0:
                s0_ref[at : at + 8, :] = slope
                b0_ref[at : at + 8, :] = bend
            else:
                t = (t1, t2)[k - 1]
                for field, v in enumerate((slope, bend)):
                    for c, part in enumerate(cols_refine(split(v), k, width, t.shape[1])):
                        t[field, c, at + 1 : at + 9, :] = part
            skip = 3 if k else 1
            if at == 0 or at == h - 8 or width % 128:
                row = row_of(slope) + at
                kept = (row >= skip) & (row < h - skip) & (lane_of(slope) < width)
                slope, bend = jnp.where(kept, slope, 0.0), jnp.where(kept, bend, 0.0)
            fs, fb = fold(slope), fold(bend * bend)
            s_sum = fs if at == 0 else s_sum + fs
            b_sum = fb if at == 0 else b_sum + fb
        acc_ref[k] = s_sum
        acc_ref[LEVELS + k] = b_sum
    for k in range(3, LEVELS):
        acc_ref[k] = jnp.zeros((8, 128), f32)
        acc_ref[LEVELS + k] = jnp.zeros((8, 128), f32)


def rows_refine(t, u, field, k, height):
    f = 1 << k
    for c in range(t.shape[1]):
        for at in range(0, height, 8):
            before, centre, after = (t[field, c, at + i : at + i + 8, :] for i in range(3))
            for s in range(f):
                near = abs((s + 0.5) / f - 0.5)
                u[field, c, pl.ds(f * at + s, 8, f), :] = (1.0 - near) * centre + near * (before if s < f // 2 else after)


def edge_kernel(sizes, mid, z0, z1, z2, r1_ref, r2_ref, r3_ref, acc_ref, s0_in, b0_in, t1_in, t2_in,
                s0_ref, b0_ref, t1, t2, u1, u2, f3, f4, sum_ref, up, lo, top0, end0, top1, end1, w2, w3, w4, tmp):
    me = lax.axis_index("rows")
    odd = lax.rem(me, 2) == 1
    first, last = me == 0, me == lax.axis_size("rows") - 1
    r1, r2 = r1_ref[...], r2_ref[...]
    if mid:
        r2 = jnp.where((me == mid) | (me == mid - 1), r3_ref[...], r2)
    up[...] = jnp.where(odd, r1, r2)
    lo[...] = jnp.where(odd, r2, r1)

    h0, width0 = sizes[0]
    for c in range(z0.shape[0]):
        block = slice(128 * c, 128 * c + 128)
        w = [z0[c, i : i + 1, :] for i in range(3)]
        top0[c, 8:16, :] = z0[c, 0:8, :]
        top0[c, 7:8, :] = jnp.where(first, w[0], up[3 * c + 2 : 3 * c + 3, :])
        tmp[0:1, block] = up[3 * c : 3 * c + 1, :] + tail(up[3 * c + 2 : 3 * c + 3, :], w[0])
        start = jnp.where(first, w[0] * 0.0625 + w[0] * 0.25, up[3 * c + 1 : 3 * c + 2, :])
        tmp[1:2, block] = (start + w[0] * 0.375) + tail(w[1], w[2])
        end0[c, 8:16, :] = z0[c, h0 - 8 : h0, :]
        end0[c, 16:19, :] = jnp.where(last, jnp.broadcast_to(z0[c, h0 - 1 : h0, :], (3, 128)), lo[3 * c : 3 * c + 3, :])
    base = 3 * z0.shape[0]
    h1, width1 = sizes[1]
    tmp[3:5, :] = rows_sum(end0, 12, 2)
    edge = cols_coarsen(tmp[...], width0)
    for c in range(z1.shape[0]):
        part = edge[:, 128 * c : 128 * c + 128]
        row0, end = part[1:2], part[3:4]
        top1[c, 8:16, :] = z1[c, 0:8, :]
        top1[c, 8:9, :] = row0
        top1[c, 7:8, :] = jnp.where(first, row0, part[0:1])
        top1[c, 6:7, :] = jnp.where(first, row0, up[base + 2 * c + 1 : base + 2 * c + 2, :])
        end1[c, 8:16, :] = z1[c, h1 - 8 : h1, :]
        end1[c, 15:16, :] = end
        end1[c, 16:17, :] = jnp.where(last, end, part[4:5])
        end1[c, 17:21, :] = jnp.where(last, jnp.broadcast_to(end, (4, 128)), lo[base + 4 * c : base + 4 * c + 4, :])
    h2, width2 = sizes[2]
    wq = up128(width1)
    for c in range(z1.shape[0]):
        tmp[0:1, 128 * c : 128 * c + 128] = up[base + 2 * c : base + 2 * c + 1, :] + tail(top1[c, 7:8, :], top1[c, 8:9, :])
    tmp[1:3, :wq] = rows_sum(top1, 6, 2)
    tmp[3:6, :wq] = rows_sum(end1, 12, 3)
    edge = cols_coarsen(tmp[:, :wq], width1)
    for c in range(z2.shape[0]):
        part = edge[:, 128 * c : 128 * c + 128]
        row0, end = part[1:2], part[3:4]
        at = base + 2 * z1.shape[0] + 13 * c
        w2[c, h2 - 14 : h2 - 1, :] = jnp.where(first, jnp.broadcast_to(row0, (13, 128)), up[at : at + 13, :])
        w2[c, h2 : 2 * h2, :] = z2[c]
        at = base + 4 * z1.shape[0] + 9 * c
        w2[c, 2 * h2 + 2 : 2 * h2 + 11, :] = jnp.where(last, jnp.broadcast_to(end, (9, 128)), lo[at : at + 9, :])
        w2[c, h2 - 1 : h2, :] = jnp.where(first, row0, part[0:1])
        w2[c, h2 : h2 + 2, :] = part[1:3]
        w2[c, 2 * h2 - 1 : 2 * h2, :] = end
        w2[c, 2 * h2 : 2 * h2 + 1, :] = jnp.where(last, end, part[4:5])
        w2[c, 2 * h2 + 1 : 2 * h2 + 2, :] = jnp.where(last, end, part[5:6])
    h3, width3 = sizes[3]
    wq = up128(width2)
    v = cols_coarsen(pad_rows(rows_sum(w2, h2 - 14, h3 + 11)), width2)
    row = row_of(v) - 6
    v = jnp.where(first & (row < 0), v[6:7], jnp.where(last & (row >= h3), v[h3 + 5 : h3 + 6], v))
    w3[0] = v
    h4, width4 = sizes[4]
    v = pad_rows(rows_sum(w3, 0, h4 + 4))
    row = row_of(v) - 2
    column = lane_of(v) & 63
    for i, step in enumerate((0, -1, 1)):
        at = 2 * jnp.clip(column + step, 0, width4 - 1)
        taps = [lanes(v, jnp.clip(at + tap, 0, width3 - 1)) for tap in (-2, -1, 0, 1, 2)]
        level = (taps[0] + taps[4]) * 0.0625 + (taps[1] + taps[3]) * 0.25 + taps[2] * 0.375
        level = jnp.where(first & (row < 0), level[2:3], jnp.where(last & (row >= h4), level[h4 + 1 : h4 + 2], level))
        w4[i, 0:8, :] = level
        w4[i, 8:16, :] = level

    totals = []

    def add(k, slope, bend, kept):
        kept = kept & (lane_of(slope) < sizes[k][1])
        totals.append((acc_ref[k] + fold(jnp.where(kept, slope, 0.0)),
                       acc_ref[LEVELS + k] + fold(jnp.where(kept, bend * bend, 0.0))))

    def ends(top, top_at, bottom, bottom_at):
        a, b = take(top, top_at, 8), take(bottom, bottom_at - 4, 8)
        return jnp.where(row_of(a) < 4, a, b)

    slope, bend = relief(*(ends(top0, 7 + i, end0, 11 + i) for i in range(3)), width0, 1.0)
    for ref, v in ((s0_ref, slope), (b0_ref, bend)):
        ref[0:4, :] = v[0:4]
        ref[h0 - 4 : h0, :] = v[4:8]
    add(0, slope, bend, (row_of(slope) == 0) | (row_of(slope) == 7))
    for k, top, bottom, top_at, bottom_at, t, u in ((1, top1, end1, 7, 13, t1, u1), (2, w2, w2, h2 - 1, 2 * h2 - 3, t2, u2)):
        h, width = sizes[k]
        slope, bend = relief(*(ends(top, top_at - 1 + i, bottom, bottom_at - 1 + i) for i in range(3)), width, float(2**k))
        add(k, slope, bend, (row_of(slope) > 0) & (row_of(slope) < 7))
        for field, v in enumerate((slope, bend)):
            row = row_of(v)
            v = jnp.where(first & (row == 0), v[1:2], jnp.where(last & (row == 7), v[6:7], v))
            for c, part in enumerate(cols_refine(split(v), k, width, t.shape[1])):
                t[field, c, 0:4, :] = part[0:4]
                t[field, c, h - 2 : h + 2, :] = part[4:8]
            rows_refine(t, u, field, k, h)
    for k, z, at, f in ((3, w3, 5, f3), (4, w4, 1, f4)):
        h, width = sizes[k]
        rows = -(-(h + 2) // 8) * 8
        if k == 3:
            slope, bend = relief(take(z, at - 1, rows), take(z, at, rows), take(z, at + 1, rows), width, float(2**k))
        else:
            around = [[z[i, at + j : at + j + rows, :] for j in (-1, 0, 1)] for i in range(3)]
            slope, bend = relief(*around[0], width, float(2**k), around[1:])
        row = row_of(slope) - 1
        if k == 3:
            add(k, slope, bend, (row >= 0) & (row < h))
        else:
            kept = (row >= 0) & (row < h)
            slope4, bend4 = jnp.where(kept, slope, 0.0), jnp.where(kept, bend * bend, 0.0)
        for field, v in enumerate((slope, bend)):
            v = jnp.where(first & (row < 0), v[1:2], jnp.where(last & (row >= h), v[h : h + 1], v))
            f[field, 0:rows, :] = jnp.where(row <= h, v, 0.0)
    table = jnp.zeros((8, 128), f32)
    lane = lane_of(table)
    for k, pair in enumerate(totals):
        for field, v in enumerate(pair):
            table = jnp.where(lane == 64 * field + width4 + k, jnp.sum(v, axis=1, keepdims=True), table)
    table = jnp.where((lane & 63) < width4, jnp.where(lane < 64, slope4, bend4), table)
    line = jnp.sum(table, axis=0, keepdims=True)
    sum_ref[...] = jnp.broadcast_to(line.reshape(1, 1, 128), sum_ref.shape)


def pad_rows(v):
    short = -v.shape[0] % 8
    return jnp.concatenate([v, jnp.zeros((short, v.shape[1]), f32)], axis=0) if short else v


def cols_refine(blocks, k, width, count):
    f = 1 << k
    lane = lax.broadcasted_iota(jnp.int32, blocks[0].shape, 1)
    west_side = (lane & (f - 1)) < f // 2
    pos = ((lane & (f - 1)).astype(f32) + 0.5) * (1.0 / f)
    other = jnp.abs(pos - 0.5)
    out = []
    for c in range(count):
        at, first = divmod((128 * c) >> k, 128)
        centre = first + (lane >> k)
        near = jnp.where(west_side, centre - 1, centre + 1)
        if c == 0:
            near = jnp.maximum(near, 0)
        if c == count - 1:
            near = jnp.minimum(near, width - 1 - 128 * at)
        near = near & 127
        side = lanes(blocks[at], near)
        if c and first == 0:
            side = jnp.where(lane < f // 2, lanes(blocks[at - 1], near), side)
        if c < count - 1 and first + (128 >> k) == 128:
            side = jnp.where(lane >= 128 - f // 2, lanes(blocks[at + 1], near), side)
        out.append((1.0 - other) * lanes(blocks[at], centre) + other * side)
    return out


def finish_kernel(sizes, cells, v_ref, s0, b0, u1, u2, f3, f4, slope_ref, bend_ref, t3, t4, u3, u4, slope_buf, bend_buf, sems):
    h0, width0 = sizes[0]
    count = width0 // 128
    sums = jnp.sum(v_ref[...], axis=0, keepdims=True)
    lane = lax.broadcasted_iota(jnp.int32, (1, 128), 1)
    slot = sizes[LEVELS][1]
    number = jnp.ones((1, 128), f32)
    for k, c in enumerate(cells):
        number = jnp.where((lane & 63) == slot + k, float(c), number)
    last = [
        jnp.sum(jnp.where((lane >= at) & (lane < at + slot), sums, 0.0), axis=1, keepdims=True) for at in (0, 64)
    ]
    sums = jnp.where(lane == slot + LEVELS, last[0], jnp.where(lane == 64 + slot + LEVELS, last[1], sums))
    mean = sums / number
    scale = jnp.where(lane < 64, 1.0 / (mean + EPS), 1.0 / jnp.sqrt(mean + EPS))
    for field in range(2):
        for k, f, t in ((4, f4, t4), (3, f3, t3)):
            for at in range(0, f.shape[1], 8):
                for c, v in enumerate(cols_refine(split(f[field, at : at + 8, :]), k, sizes[k][1], count)):
                    t[field, c, at : at + 8, :] = v
        rows_refine(t3, u3, field, 3, sizes[3][0])
        pos = (lax.broadcasted_iota(jnp.int32, (8, 128), 0).astype(f32) + 0.5) * 0.0625
        for c in range(count):
            for at in range(0, h0, 16):
                a, b, d = (jnp.broadcast_to(t4[field, c, at // 16 + i : at // 16 + i + 1, :], (8, 128)) for i in range(3))
                u4[field, c, at : at + 8, :] = (0.5 - pos) * a + (0.5 + pos) * b
                u4[field, c, at + 8 : at + 16, :] = (1.0 - pos) * b + pos * d
    copies = []
    for field, (base, buf, out) in enumerate(((s0, slope_buf, slope_ref), (b0, bend_buf, bend_ref))):
        weights = [jnp.broadcast_to(scale[:, i : i + 1], (8, 128)) for i in range(64 * field + slot, 64 * field + slot + LEVELS + 1)]
        for part in range(2):
            begin, end = part * h0 // 2, (part + 1) * h0 // 2
            for c in range(count):
                for at in range(begin, end, 8):
                    total = base[at : at + 8, 128 * c : 128 * c + 128] * weights[0]
                    for weight, u in zip(weights[1:], (u1, u2, u3, u4)):
                        total = total + u[field, c, at : at + 8, :] * weight
                    buf[at : at + 8, 128 * c : 128 * c + 128] = total
            rows = pl.ds(begin, end - begin)
            copy = pltpu.make_async_copy(buf.at[rows], out.at[rows], sems.at[2 * field + part])
            copy.start()
            copies.append(copy)
    for copy in copies:
        copy.wait()


def halo_pairs(count):
    both = lambda pairs: [(a, b) for a, b in pairs] + [(b, a) for a, b in pairs]
    even = [(i, i + 1) for i in range(0, count - 1, 2)]
    odd = [(i, i + 1) for i in range(1, count - 1, 2)]
    if count % 2 or count < 8:
        return both(even), both(odd), None, 0
    mid = count * 13 // 16 & ~1
    second = [e for e in odd if e[1] != mid] + [(0, mid - 1), (mid, count - 1)]
    third = [e for e in even if e[0] not in (mid - 2, mid)] + [(mid - 1, mid), (mid - 2, mid + 1)]
    return both(even), both(second), both(third), mid


VM = pl.BlockSpec(memory_space=pltpu.VMEM)
ANY = pl.BlockSpec(memory_space=pl.ANY)


def call(kernel, outs, scratch=(), in_specs=None, out_specs=None, flops=10**6, limit=8 << 20, aliases=None):
    return lambda *args: pl.pallas_call(
        kernel,
        out_shape=[jax.ShapeDtypeStruct(s, f32) for s in outs],
        in_specs=in_specs or [VM] * len(args),
        out_specs=out_specs or [VM] * len(outs),
        scratch_shapes=list(scratch),
        input_output_aliases=aliases or {},
        compiler_params=pltpu.CompilerParams(vmem_limit_bytes=limit),
        cost_estimate=pl.CostEstimate(flops=flops, bytes_accessed=1 << 19, transcendentals=0),
    )(*args)


def local(grid):
    h0, width0 = grid.shape
    count = lax.axis_size("rows")
    sizes = [(h0 >> k, width0 >> k) for k in range(LEVELS + 1)]

    def blocks(rows, width):
        return (up128(width) // 128, -(-rows // 8) * 8, 128)

    z_shapes = [blocks(*size) for size in sizes]
    rows = 3 * z_shapes[0][0] + max(2 * z_shapes[1][0] + 13 * z_shapes[2][0], 4 * z_shapes[1][0] + 9 * z_shapes[2][0])
    msg = (-(-rows // 8) * 8, 128)
    m1, m2, z0, z1, z2 = call(
        functools.partial(pyramid_kernel, sizes),
        [msg, msg] + z_shapes[:3],
        [pltpu.VMEM((h0 // 2, width0), f32)] + [pltpu.VMEM(msg, f32)] * 2 + [pltpu.SemaphoreType.DMA((z_shapes[0][0],))],
        in_specs=[pl.BlockSpec(memory_space=pltpu.HBM)],
    )(pltpu.with_memory_space_constraint(grid, pltpu.HBM))
    pairs1, pairs2, pairs3, mid = halo_pairs(count)
    r2 = lax.ppermute(m2, "rows", pairs2)
    r1 = lax.ppermute(m1, "rows", pairs1)
    r3 = lax.ppermute(m2, "rows", pairs3) if mid else m2
    acc = (2 * LEVELS, 8, 128)
    fine = [(2, z_shapes[0][0], -(-(h + 2) // 8) * 8, 128) for h, _ in sizes[1:]]
    whole = (2, *z_shapes[0])
    f_shapes = fine[:2] + [whole] * 2 + [(2, -(-(h + 2) // 8) * 8, up128(w)) for h, w in sizes[3:]]
    s0, b0, t1, t2, sums = call(
        functools.partial(inner_kernel, sizes), [grid.shape, grid.shape] + fine[:2] + [acc], flops=10**8
    )(z0, z1, z2)
    s0, b0, _, _, u1, u2, f3, f4, sums = call(
        functools.partial(edge_kernel, sizes, mid),
        [grid.shape, grid.shape] + f_shapes + [(count, 1, 128)],
        [pltpu.VMEM(msg, f32)] * 2
        + [pltpu.VMEM(blocks(rows, sizes[k][1]), f32) for k in range(2) for rows in (24, 24)]
        + [pltpu.VMEM(blocks(3 * sizes[2][0], sizes[2][1]), f32)]
        + [pltpu.VMEM(blocks(sizes[3][0] + 16, sizes[3][1]), f32)]
        + [pltpu.VMEM((3, 16, 128), f32), pltpu.VMEM((8, width0), f32)],
        aliases={7: 0, 8: 1, 9: 2, 10: 3},
    )(z0, z1, z2, r1, r2, r3, sums, s0, b0, t1, t2)
    seen = lax.all_to_all(sums, "rows", 0, 0, tiled=True).reshape(count, 128)
    cells = [count * h * w for h, w in sizes]
    return tuple(
        call(
            functools.partial(finish_kernel, sizes, cells),
            [grid.shape, grid.shape],
            [pltpu.VMEM(v, f32) for v in fine[2:] + [whole] * 2 + [grid.shape] * 2] + [pltpu.SemaphoreType.DMA((4,))],
            out_specs=[ANY, ANY],
        )(seen, s0, b0, u1, u2, f3, f4)
    )


def solution(mesh):
    return jax.shard_map(
        local,
        mesh=mesh,
        in_specs=(P("rows", None),),
        out_specs=(P("rows", None), P("rows", None)),
        check_vma=False,
    )
```

```python
import functools

import jax
import jax.numpy as jnp
from jax import lax
from jax.experimental import pallas as pl
from jax.experimental.pallas import tpu as pltpu
from jax.sharding import PartitionSpec as P

LEVELS = 4
EPS = 1e-06
f32 = jnp.float32
ATAN = (
    1.0,
    -0.3333314528,
    0.1999355085,
    -0.1420889944,
    0.1065626393,
    -0.0752896400,
    0.0429096138,
    -0.0161657367,
    0.0028662257,
)


def up128(n):
    return -(-n // 128) * 128


def lane_of(v):
    return lax.broadcasted_iota(jnp.int32, v.shape, 1)


def row_of(v):
    return lax.broadcasted_iota(jnp.int32, v.shape, 0)


def west(v):
    return jnp.where(lane_of(v) == 0, v, pltpu.roll(v, 1, 1))


def east(v, width):
    return jnp.where(lane_of(v) == width - 1, v, pltpu.roll(v, v.shape[1] - 1, 1))


def take(ref, at, count):
    return jnp.concatenate([ref[c, at : at + count, :] for c in range(ref.shape[0])], axis=1)


def store(ref, at, v):
    for c in range(ref.shape[0]):
        ref[c, at : at + v.shape[0], :] = v[:, 128 * c : 128 * c + 128]


def head(a, b, c):
    return (a * 0.0625 + b * 0.25) + c * 0.375


def tail(d, e):
    return d * 0.25 + e * 0.0625


def rows_sum(ref, start, count):
    out = []
    for c in range(ref.shape[0]):
        part = [ref[c, pl.ds(start + a, count, 2), :] for a in range(5)]
        out.append(head(*part[:3]) + tail(*part[3:]))
    return jnp.concatenate(out, axis=1)


def lanes(v, at):
    return jnp.take_along_axis(v, at, axis=1, mode="promise_in_bounds")


def split(v):
    return [v[:, at : at + 128] for at in range(0, v.shape[1], 128)]


def cols_coarsen(v, width):
    blocks = split(v)
    lane = lax.broadcasted_iota(jnp.int32, blocks[0].shape, 1)
    patterns = [(2 * lane + tap + 128) & 127 for tap in (-2, -1, 0, 1, 2)]
    found = [[lanes(v, at) for v in blocks] for at in patterns]
    out = []
    for c in range(0, len(blocks), 2):
        taps = []
        for tap, got in zip((-2, -1, 0, 1, 2), found):
            part = got[c]
            if c + 1 < len(blocks):
                part = jnp.where(2 * lane + tap < 128, part, got[c + 1])
            if tap < 0 and c:
                part = jnp.where(lane == 0, got[c - 1], part)
            if tap > 1 and c + 2 < len(blocks):
                part = jnp.where(lane == 127, got[c + 2], part)
            taps.append(part)
        if c == 0:
            taps[0] = jnp.where(lane == 0, taps[2], taps[0])
            taps[1] = jnp.where(lane == 0, taps[2], taps[1])
        taps[4] = jnp.where(lane == width // 2 - 1 - 64 * c, taps[3], taps[4])
        out.append((taps[0] + taps[4]) * 0.0625 + (taps[1] + taps[3]) * 0.25 + taps[2] * 0.375)
    return out[0] if len(out) == 1 else jnp.concatenate(out, axis=1)


def pyramid_kernel(sizes, x_ref, m1_ref, m2_ref, z0, z1, z2, tmp, below, above, sems):
    copies = [
        pltpu.make_async_copy(x_ref.at[:, pl.ds(128 * c, 128)], z0.at[c], sems.at[c]) for c in range(z0.shape[0])
    ]
    for copy in copies:
        copy.start()
    odd = lax.rem(lax.axis_index("rows"), 2) == 1
    h = sizes[0][0]
    for copy in copies:
        copy.wait()

    for c in range(z0.shape[0]):
        above[3 * c : 3 * c + 3, :] = z0[c, 0:3, :]
        w = [z0[c, h - 4 + i : h - 3 + i, :] for i in range(4)]
        below[3 * c : 3 * c + 1, :] = head(*w[:3])
        below[3 * c + 1 : 3 * c + 2, :] = w[2] * 0.0625 + w[3] * 0.25
        below[3 * c + 2 : 3 * c + 3, :] = w[3]
    row = 3 * z0.shape[0]
    for k, z in ((0, z1), (1, z2)):
        half, wp = sizes[k + 1][0], up128(sizes[k][1])
        low = k + 1
        tmp[low : half - 1, :wp] = rows_sum((z0, z1)[k], 2 * low - 2, half - 1 - low)
        store(z, 0, cols_coarsen(tmp[0:half, :wp], sizes[k][1]))
    h1, h2 = sizes[1][0], sizes[2][0]
    at = row
    for c in range(z1.shape[0]):
        above[row + 4 * c : row + 4 * c + 4, :] = z1[c, 1:5, :]
        w = [z1[c, h1 - 4 + i : h1 - 3 + i, :] for i in range(3)]
        below[at : at + 1, :] = head(*w)
        below[at + 1 : at + 2, :] = w[2]
        at += 2
    row += 4 * z1.shape[0]
    for c in range(z2.shape[0]):
        above[row + 9 * c : row + 9 * c + 9, :] = z2[c, 2:11, :]
        below[at + 13 * c : at + 13 * c + 13, :] = z2[c, h2 - 14 : h2 - 1, :]
    m1_ref[...] = jnp.where(odd, above[...], below[...])
    m2_ref[...] = jnp.where(odd, below[...], above[...])


def relief(upper, middle, lower, width, spacing, sides=None):
    diff = lower - upper
    if sides is None:
        tall = lower + upper + 2.0 * middle
        (d_w, m_w, t_w), (d_e, m_e, t_e) = ([west(v) for v in (diff, middle, tall)], [east(v, width) for v in (diff, middle, tall)])
    else:
        (d_w, m_w, t_w), (d_e, m_e, t_e) = ((c - a, b, c + a + 2.0 * b) for a, b, c in sides)
    p = (t_e - t_w) * (1.0 / (8.0 * spacing))
    q = (d_e + d_w + 2.0 * diff) * (1.0 / (8.0 * spacing))
    inv = 1.0 / (spacing * spacing)
    r = ((m_e - middle) - (middle - m_w)) * inv
    t = ((lower - middle) - (middle - upper)) * inv
    u = (d_e - d_w) * (0.25 * inv)
    pp, qq = p * p, q * q
    steep = pp + qq
    base = 1.0 + steep
    root = jnp.sqrt(base)
    y = jnp.sqrt(steep) / (1.0 + root)
    y2 = y * y
    acc = ATAN[-1]
    for c in ATAN[-2::-1]:
        acc = acc * y2 + c
    slope = 2.0 * y * acc
    bend = -(pp * r + 2.0 * (p * q) * u + qq * t) / (base * root)
    return slope, bend


def fold(v):
    total = None
    for row in range(0, v.shape[0], 8):
        for at in range(0, v.shape[1], 128):
            part = v[row : row + 8, at : at + 128]
            total = part if total is None else total + part
    return total


def inner_kernel(sizes, z0, z1, z2, s0_ref, b0_ref, t1, t2, acc_ref):
    for k, z in enumerate((z0, z1, z2)):
        h, width = sizes[k]
        s_sum = b_sum = None
        for at in range(0, h, 8):
            middle = take(z, at, 8)
            upper = take(z, at - 1, 8) if at else pltpu.roll(middle, 1, 0)
            lower = take(z, at + 1, 8) if at < h - 8 else pltpu.roll(middle, 7, 0)
            slope, bend = relief(upper, middle, lower, width, float(2**k))
            if k == 0:
                s0_ref[at : at + 8, :] = slope
                b0_ref[at : at + 8, :] = bend
            else:
                t = (t1, t2)[k - 1]
                for field, v in enumerate((slope, bend)):
                    for c, part in enumerate(cols_refine(split(v), k, width, t.shape[1])):
                        t[field, c, at + 1 : at + 9, :] = part
            skip = 3 if k else 1
            if at == 0 or at == h - 8 or width % 128:
                row = row_of(slope) + at
                kept = (row >= skip) & (row < h - skip) & (lane_of(slope) < width)
                slope, bend = jnp.where(kept, slope, 0.0), jnp.where(kept, bend, 0.0)
            fs, fb = fold(slope), fold(bend * bend)
            s_sum = fs if at == 0 else s_sum + fs
            b_sum = fb if at == 0 else b_sum + fb
        acc_ref[k] = s_sum
        acc_ref[LEVELS + k] = b_sum
    for k in range(3, LEVELS):
        acc_ref[k] = jnp.zeros((8, 128), f32)
        acc_ref[LEVELS + k] = jnp.zeros((8, 128), f32)


def rows_refine(t, u, field, k, height):
    f = 1 << k
    for c in range(t.shape[1]):
        for at in range(0, height, 8):
            before, centre, after = (t[field, c, at + i : at + i + 8, :] for i in range(3))
            for s in range(f):
                near = abs((s + 0.5) / f - 0.5)
                u[field, c, pl.ds(f * at + s, 8, f), :] = (1.0 - near) * centre + near * (before if s < f // 2 else after)


def edge_kernel(sizes, mid, z0, z1, z2, r1_ref, r2_ref, r3_ref, acc_ref, s0_in, b0_in, t1_in, t2_in,
                s0_ref, b0_ref, t1, t2, u1, u2, f3, f4, sum_ref, up, lo, top0, end0, top1, end1, w2, w3, w4, tmp):
    me = lax.axis_index("rows")
    odd = lax.rem(me, 2) == 1
    first, last = me == 0, me == lax.axis_size("rows") - 1
    r1, r2 = r1_ref[...], r2_ref[...]
    if mid:
        r2 = jnp.where((me == mid) | (me == mid - 1), r3_ref[...], r2)
    up[...] = jnp.where(odd, r1, r2)
    lo[...] = jnp.where(odd, r2, r1)

    h0, width0 = sizes[0]
    for c in range(z0.shape[0]):
        block = slice(128 * c, 128 * c + 128)
        w = [z0[c, i : i + 1, :] for i in range(3)]
        top0[c, 8:16, :] = z0[c, 0:8, :]
        top0[c, 7:8, :] = jnp.where(first, w[0], up[3 * c + 2 : 3 * c + 3, :])
        tmp[0:1, block] = up[3 * c : 3 * c + 1, :] + tail(up[3 * c + 2 : 3 * c + 3, :], w[0])
        start = jnp.where(first, w[0] * 0.0625 + w[0] * 0.25, up[3 * c + 1 : 3 * c + 2, :])
        tmp[1:2, block] = (start + w[0] * 0.375) + tail(w[1], w[2])
        end0[c, 8:16, :] = z0[c, h0 - 8 : h0, :]
        end0[c, 16:19, :] = jnp.where(last, jnp.broadcast_to(z0[c, h0 - 1 : h0, :], (3, 128)), lo[3 * c : 3 * c + 3, :])
    base = 3 * z0.shape[0]
    h1, width1 = sizes[1]
    tmp[3:5, :] = rows_sum(end0, 12, 2)
    edge = cols_coarsen(tmp[...], width0)
    for c in range(z1.shape[0]):
        part = edge[:, 128 * c : 128 * c + 128]
        row0, end = part[1:2], part[3:4]
        top1[c, 8:16, :] = z1[c, 0:8, :]
        top1[c, 8:9, :] = row0
        top1[c, 7:8, :] = jnp.where(first, row0, part[0:1])
        top1[c, 6:7, :] = jnp.where(first, row0, up[base + 2 * c + 1 : base + 2 * c + 2, :])
        end1[c, 8:16, :] = z1[c, h1 - 8 : h1, :]
        end1[c, 15:16, :] = end
        end1[c, 16:17, :] = jnp.where(last, end, part[4:5])
        end1[c, 17:21, :] = jnp.where(last, jnp.broadcast_to(end, (4, 128)), lo[base + 4 * c : base + 4 * c + 4, :])
    h2, width2 = sizes[2]
    wq = up128(width1)
    for c in range(z1.shape[0]):
        tmp[0:1, 128 * c : 128 * c + 128] = up[base + 2 * c : base + 2 * c + 1, :] + tail(top1[c, 7:8, :], top1[c, 8:9, :])
    tmp[1:3, :wq] = rows_sum(top1, 6, 2)
    tmp[3:6, :wq] = rows_sum(end1, 12, 3)
    edge = cols_coarsen(tmp[:, :wq], width1)
    for c in range(z2.shape[0]):
        part = edge[:, 128 * c : 128 * c + 128]
        row0, end = part[1:2], part[3:4]
        at = base + 2 * z1.shape[0] + 13 * c
        w2[c, h2 - 14 : h2 - 1, :] = jnp.where(first, jnp.broadcast_to(row0, (13, 128)), up[at : at + 13, :])
        w2[c, h2 : 2 * h2, :] = z2[c]
        at = base + 4 * z1.shape[0] + 9 * c
        w2[c, 2 * h2 + 2 : 2 * h2 + 11, :] = jnp.where(last, jnp.broadcast_to(end, (9, 128)), lo[at : at + 9, :])
        w2[c, h2 - 1 : h2, :] = jnp.where(first, row0, part[0:1])
        w2[c, h2 : h2 + 2, :] = part[1:3]
        w2[c, 2 * h2 - 1 : 2 * h2, :] = end
        w2[c, 2 * h2 : 2 * h2 + 1, :] = jnp.where(last, end, part[4:5])
        w2[c, 2 * h2 + 1 : 2 * h2 + 2, :] = jnp.where(last, end, part[5:6])
    h3, width3 = sizes[3]
    wq = up128(width2)
    v = cols_coarsen(pad_rows(rows_sum(w2, h2 - 14, h3 + 11)), width2)
    row = row_of(v) - 6
    v = jnp.where(first & (row < 0), v[6:7], jnp.where(last & (row >= h3), v[h3 + 5 : h3 + 6], v))
    w3[0] = v
    h4, width4 = sizes[4]
    v = pad_rows(rows_sum(w3, 0, h4 + 4))
    row = row_of(v) - 2
    column = lane_of(v) & 63
    for i, step in enumerate((0, -1, 1)):
        at = 2 * jnp.clip(column + step, 0, width4 - 1)
        taps = [lanes(v, jnp.clip(at + tap, 0, width3 - 1)) for tap in (-2, -1, 0, 1, 2)]
        level = (taps[0] + taps[4]) * 0.0625 + (taps[1] + taps[3]) * 0.25 + taps[2] * 0.375
        level = jnp.where(first & (row < 0), level[2:3], jnp.where(last & (row >= h4), level[h4 + 1 : h4 + 2], level))
        w4[i, 0:8, :] = level
        w4[i, 8:16, :] = level

    totals = []

    def add(k, slope, bend, kept):
        kept = kept & (lane_of(slope) < sizes[k][1])
        totals.append((acc_ref[k] + fold(jnp.where(kept, slope, 0.0)),
                       acc_ref[LEVELS + k] + fold(jnp.where(kept, bend * bend, 0.0))))

    def ends(top, top_at, bottom, bottom_at):
        a, b = take(top, top_at, 8), take(bottom, bottom_at - 4, 8)
        return jnp.where(row_of(a) < 4, a, b)

    slope, bend = relief(*(ends(top0, 7 + i, end0, 11 + i) for i in range(3)), width0, 1.0)
    for ref, v in ((s0_ref, slope), (b0_ref, bend)):
        ref[0:4, :] = v[0:4]
        ref[h0 - 4 : h0, :] = v[4:8]
    add(0, slope, bend, (row_of(slope) == 0) | (row_of(slope) == 7))
    for k, top, bottom, top_at, bottom_at, t, u in ((1, top1, end1, 7, 13, t1, u1), (2, w2, w2, h2 - 1, 2 * h2 - 3, t2, u2)):
        h, width = sizes[k]
        slope, bend = relief(*(ends(top, top_at - 1 + i, bottom, bottom_at - 1 + i) for i in range(3)), width, float(2**k))
        add(k, slope, bend, (row_of(slope) > 0) & (row_of(slope) < 7))
        for field, v in enumerate((slope, bend)):
            row = row_of(v)
            v = jnp.where(first & (row == 0), v[1:2], jnp.where(last & (row == 7), v[6:7], v))
            for c, part in enumerate(cols_refine(split(v), k, width, t.shape[1])):
                t[field, c, 0:4, :] = part[0:4]
                t[field, c, h - 2 : h + 2, :] = part[4:8]
            rows_refine(t, u, field, k, h)
    for k, z, at, f in ((3, w3, 5, f3), (4, w4, 1, f4)):
        h, width = sizes[k]
        rows = -(-(h + 2) // 8) * 8
        if k == 3:
            slope, bend = relief(take(z, at - 1, rows), take(z, at, rows), take(z, at + 1, rows), width, float(2**k))
        else:
            around = [[z[i, at + j : at + j + rows, :] for j in (-1, 0, 1)] for i in range(3)]
            slope, bend = relief(*around[0], width, float(2**k), around[1:])
        row = row_of(slope) - 1
        if k == 3:
            add(k, slope, bend, (row >= 0) & (row < h))
        else:
            kept = (row >= 0) & (row < h)
            slope4, bend4 = jnp.where(kept, slope, 0.0), jnp.where(kept, bend * bend, 0.0)
        for field, v in enumerate((slope, bend)):
            v = jnp.where(first & (row < 0), v[1:2], jnp.where(last & (row >= h), v[h : h + 1], v))
            if k == 3:
                f[field] = v[0:8]
                f4[field, sizes[4][0] + 2 :, :] = pad_rows(v[8 : h + 2])[0 : 6 - sizes[4][0]]
            else:
                f[field, 0 : h + 2, :] = v[0 : h + 2]
    table = jnp.zeros((8, 128), f32)
    lane = lane_of(table)
    for k, pair in enumerate(totals):
        for field, v in enumerate(pair):
            table = jnp.where(lane == 64 * field + width4 + k, jnp.sum(v, axis=1, keepdims=True), table)
    table = jnp.where((lane & 63) < width4, jnp.where(lane < 64, slope4, bend4), table)
    line = jnp.sum(table, axis=0, keepdims=True)
    sum_ref[...] = jnp.broadcast_to(line.reshape(1, 1, 128), sum_ref.shape)


def pad_rows(v):
    short = -v.shape[0] % 8
    return jnp.concatenate([v, jnp.zeros((short, v.shape[1]), f32)], axis=0) if short else v


def cols_refine(blocks, k, width, count):
    f = 1 << k
    lane = lax.broadcasted_iota(jnp.int32, blocks[0].shape, 1)
    west_side = (lane & (f - 1)) < f // 2
    pos = ((lane & (f - 1)).astype(f32) + 0.5) * (1.0 / f)
    other = jnp.abs(pos - 0.5)
    out = []
    for c in range(count):
        at, first = divmod((128 * c) >> k, 128)
        centre = first + (lane >> k)
        near = jnp.where(west_side, centre - 1, centre + 1)
        if c == 0:
            near = jnp.maximum(near, 0)
        if c == count - 1:
            near = jnp.minimum(near, width - 1 - 128 * at)
        near = near & 127
        side = lanes(blocks[at], near)
        if c and first == 0:
            side = jnp.where(lane < f // 2, lanes(blocks[at - 1], near), side)
        if c < count - 1 and first + (128 >> k) == 128:
            side = jnp.where(lane >= 128 - f // 2, lanes(blocks[at + 1], near), side)
        out.append((1.0 - other) * lanes(blocks[at], centre) + other * side)
    return out


def last_refine(sizes, v, count):
    lane, coarse = lane_of(v), row_of(v) < sizes[LEVELS][0] + 2
    f = jnp.where(coarse, 1 << LEVELS, 1 << (LEVELS - 1))
    phase = lane & (f - 1)
    step = jnp.where(phase < f >> 1, -1, 1)
    other = jnp.abs((phase.astype(f32) + 0.5) * jnp.where(coarse, 2.0**-LEVELS, 2.0 ** (1 - LEVELS)) - 0.5)
    end = jnp.where(coarse, sizes[LEVELS][1] - 1, sizes[LEVELS - 1][1] - 1)
    out = []
    for c in range(count):
        centre = jnp.where(coarse, (128 * c + lane) >> LEVELS, (128 * c + lane) >> (LEVELS - 1))
        near = jnp.clip(centre + step, 0, end)
        out.append((1.0 - other) * lanes(v, centre) + other * lanes(v, near))
    return out


def finish_kernel(sizes, cells, v_ref, s0, b0, u1, u2, f3, f4, slope_ref, bend_ref, t3, t4, u3, u4, slope_buf, bend_buf, sems):
    h0, width0 = sizes[0]
    count = width0 // 128
    sums = jnp.sum(v_ref[...], axis=0, keepdims=True)
    lane = lax.broadcasted_iota(jnp.int32, (1, 128), 1)
    slot = sizes[LEVELS][1]
    number = jnp.ones((1, 128), f32)
    for k, c in enumerate(cells):
        number = jnp.where((lane & 63) == slot + k, float(c), number)
    last = [
        jnp.sum(jnp.where((lane >= at) & (lane < at + slot), sums, 0.0), axis=1, keepdims=True) for at in (0, 64)
    ]
    sums = jnp.where(lane == slot + LEVELS, last[0], jnp.where(lane == 64 + slot + LEVELS, last[1], sums))
    mean = sums / number
    scale = jnp.where(lane < 64, 1.0 / (mean + EPS), 1.0 / jnp.sqrt(mean + EPS))
    for field in range(2):
        for c, v in enumerate(cols_refine([f3[field]], 3, sizes[3][1], count)):
            t3[field, c, 0:8, :] = v
        for c, v in enumerate(last_refine(sizes, f4[field], count)):
            t4[field, c] = v
            t3[field, c, 8 : sizes[3][0] + 2, :] = v[sizes[4][0] + 2 : sizes[4][0] + sizes[3][0] - 4]
        rows_refine(t3, u3, field, 3, sizes[3][0])
        pos = (lax.broadcasted_iota(jnp.int32, (8, 128), 0).astype(f32) + 0.5) * 0.0625
        for c in range(count):
            for at in range(0, h0, 16):
                a, b, d = (jnp.broadcast_to(t4[field, c, at // 16 + i : at // 16 + i + 1, :], (8, 128)) for i in range(3))
                u4[field, c, at : at + 8, :] = (0.5 - pos) * a + (0.5 + pos) * b
                u4[field, c, at + 8 : at + 16, :] = (1.0 - pos) * b + pos * d
    copies = []
    for field, (base, buf, out) in enumerate(((s0, slope_buf, slope_ref), (b0, bend_buf, bend_ref))):
        weights = [jnp.broadcast_to(scale[:, i : i + 1], (8, 128)) for i in range(64 * field + slot, 64 * field + slot + LEVELS + 1)]
        for part in range(2):
            begin, end = part * h0 // 2, (part + 1) * h0 // 2
            for c in range(count):
                for at in range(begin, end, 8):
                    total = base[at : at + 8, 128 * c : 128 * c + 128] * weights[0]
                    for weight, u in zip(weights[1:], (u1, u2, u3, u4)):
                        total = total + u[field, c, at : at + 8, :] * weight
                    buf[at : at + 8, 128 * c : 128 * c + 128] = total
            rows = pl.ds(begin, end - begin)
            copy = pltpu.make_async_copy(buf.at[rows], out.at[rows], sems.at[2 * field + part])
            copy.start()
            copies.append(copy)
    for copy in copies:
        copy.wait()


def halo_pairs(count):
    both = lambda pairs: [(a, b) for a, b in pairs] + [(b, a) for a, b in pairs]
    even = [(i, i + 1) for i in range(0, count - 1, 2)]
    odd = [(i, i + 1) for i in range(1, count - 1, 2)]
    if count % 2 or count < 8:
        return both(even), both(odd), None, 0
    mid = count * 13 // 16 & ~1
    second = [e for e in odd if e[1] != mid] + [(0, mid - 1), (mid, count - 1)]
    third = [e for e in even if e[0] not in (mid - 2, mid)] + [(mid - 1, mid), (mid - 2, mid + 1)]
    return both(even), both(second), both(third), mid


VM = pl.BlockSpec(memory_space=pltpu.VMEM)
ANY = pl.BlockSpec(memory_space=pl.ANY)


def call(kernel, outs, scratch=(), in_specs=None, out_specs=None, flops=10**6, limit=8 << 20, aliases=None):
    return lambda *args: pl.pallas_call(
        kernel,
        out_shape=[jax.ShapeDtypeStruct(s, f32) for s in outs],
        in_specs=in_specs or [VM] * len(args),
        out_specs=out_specs or [VM] * len(outs),
        scratch_shapes=list(scratch),
        input_output_aliases=aliases or {},
        compiler_params=pltpu.CompilerParams(vmem_limit_bytes=limit),
        cost_estimate=pl.CostEstimate(flops=flops, bytes_accessed=1 << 19, transcendentals=0),
    )(*args)


def local(grid):
    h0, width0 = grid.shape
    count = lax.axis_size("rows")
    sizes = [(h0 >> k, width0 >> k) for k in range(LEVELS + 1)]

    def blocks(rows, width):
        return (up128(width) // 128, -(-rows // 8) * 8, 128)

    z_shapes = [blocks(*size) for size in sizes]
    rows = 3 * z_shapes[0][0] + max(2 * z_shapes[1][0] + 13 * z_shapes[2][0], 4 * z_shapes[1][0] + 9 * z_shapes[2][0])
    msg = (-(-rows // 8) * 8, 128)
    m1, m2, z0, z1, z2 = call(
        functools.partial(pyramid_kernel, sizes),
        [msg, msg] + z_shapes[:3],
        [pltpu.VMEM((h0 // 2, width0), f32)] + [pltpu.VMEM(msg, f32)] * 2 + [pltpu.SemaphoreType.DMA((z_shapes[0][0],))],
        in_specs=[pl.BlockSpec(memory_space=pltpu.HBM)],
    )(pltpu.with_memory_space_constraint(grid, pltpu.HBM))
    pairs1, pairs2, pairs3, mid = halo_pairs(count)
    r2 = lax.ppermute(m2, "rows", pairs2)
    r1 = lax.ppermute(m1, "rows", pairs1)
    r3 = lax.ppermute(m2, "rows", pairs3) if mid else m2
    acc = (2 * LEVELS, 8, 128)
    fine = [(2, z_shapes[0][0], -(-(h + 2) // 8) * 8, 128) for h, _ in sizes[1:]]
    whole = (2, *z_shapes[0])
    f_shapes = fine[:2] + [whole] * 2 + [(2, 8, up128(w)) for _, w in sizes[3:]]
    s0, b0, t1, t2, sums = call(
        functools.partial(inner_kernel, sizes), [grid.shape, grid.shape] + fine[:2] + [acc], flops=10**8
    )(z0, z1, z2)
    s0, b0, _, _, u1, u2, f3, f4, sums = call(
        functools.partial(edge_kernel, sizes, mid),
        [grid.shape, grid.shape] + f_shapes + [(count, 1, 128)],
        [pltpu.VMEM(msg, f32)] * 2
        + [pltpu.VMEM(blocks(rows, sizes[k][1]), f32) for k in range(2) for rows in (24, 24)]
        + [pltpu.VMEM(blocks(3 * sizes[2][0], sizes[2][1]), f32)]
        + [pltpu.VMEM(blocks(sizes[3][0] + 16, sizes[3][1]), f32)]
        + [pltpu.VMEM((3, 16, 128), f32), pltpu.VMEM((8, width0), f32)],
        aliases={7: 0, 8: 1, 9: 2, 10: 3},
    )(z0, z1, z2, r1, r2, r3, sums, s0, b0, t1, t2)
    seen = lax.all_to_all(sums, "rows", 0, 0, tiled=True).reshape(count, 128)
    cells = [count * h * w for h, w in sizes]
    return tuple(
        call(
            functools.partial(finish_kernel, sizes, cells),
            [grid.shape, grid.shape],
            [pltpu.VMEM(v, f32) for v in fine[2:] + [whole] * 2 + [grid.shape] * 2] + [pltpu.SemaphoreType.DMA((4,))],
            out_specs=[ANY, ANY],
        )(seen, s0, b0, u1, u2, f3, f4)
    )


def solution(mesh):
    return jax.shard_map(
        local,
        mesh=mesh,
        in_specs=(P("rows", None),),
        out_specs=(P("rows", None), P("rows", None)),
        check_vma=False,
    )
```

```python
import functools

import jax
import jax.numpy as jnp
from jax import lax
from jax.experimental import pallas as pl
from jax.experimental.pallas import tpu as pltpu
from jax.sharding import PartitionSpec as P

LEVELS = 4
EPS = 1e-06
f32 = jnp.float32
ATAN = (
    1.0,
    -0.3333314528,
    0.1999355085,
    -0.1420889944,
    0.1065626393,
    -0.0752896400,
    0.0429096138,
    -0.0161657367,
    0.0028662257,
)


def up128(n):
    return -(-n // 128) * 128


def lane_of(v):
    return lax.broadcasted_iota(jnp.int32, v.shape, 1)


def row_of(v):
    return lax.broadcasted_iota(jnp.int32, v.shape, 0)


def west(v):
    return jnp.where(lane_of(v) == 0, v, pltpu.roll(v, 1, 1))


def east(v, width):
    return jnp.where(lane_of(v) == width - 1, v, pltpu.roll(v, v.shape[1] - 1, 1))


def take(ref, at, count):
    return jnp.concatenate([ref[c, at : at + count, :] for c in range(ref.shape[0])], axis=1)


def store(ref, at, v):
    for c in range(ref.shape[0]):
        ref[c, at : at + v.shape[0], :] = v[:, 128 * c : 128 * c + 128]


def head(a, b, c):
    return (a * 0.0625 + b * 0.25) + c * 0.375


def tail(d, e):
    return d * 0.25 + e * 0.0625


def rows_sum(ref, start, count):
    out = []
    for c in range(ref.shape[0]):
        part = [ref[c, pl.ds(start + a, count, 2), :] for a in range(5)]
        out.append(head(*part[:3]) + tail(*part[3:]))
    return jnp.concatenate(out, axis=1)


def lanes(v, at):
    return jnp.take_along_axis(v, at, axis=1, mode="promise_in_bounds")


def split(v):
    return [v[:, at : at + 128] for at in range(0, v.shape[1], 128)]


def cols_coarsen(v, width):
    blocks = split(v)
    lane = lax.broadcasted_iota(jnp.int32, blocks[0].shape, 1)
    patterns = [(2 * lane + tap + 128) & 127 for tap in (-2, -1, 0, 1, 2)]
    found = [[lanes(v, at) for v in blocks] for at in patterns]
    out = []
    for c in range(0, len(blocks), 2):
        taps = []
        for tap, got in zip((-2, -1, 0, 1, 2), found):
            part = got[c]
            if c + 1 < len(blocks):
                part = jnp.where(2 * lane + tap < 128, part, got[c + 1])
            if tap < 0 and c:
                part = jnp.where(lane == 0, got[c - 1], part)
            if tap > 1 and c + 2 < len(blocks):
                part = jnp.where(lane == 127, got[c + 2], part)
            taps.append(part)
        if c == 0:
            taps[0] = jnp.where(lane == 0, taps[2], taps[0])
            taps[1] = jnp.where(lane == 0, taps[2], taps[1])
        taps[4] = jnp.where(lane == width // 2 - 1 - 64 * c, taps[3], taps[4])
        out.append((taps[0] + taps[4]) * 0.0625 + (taps[1] + taps[3]) * 0.25 + taps[2] * 0.375)
    return out[0] if len(out) == 1 else jnp.concatenate(out, axis=1)


def pyramid_kernel(sizes, x_ref, m1_ref, m2_ref, z0, z1, z2, tmp, below, above, sems):
    copies = [
        pltpu.make_async_copy(x_ref.at[:, pl.ds(128 * c, 128)], z0.at[c], sems.at[c]) for c in range(z0.shape[0])
    ]
    for copy in copies:
        copy.start()
    odd = lax.rem(lax.axis_index("rows"), 2) == 1
    h = sizes[0][0]
    for copy in copies:
        copy.wait()

    for c in range(z0.shape[0]):
        above[3 * c : 3 * c + 3, :] = z0[c, 0:3, :]
        w = [z0[c, h - 4 + i : h - 3 + i, :] for i in range(4)]
        below[3 * c : 3 * c + 1, :] = head(*w[:3])
        below[3 * c + 1 : 3 * c + 2, :] = w[2] * 0.0625 + w[3] * 0.25
        below[3 * c + 2 : 3 * c + 3, :] = w[3]
    row = 3 * z0.shape[0]
    for k, z in ((0, z1), (1, z2)):
        half, wp = sizes[k + 1][0], up128(sizes[k][1])
        low = k + 1
        tmp[low : half - 1, :wp] = rows_sum((z0, z1)[k], 2 * low - 2, half - 1 - low)
        store(z, 0, cols_coarsen(tmp[0:half, :wp], sizes[k][1]))
    h1, h2 = sizes[1][0], sizes[2][0]
    at = row
    for c in range(z1.shape[0]):
        above[row + 4 * c : row + 4 * c + 4, :] = z1[c, 1:5, :]
        w = [z1[c, h1 - 4 + i : h1 - 3 + i, :] for i in range(3)]
        below[at : at + 1, :] = head(*w)
        below[at + 1 : at + 2, :] = w[2]
        at += 2
    row += 4 * z1.shape[0]
    for c in range(z2.shape[0]):
        above[row + 9 * c : row + 9 * c + 9, :] = z2[c, 2:11, :]
        below[at + 13 * c : at + 13 * c + 13, :] = z2[c, h2 - 14 : h2 - 1, :]
    m1_ref[...] = jnp.where(odd, above[...], below[...])
    m2_ref[...] = jnp.where(odd, below[...], above[...])


def relief(upper, middle, lower, width, spacing, sides=None):
    diff = lower - upper
    if sides is None:
        tall = lower + upper + 2.0 * middle
        (d_w, m_w, t_w), (d_e, m_e, t_e) = ([west(v) for v in (diff, middle, tall)], [east(v, width) for v in (diff, middle, tall)])
    else:
        (d_w, m_w, t_w), (d_e, m_e, t_e) = ((c - a, b, c + a + 2.0 * b) for a, b, c in sides)
    p = (t_e - t_w) * (1.0 / (8.0 * spacing))
    q = (d_e + d_w + 2.0 * diff) * (1.0 / (8.0 * spacing))
    inv = 1.0 / (spacing * spacing)
    r = ((m_e - middle) - (middle - m_w)) * inv
    t = ((lower - middle) - (middle - upper)) * inv
    u = (d_e - d_w) * (0.25 * inv)
    pp, qq = p * p, q * q
    steep = pp + qq
    base = 1.0 + steep
    root = jnp.sqrt(base)
    y = jnp.sqrt(steep) / (1.0 + root)
    y2 = y * y
    y4 = y2 * y2
    y8 = y4 * y4
    pairs = [ATAN[i] + ATAN[i + 1] * y2 for i in range(0, 8, 2)]
    acc = (pairs[0] + pairs[1] * y4) + ((pairs[2] + pairs[3] * y4) + ATAN[8] * y8) * y8
    slope = 2.0 * y * acc
    bend = -(pp * r + 2.0 * (p * q) * u + qq * t) / (base * root)
    return slope, bend


def fold(v):
    total = None
    for row in range(0, v.shape[0], 8):
        for at in range(0, v.shape[1], 128):
            part = v[row : row + 8, at : at + 128]
            total = part if total is None else total + part
    return total


def inner_kernel(sizes, z0, z1, z2, s0_ref, b0_ref, t1, t2, acc_ref):
    for k, z in enumerate((z0, z1, z2)):
        h, width = sizes[k]
        s_sum = b_sum = None
        for at in range(0, h, 8):
            middle = take(z, at, 8)
            upper = take(z, at - 1, 8) if at else pltpu.roll(middle, 1, 0)
            lower = take(z, at + 1, 8) if at < h - 8 else pltpu.roll(middle, 7, 0)
            slope, bend = relief(upper, middle, lower, width, float(2**k))
            if k == 0:
                s0_ref[at : at + 8, :] = slope
                b0_ref[at : at + 8, :] = bend
            else:
                t = (t1, t2)[k - 1]
                for field, v in enumerate((slope, bend)):
                    for c, part in enumerate(cols_refine(split(v), k, width, t.shape[1])):
                        t[field, c, at + 1 : at + 9, :] = part
            skip = 3 if k else 1
            if at == 0 or at == h - 8 or width % 128:
                row = row_of(slope) + at
                kept = (row >= skip) & (row < h - skip) & (lane_of(slope) < width)
                slope, bend = jnp.where(kept, slope, 0.0), jnp.where(kept, bend, 0.0)
            fs, fb = fold(slope), fold(bend * bend)
            s_sum = fs if at == 0 else s_sum + fs
            b_sum = fb if at == 0 else b_sum + fb
        acc_ref[k] = s_sum
        acc_ref[LEVELS + k] = b_sum
    for k in range(3, LEVELS):
        acc_ref[k] = jnp.zeros((8, 128), f32)
        acc_ref[LEVELS + k] = jnp.zeros((8, 128), f32)


def rows_refine(t, u, field, k, height):
    f = 1 << k
    for c in range(t.shape[1]):
        for at in range(0, height, 8):
            before, centre, after = (t[field, c, at + i : at + i + 8, :] for i in range(3))
            for s in range(f):
                near = abs((s + 0.5) / f - 0.5)
                u[field, c, pl.ds(f * at + s, 8, f), :] = (1.0 - near) * centre + near * (before if s < f // 2 else after)


def edge_kernel(sizes, mid, z0, z1, z2, r1_ref, r2_ref, r3_ref, acc_ref, s0_in, b0_in, t1_in, t2_in,
                s0_ref, b0_ref, t1, t2, u1, u2, f3, f4, sum_ref, up, lo, top0, end0, top1, end1, w2, w3, w4, tmp):
    me = lax.axis_index("rows")
    odd = lax.rem(me, 2) == 1
    first, last = me == 0, me == lax.axis_size("rows") - 1
    r1, r2 = r1_ref[...], r2_ref[...]
    if mid:
        r2 = jnp.where((me == mid) | (me == mid - 1), r3_ref[...], r2)
    up[...] = jnp.where(odd, r1, r2)
    lo[...] = jnp.where(odd, r2, r1)

    h0, width0 = sizes[0]
    for c in range(z0.shape[0]):
        block = slice(128 * c, 128 * c + 128)
        w = [z0[c, i : i + 1, :] for i in range(3)]
        top0[c, 8:16, :] = z0[c, 0:8, :]
        top0[c, 7:8, :] = jnp.where(first, w[0], up[3 * c + 2 : 3 * c + 3, :])
        tmp[0:1, block] = up[3 * c : 3 * c + 1, :] + tail(up[3 * c + 2 : 3 * c + 3, :], w[0])
        start = jnp.where(first, w[0] * 0.0625 + w[0] * 0.25, up[3 * c + 1 : 3 * c + 2, :])
        tmp[1:2, block] = (start + w[0] * 0.375) + tail(w[1], w[2])
        end0[c, 8:16, :] = z0[c, h0 - 8 : h0, :]
        end0[c, 16:19, :] = jnp.where(last, jnp.broadcast_to(z0[c, h0 - 1 : h0, :], (3, 128)), lo[3 * c : 3 * c + 3, :])
    base = 3 * z0.shape[0]
    h1, width1 = sizes[1]
    tmp[3:5, :] = rows_sum(end0, 12, 2)
    edge = cols_coarsen(tmp[...], width0)
    for c in range(z1.shape[0]):
        part = edge[:, 128 * c : 128 * c + 128]
        row0, end = part[1:2], part[3:4]
        top1[c, 8:16, :] = z1[c, 0:8, :]
        top1[c, 8:9, :] = row0
        top1[c, 7:8, :] = jnp.where(first, row0, part[0:1])
        top1[c, 6:7, :] = jnp.where(first, row0, up[base + 2 * c + 1 : base + 2 * c + 2, :])
        end1[c, 8:16, :] = z1[c, h1 - 8 : h1, :]
        end1[c, 15:16, :] = end
        end1[c, 16:17, :] = jnp.where(last, end, part[4:5])
        end1[c, 17:21, :] = jnp.where(last, jnp.broadcast_to(end, (4, 128)), lo[base + 4 * c : base + 4 * c + 4, :])
    h2, width2 = sizes[2]
    wq = up128(width1)
    for c in range(z1.shape[0]):
        tmp[0:1, 128 * c : 128 * c + 128] = up[base + 2 * c : base + 2 * c + 1, :] + tail(top1[c, 7:8, :], top1[c, 8:9, :])
    tmp[1:3, :wq] = rows_sum(top1, 6, 2)
    tmp[3:6, :wq] = rows_sum(end1, 12, 3)
    edge = cols_coarsen(tmp[:, :wq], width1)
    for c in range(z2.shape[0]):
        part = edge[:, 128 * c : 128 * c + 128]
        row0, end = part[1:2], part[3:4]
        at = base + 2 * z1.shape[0] + 13 * c
        w2[c, h2 - 14 : h2 - 1, :] = jnp.where(first, jnp.broadcast_to(row0, (13, 128)), up[at : at + 13, :])
        w2[c, h2 : 2 * h2, :] = z2[c]
        at = base + 4 * z1.shape[0] + 9 * c
        w2[c, 2 * h2 + 2 : 2 * h2 + 11, :] = jnp.where(last, jnp.broadcast_to(end, (9, 128)), lo[at : at + 9, :])
        w2[c, h2 - 1 : h2, :] = jnp.where(first, row0, part[0:1])
        w2[c, h2 : h2 + 2, :] = part[1:3]
        w2[c, 2 * h2 - 1 : 2 * h2, :] = end
        w2[c, 2 * h2 : 2 * h2 + 1, :] = jnp.where(last, end, part[4:5])
        w2[c, 2 * h2 + 1 : 2 * h2 + 2, :] = jnp.where(last, end, part[5:6])
    h3, width3 = sizes[3]
    wq = up128(width2)
    v = cols_coarsen(pad_rows(rows_sum(w2, h2 - 14, h3 + 11)), width2)
    row = row_of(v) - 6
    v = jnp.where(first & (row < 0), v[6:7], jnp.where(last & (row >= h3), v[h3 + 5 : h3 + 6], v))
    w3[0] = v
    h4, width4 = sizes[4]
    v = pad_rows(rows_sum(w3, 0, h4 + 4))
    row = row_of(v) - 2
    column = lane_of(v) & 63
    for i, step in enumerate((0, -1, 1)):
        at = 2 * jnp.clip(column + step, 0, width4 - 1)
        taps = [lanes(v, jnp.clip(at + tap, 0, width3 - 1)) for tap in (-2, -1, 0, 1, 2)]
        level = (taps[0] + taps[4]) * 0.0625 + (taps[1] + taps[3]) * 0.25 + taps[2] * 0.375
        level = jnp.where(first & (row < 0), level[2:3], jnp.where(last & (row >= h4), level[h4 + 1 : h4 + 2], level))
        w4[i, 0:8, :] = level
        w4[i, 8:16, :] = level

    totals = []

    def add(k, slope, bend, kept):
        kept = kept & (lane_of(slope) < sizes[k][1])
        totals.append((acc_ref[k] + fold(jnp.where(kept, slope, 0.0)),
                       acc_ref[LEVELS + k] + fold(jnp.where(kept, bend * bend, 0.0))))

    def ends(top, top_at, bottom, bottom_at):
        a, b = take(top, top_at, 8), take(bottom, bottom_at - 4, 8)
        return jnp.where(row_of(a) < 4, a, b)

    slope, bend = relief(*(ends(top0, 7 + i, end0, 11 + i) for i in range(3)), width0, 1.0)
    for ref, v in ((s0_ref, slope), (b0_ref, bend)):
        ref[0:4, :] = v[0:4]
        ref[h0 - 4 : h0, :] = v[4:8]
    add(0, slope, bend, (row_of(slope) == 0) | (row_of(slope) == 7))
    for k, top, bottom, top_at, bottom_at, t, u in ((1, top1, end1, 7, 13, t1, u1), (2, w2, w2, h2 - 1, 2 * h2 - 3, t2, u2)):
        h, width = sizes[k]
        slope, bend = relief(*(ends(top, top_at - 1 + i, bottom, bottom_at - 1 + i) for i in range(3)), width, float(2**k))
        add(k, slope, bend, (row_of(slope) > 0) & (row_of(slope) < 7))
        for field, v in enumerate((slope, bend)):
            row = row_of(v)
            v = jnp.where(first & (row == 0), v[1:2], jnp.where(last & (row == 7), v[6:7], v))
            for c, part in enumerate(cols_refine(split(v), k, width, t.shape[1])):
                t[field, c, 0:4, :] = part[0:4]
                t[field, c, h - 2 : h + 2, :] = part[4:8]
            rows_refine(t, u, field, k, h)
    for k, z, at, f in ((3, w3, 5, f3), (4, w4, 1, f4)):
        h, width = sizes[k]
        rows = -(-(h + 2) // 8) * 8
        if k == 3:
            slope, bend = relief(take(z, at - 1, rows), take(z, at, rows), take(z, at + 1, rows), width, float(2**k))
        else:
            around = [[z[i, at + j : at + j + rows, :] for j in (-1, 0, 1)] for i in range(3)]
            slope, bend = relief(*around[0], width, float(2**k), around[1:])
        row = row_of(slope) - 1
        if k == 3:
            add(k, slope, bend, (row >= 0) & (row < h))
        else:
            kept = (row >= 0) & (row < h)
            slope4, bend4 = jnp.where(kept, slope, 0.0), jnp.where(kept, bend * bend, 0.0)
        for field, v in enumerate((slope, bend)):
            v = jnp.where(first & (row < 0), v[1:2], jnp.where(last & (row >= h), v[h : h + 1], v))
            if k == 3:
                f[field] = v[0:8]
                f4[field, sizes[4][0] + 2 :, :] = pad_rows(v[8 : h + 2])[0 : 6 - sizes[4][0]]
            else:
                f[field, 0 : h + 2, :] = v[0 : h + 2]
    table = jnp.zeros((8, 128), f32)
    lane = lane_of(table)
    for k, pair in enumerate(totals):
        for field, v in enumerate(pair):
            table = jnp.where(lane == 64 * field + width4 + k, jnp.sum(v, axis=1, keepdims=True), table)
    table = jnp.where((lane & 63) < width4, jnp.where(lane < 64, slope4, bend4), table)
    line = jnp.sum(table, axis=0, keepdims=True)
    sum_ref[...] = jnp.broadcast_to(line.reshape(1, 1, 128), sum_ref.shape)


def pad_rows(v):
    short = -v.shape[0] % 8
    return jnp.concatenate([v, jnp.zeros((short, v.shape[1]), f32)], axis=0) if short else v


def cols_refine(blocks, k, width, count):
    f = 1 << k
    lane = lax.broadcasted_iota(jnp.int32, blocks[0].shape, 1)
    west_side = (lane & (f - 1)) < f // 2
    pos = ((lane & (f - 1)).astype(f32) + 0.5) * (1.0 / f)
    other = jnp.abs(pos - 0.5)
    out = []
    for c in range(count):
        at, first = divmod((128 * c) >> k, 128)
        centre = first + (lane >> k)
        near = jnp.where(west_side, centre - 1, centre + 1)
        if c == 0:
            near = jnp.maximum(near, 0)
        if c == count - 1:
            near = jnp.minimum(near, width - 1 - 128 * at)
        near = near & 127
        side = lanes(blocks[at], near)
        if c and first == 0:
            side = jnp.where(lane < f // 2, lanes(blocks[at - 1], near), side)
        if c < count - 1 and first + (128 >> k) == 128:
            side = jnp.where(lane >= 128 - f // 2, lanes(blocks[at + 1], near), side)
        out.append((1.0 - other) * lanes(blocks[at], centre) + other * side)
    return out


def last_refine(sizes, v, count):
    lane, coarse = lane_of(v), row_of(v) < sizes[LEVELS][0] + 2
    f = jnp.where(coarse, 1 << LEVELS, 1 << (LEVELS - 1))
    phase = lane & (f - 1)
    step = jnp.where(phase < f >> 1, -1, 1)
    other = jnp.abs((phase.astype(f32) + 0.5) * jnp.where(coarse, 2.0**-LEVELS, 2.0 ** (1 - LEVELS)) - 0.5)
    end = jnp.where(coarse, sizes[LEVELS][1] - 1, sizes[LEVELS - 1][1] - 1)
    out = []
    for c in range(count):
        centre = jnp.where(coarse, (128 * c + lane) >> LEVELS, (128 * c + lane) >> (LEVELS - 1))
        near = jnp.clip(centre + step, 0, end)
        out.append((1.0 - other) * lanes(v, centre) + other * lanes(v, near))
    return out


def finish_kernel(sizes, cells, v_ref, s0, b0, u1, u2, f3, f4, slope_ref, bend_ref, t3, t4, u3, u4, slope_buf, bend_buf, sems):
    h0, width0 = sizes[0]
    count = width0 // 128
    sums = jnp.sum(v_ref[...], axis=0, keepdims=True)
    lane = lax.broadcasted_iota(jnp.int32, (1, 128), 1)
    slot = sizes[LEVELS][1]
    number = jnp.ones((1, 128), f32)
    for k, c in enumerate(cells):
        number = jnp.where((lane & 63) == slot + k, float(c), number)
    last = [
        jnp.sum(jnp.where((lane >= at) & (lane < at + slot), sums, 0.0), axis=1, keepdims=True) for at in (0, 64)
    ]
    sums = jnp.where(lane == slot + LEVELS, last[0], jnp.where(lane == 64 + slot + LEVELS, last[1], sums))
    mean = sums / number
    scale = jnp.where(lane < 64, 1.0 / (mean + EPS), 1.0 / jnp.sqrt(mean + EPS))
    for field in range(2):
        for c, v in enumerate(cols_refine([f3[field]], 3, sizes[3][1], count)):
            t3[field, c, 0:8, :] = v
        for c, v in enumerate(last_refine(sizes, f4[field], count)):
            t4[field, c] = v
            t3[field, c, 8 : sizes[3][0] + 2, :] = v[sizes[4][0] + 2 : sizes[4][0] + sizes[3][0] - 4]
        rows_refine(t3, u3, field, 3, sizes[3][0])
        pos = (lax.broadcasted_iota(jnp.int32, (8, 128), 0).astype(f32) + 0.5) * 0.0625
        for c in range(count):
            for at in range(0, h0, 16):
                a, b, d = (jnp.broadcast_to(t4[field, c, at // 16 + i : at // 16 + i + 1, :], (8, 128)) for i in range(3))
                u4[field, c, at : at + 8, :] = (0.5 - pos) * a + (0.5 + pos) * b
                u4[field, c, at + 8 : at + 16, :] = (1.0 - pos) * b + pos * d
    copies = []
    for field, (base, buf, out) in enumerate(((s0, slope_buf, slope_ref), (b0, bend_buf, bend_ref))):
        weights = [jnp.broadcast_to(scale[:, i : i + 1], (8, 128)) for i in range(64 * field + slot, 64 * field + slot + LEVELS + 1)]
        for part in range(2):
            begin, end = part * h0 // 2, (part + 1) * h0 // 2
            for c in range(count):
                for at in range(begin, end, 8):
                    total = base[at : at + 8, 128 * c : 128 * c + 128] * weights[0]
                    for weight, u in zip(weights[1:], (u1, u2, u3, u4)):
                        total = total + u[field, c, at : at + 8, :] * weight
                    buf[at : at + 8, 128 * c : 128 * c + 128] = total
            rows = pl.ds(begin, end - begin)
            copy = pltpu.make_async_copy(buf.at[rows], out.at[rows], sems.at[2 * field + part])
            copy.start()
            copies.append(copy)
    for copy in copies:
        copy.wait()


def halo_pairs(count):
    both = lambda pairs: [(a, b) for a, b in pairs] + [(b, a) for a, b in pairs]
    even = [(i, i + 1) for i in range(0, count - 1, 2)]
    odd = [(i, i + 1) for i in range(1, count - 1, 2)]
    if count % 2 or count < 8:
        return both(even), both(odd), None, 0
    mid = count * 13 // 16 & ~1
    second = [e for e in odd if e[1] != mid] + [(0, mid - 1), (mid, count - 1)]
    third = [e for e in even if e[0] not in (mid - 2, mid)] + [(mid - 1, mid), (mid - 2, mid + 1)]
    return both(even), both(second), both(third), mid


VM = pl.BlockSpec(memory_space=pltpu.VMEM)
ANY = pl.BlockSpec(memory_space=pl.ANY)


def call(kernel, outs, scratch=(), in_specs=None, out_specs=None, flops=10**6, limit=8 << 20, aliases=None):
    return lambda *args: pl.pallas_call(
        kernel,
        out_shape=[jax.ShapeDtypeStruct(s, f32) for s in outs],
        in_specs=in_specs or [VM] * len(args),
        out_specs=out_specs or [VM] * len(outs),
        scratch_shapes=list(scratch),
        input_output_aliases=aliases or {},
        compiler_params=pltpu.CompilerParams(vmem_limit_bytes=limit),
        cost_estimate=pl.CostEstimate(flops=flops, bytes_accessed=1 << 19, transcendentals=0),
    )(*args)


def local(grid):
    h0, width0 = grid.shape
    count = lax.axis_size("rows")
    sizes = [(h0 >> k, width0 >> k) for k in range(LEVELS + 1)]

    def blocks(rows, width):
        return (up128(width) // 128, -(-rows // 8) * 8, 128)

    z_shapes = [blocks(*size) for size in sizes]
    rows = 3 * z_shapes[0][0] + max(2 * z_shapes[1][0] + 13 * z_shapes[2][0], 4 * z_shapes[1][0] + 9 * z_shapes[2][0])
    msg = (-(-rows // 8) * 8, 128)
    m1, m2, z0, z1, z2 = call(
        functools.partial(pyramid_kernel, sizes),
        [msg, msg] + z_shapes[:3],
        [pltpu.VMEM((h0 // 2, width0), f32)] + [pltpu.VMEM(msg, f32)] * 2 + [pltpu.SemaphoreType.DMA((z_shapes[0][0],))],
        in_specs=[pl.BlockSpec(memory_space=pltpu.HBM)],
    )(pltpu.with_memory_space_constraint(grid, pltpu.HBM))
    pairs1, pairs2, pairs3, mid = halo_pairs(count)
    r2 = lax.ppermute(m2, "rows", pairs2)
    r1 = lax.ppermute(m1, "rows", pairs1)
    r3 = lax.ppermute(m2, "rows", pairs3) if mid else m2
    acc = (2 * LEVELS, 8, 128)
    fine = [(2, z_shapes[0][0], -(-(h + 2) // 8) * 8, 128) for h, _ in sizes[1:]]
    whole = (2, *z_shapes[0])
    f_shapes = fine[:2] + [whole] * 2 + [(2, 8, up128(w)) for _, w in sizes[3:]]
    s0, b0, t1, t2, sums = call(
        functools.partial(inner_kernel, sizes), [grid.shape, grid.shape] + fine[:2] + [acc], flops=10**8
    )(z0, z1, z2)
    s0, b0, _, _, u1, u2, f3, f4, sums = call(
        functools.partial(edge_kernel, sizes, mid),
        [grid.shape, grid.shape] + f_shapes + [(count, 1, 128)],
        [pltpu.VMEM(msg, f32)] * 2
        + [pltpu.VMEM(blocks(rows, sizes[k][1]), f32) for k in range(2) for rows in (24, 24)]
        + [pltpu.VMEM(blocks(3 * sizes[2][0], sizes[2][1]), f32)]
        + [pltpu.VMEM(blocks(sizes[3][0] + 16, sizes[3][1]), f32)]
        + [pltpu.VMEM((3, 16, 128), f32), pltpu.VMEM((8, width0), f32)],
        aliases={7: 0, 8: 1, 9: 2, 10: 3},
    )(z0, z1, z2, r1, r2, r3, sums, s0, b0, t1, t2)
    seen = lax.all_to_all(sums, "rows", 0, 0, tiled=True).reshape(count, 128)
    cells = [count * h * w for h, w in sizes]
    return tuple(
        call(
            functools.partial(finish_kernel, sizes, cells),
            [grid.shape, grid.shape],
            [pltpu.VMEM(v, f32) for v in fine[2:] + [whole] * 2 + [grid.shape] * 2] + [pltpu.SemaphoreType.DMA((4,))],
            out_specs=[ANY, ANY],
        )(seen, s0, b0, u1, u2, f3, f4)
    )


def solution(mesh):
    return jax.shard_map(
        local,
        mesh=mesh,
        in_specs=(P("rows", None),),
        out_specs=(P("rows", None), P("rows", None)),
        check_vma=False,
    )
```
